16 devices in a mesh: rep: 4 (over y, z, core), dp: 4 (over x).
Axes of the slice: x: 4, y: 2, z: 1, core: 2. Of those that a mesh axis runs over, the one named last changes fastest.
The devices are a block of a 4x4x8 slice.
Arguments:
- x: bfloat16 [16, 4096, 640], P(('rep', 'dp')), parts along dimension 0
- dy: bfloat16 [16, 4096, 640], P(('rep', 'dp')), parts along dimension 0
- w_gate: bfloat16 [2, 640, 2048], P(None, 'dp')
- w_up: bfloat16 [2, 640, 2048], P(None, 'dp')
- w_down: bfloat16 [2, 2048, 640], P(None, 'dp')
- m_w_gate: float32 [2, 640, 2048], P(None, 'dp')
- m_w_up: float32 [2, 640, 2048], P(None, 'dp')
- m_w_down: float32 [2, 2048, 640], P(None, 'dp')
- v_w_gate: float32 [2, 640, 2048], P(None, 'dp')
- v_w_up: float32 [2, 640, 2048], P(None, 'dp')
- v_w_down: float32 [2, 2048, 640], P(None, 'dp')
Outputs:
- output 1: bfloat16 [8, 640, 2048], P('rep', 'dp'), parts along dimension 0
- output 2: bfloat16 [8, 640, 2048], P('rep', 'dp'), parts along dimension 0
- output 3: bfloat16 [8, 2048, 640], P('rep', 'dp'), parts along dimension 0
- output 4: float32 [8, 640, 2048], P('rep', 'dp'), parts along dimension 0
- output 5: float32 [8, 640, 2048], P('rep', 'dp'), parts along dimension 0
- output 6: float32 [8, 2048, 640], P('rep', 'dp'), parts along dimension 0
- output 7: float32 [8, 640, 2048], P('rep', 'dp'), parts along dimension 0
- output 8: float32 [8, 640, 2048], P('rep', 'dp'), parts along dimension 0
- output 9: float32 [8, 2048, 640], P('rep', 'dp'), parts along dimension 0
There are 4 independent parts. The reference program is written for one: setup_inputs(seed, part) draws one part's arguments, and reference() takes and returns one part's arrays. A program takes and returns all parts, laid end to end along the dimension named above; an argument that names none is the same for every part.
All inputs are finite; a program needn't handle non-finite values.
Results may differ from the reference program's by a relative error of at most 0.022.
Values are sent between devices in bfloat16 or wider.
A program may use at most 768 MiB of HBM per device.

```python
import jax
import jax.numpy as jnp
from jax import lax

SEQUENCES = 4
TOKENS = 4096
D = 640
FF = 2048
LAYERS = 2
NAMES = ("w_gate", "w_up", "w_down")
SHAPES = {"w_gate": (LAYERS, D, FF), "w_up": (LAYERS, D, FF), "w_down": (LAYERS, FF, D)}


def bump(key, n, height):
    away = (jnp.arange(n, dtype=jnp.int32) - jax.random.randint(key, (), 0, n, jnp.int32)) % n
    return jnp.where(away < n // 8, height, 1.0)


def together(key, own, strength):
    shared = jax.random.normal(key, own.shape[1:], jnp.float32)
    return (own + strength * shared) * lax.rsqrt(1 + strength * strength)


def setup_inputs(seed: int = 0, part: int = 0) -> dict:
    kx, kdy, ka, kb, kz, kf, kh, kl, *keys = jax.random.split(jax.random.key(seed), 8 + 3 * len(NAMES))
    kx, kdy, ka, kb = (jax.random.fold_in(k, part) for k in (kx, kdy, ka, kb))
    kw, km, kv = (keys[i::3] for i in range(3))
    shape = (SEQUENCES, TOKENS, D)
    much_x, much_dy = jax.random.uniform(kz, (2,), jnp.float32, 0.0, 1.0)
    loud = 2.0 ** jax.random.uniform(jax.random.fold_in(kz, 1), (), jnp.float32, -1.0, 2.0)
    layers = 2.0 ** jax.random.uniform(kl, (LAYERS, 1, 1), jnp.float32, -1.0, 1.0)
    x = together(ka, jax.random.normal(kx, shape, jnp.float32), much_x) * bump(kf, D, 4.0)
    dy = together(kb, jax.random.normal(kdy, shape, jnp.float32), much_dy)
    drawn = {"x": x.astype(jnp.bfloat16), "dy": (loud * dy * (SEQUENCES * TOKENS) ** -0.5).astype(jnp.bfloat16)}
    for key, name in zip(kw, NAMES, strict=True):
        w = jax.random.normal(key, SHAPES[name], jnp.float32) * SHAPES[name][1] ** -0.5
        drawn[name] = (w * {"w_gate": 1.0, "w_up": bump(kh, FF, 4.0), "w_down": layers}[name]).astype(jnp.bfloat16)
    for key, name in zip(km, NAMES, strict=True):
        drawn[f"m_{name}"] = 0.1 * jax.random.normal(key, SHAPES[name], jnp.float32)
    for key, name in zip(kv, NAMES, strict=True):
        drawn[f"v_{name}"] = jax.random.uniform(key, SHAPES[name], jnp.float32, 0.005, 0.015)
    return drawn


def matmul(a, w):
    return jnp.dot(a, w, preferred_element_type=jnp.float32).astype(jnp.bfloat16)


def normed(h):
    wide = h.astype(jnp.float32)
    scale = lax.rsqrt(jnp.mean(wide**2, -1, keepdims=True) + 1e-6)
    return (wide * scale).astype(jnp.bfloat16)


def layer(h, w):
    a = normed(h)
    gate = jnp.dot(a, w["w_gate"], preferred_element_type=jnp.float32)
    up = jnp.dot(a, w["w_up"], preferred_element_type=jnp.float32)
    return h + matmul((jax.nn.silu(gate) * up).astype(jnp.bfloat16), w["w_down"])


def adamw(w, m, v, g):
    m = 0.9 * m + 0.1 * g
    v = 0.95 * v + 0.05 * g * g
    step = m * lax.rsqrt(v + 1e-8) + 0.1 * w
    return (w - 0.02 * step).astype(jnp.bfloat16), m, v


def clipped(gradients, sum_of_squares, count):
    factor = jnp.minimum(1.0, 0.5 * lax.rsqrt(sum_of_squares / count + 1e-30))
    return [g * factor for g in gradients]


def stack(weights, h):
    return lax.scan(lambda h, w: (layer(h, w), None), h, weights)[0]


def reference(x, dy, w_gate, w_up, w_down, m_w_gate, m_w_up, m_w_down, v_w_gate, v_w_up, v_w_down):
    weights = dict(zip(NAMES, (w_gate, w_up, w_down), strict=True))

    def take(so_far, sequence):
        h, by_y = sequence
        _, back = jax.vjp(lambda w: stack(w, h), weights)
        return jax.tree.map(lambda total, term: total + term.astype(jnp.float32), so_far, back(by_y)[0]), None

    none_yet = {name: jnp.zeros(w.shape, jnp.float32) for name, w in weights.items()}
    by_weights, _ = lax.scan(take, none_yet, (x, dy))
    gradients = [by_weights[name].astype(jnp.bfloat16).astype(jnp.float32) for name in NAMES]
    gradients = clipped(gradients, sum(jnp.sum(g * g) for g in gradients), sum(g.size for g in gradients))
    new = [
        adamw(w.astype(jnp.float32), m, v, g)
        for w, m, v, g in zip((w_gate, w_up, w_down), (m_w_gate, m_w_up, m_w_down), (v_w_gate, v_w_up, v_w_down), gradients, strict=True)
    ]
    return tuple(one[which] for which in range(3) for one in new)
```

```python
import dataclasses
import functools

import jax
import jax.numpy as jnp
from jax import lax
from jax.experimental import pallas as pl
from jax.experimental.pallas import tpu as pltpu
from jax.sharding import PartitionSpec as P

BF, F32 = jnp.bfloat16, jnp.float32
LANES = 128
TILE = 512
VMEM_LIMIT = 67043328
NT = (((1,), (1,)), ((), ()))
NN = (((1,), (0,)), ((), ()))


@dataclasses.dataclass(frozen=True)
class Dims:
    layers: int
    tokens: int
    d: int
    ff: int
    n: int

    @property
    def own_ff(self):
        return self.ff // self.n

    @property
    def rows(self):
        return self.d // self.n

    @property
    def chunk(self):
        return self.n * LANES

    @property
    def chunks(self):
        return self.own_ff // LANES

    @property
    def tiles(self):
        return self.tokens // TILE

    @property
    def packed(self):
        return self.rows + self.d // 2 // self.n


def dot(a, b, dims=NN):
    return lax.dot_general(a, b, dims, preferred_element_type=F32)


def sliced(i, size):
    return pl.ds(pl.multiple_of(i * size, size), size)


def ring(n):
    me = lax.axis_index("dp")
    return me, lax.rem(me + 1, n), lax.rem(me + n - 1, n)


def partner():
    rep = lax.axis_index("rep")
    core = lax.rem(rep, 2)
    return core, rep + 1 - 2 * core


def greet(*others):
    barrier = pltpu.get_barrier_semaphore()
    for other in others:
        pl.semaphore_signal(barrier, inc=1, device_id=other, device_id_type=pl.DeviceIdType.MESH)
    pl.semaphore_wait(barrier, len(others))


def remote(src, dst, send, recv, device):
    return pltpu.make_async_remote_copy(src_ref=src, dst_ref=dst, send_sem=send, recv_sem=recv, device_id=device, device_id_type=pl.DeviceIdType.MESH)


class Gather:
    COPIES = 14

    def __init__(self, dm, w, sends, recvs):
        self.dm, self.w, self.sends, self.recvs = dm, w, sends, recvs
        self.me, self.right, self.left = ring(dm.n)
        self.far = lax.rem(self.me + 2, dm.n)
        self.core, self.other = partner()

    def _both(self, unit, source):
        half = self.dm.rows // 2
        at = pl.multiple_of(source * self.dm.rows + self.core * half, half)
        return self.w.at[unit, 0:2, pl.ds(at, half), :]

    def _one(self, unit, which, source):
        half = self.dm.rows // 2
        at = pl.multiple_of(source * self.dm.rows + self.core * half, half)
        return self.w.at[unit, which, pl.ds(at, half), :]

    def _down(self, unit, source, quarter=None):
        half = self.dm.d // 2
        columns = pl.ds(pl.multiple_of(source * LANES, LANES), LANES)
        if quarter is None:
            return self.w.at[unit, 2, pl.ds(pl.multiple_of(self.core * half, half), half), columns]
        return self.w.at[unit, 2, pl.ds(pl.multiple_of(self.core * half + quarter * (half // 2), half // 2), half // 2), columns]

    def _copy(self, unit, index, ref, device):
        return remote(ref, ref, self.sends.at[unit, index], self.recvs.at[unit, index], device)

    def own(self, unit):
        out = []
        for to, device in enumerate(({"dp": self.right}, {"dp": self.left})):
            out.append(self._copy(unit, 2 * to, self._both(unit, self.me), device))
            out.append(self._copy(unit, 2 * to + 1, self._down(unit, self.me), device))
        return out

    def relayed(self, unit):
        return [
            self._copy(unit, 4, self._one(unit, 0, self.left), {"dp": self.right}),
            self._copy(unit, 5, self._down(unit, self.left, 0), {"dp": self.right}),
            self._copy(unit, 6, self._one(unit, 1, self.right), {"dp": self.left}),
            self._copy(unit, 7, self._down(unit, self.right, 1), {"dp": self.left}),
        ]

    def shared(self, unit, sources):
        out = []
        for s in sources:
            source = (self.left, self.right, self.far)[s]
            out.append(self._copy(unit, 8 + 2 * s, self._both(unit, source), {"rep": self.other}))
            out.append(self._copy(unit, 9 + 2 * s, self._down(unit, source), {"rep": self.other}))
        return out

    def _arrivals(self, unit, index, ref):
        return remote(ref, ref, self.sends.at[unit, index], self.recvs.at[unit, index], {"dp": self.right})

    def step1(self, unit):
        for copy in self.own(unit):
            copy.start()

    def step2(self, unit):
        for to, source in enumerate((self.left, self.right)):
            self._arrivals(unit, 2 * to, self._both(unit, source)).wait_recv()
            self._arrivals(unit, 2 * to + 1, self._down(unit, source)).wait_recv()
        for copy in self.relayed(unit) + self.shared(unit, (0, 1)):
            copy.start()

    def step3(self, unit):
        self._arrivals(unit, 4, self._one(unit, 0, self.far)).wait_recv()
        self._arrivals(unit, 5, self._down(unit, self.far, 0)).wait_recv()
        self._arrivals(unit, 6, self._one(unit, 1, self.far)).wait_recv()
        self._arrivals(unit, 7, self._down(unit, self.far, 1)).wait_recv()
        for copy in self.shared(unit, (2,)):
            copy.start()

    def _theirs(self, unit, s):
        dm, other = self.dm, 1 - self.core
        source = (self.left, self.right, self.far)[s]
        half = dm.rows // 2
        at = pl.multiple_of(source * dm.rows + other * half, half)
        columns = pl.ds(pl.multiple_of(source * LANES, LANES), LANES)
        rows = pl.ds(pl.multiple_of(other * (dm.d // 2), dm.d // 2), dm.d // 2)
        return self.w.at[unit, 0:2, pl.ds(at, half), :], self.w.at[unit, 2, rows, columns]

    def done(self, unit):
        for s in range(3):
            both, down = self._theirs(unit, s)
            self._arrivals(unit, 8 + 2 * s, both).wait_recv()
            self._arrivals(unit, 9 + 2 * s, down).wait_recv()

    def drain(self, unit):
        for copy in self.own(unit) + self.relayed(unit) + self.shared(unit, (0, 1, 2)):
            copy.wait_send()


def fetch_own(dm, layer, chunk, unit, me, w, sources, sem):
    for which in range(2):
        for q in range(dm.n):
            pltpu.make_async_copy(
                sources[which].at[layer, :, pl.ds(q * dm.own_ff + chunk * LANES, LANES)],
                w.at[unit, which, sliced(me, dm.rows), pl.ds(q * LANES, LANES)],
                sem,
            ).start()


def await_own(dm, unit, me, w, sem):
    ref = w.at[unit, 0:2, sliced(me, dm.rows), :]
    pltpu.make_async_copy(ref, ref, sem).wait()


def scale_of(wide, axis, count):
    return lax.rsqrt(jnp.sum(wide * wide, axis, keepdims=True) / count + 1e-6)


def forward_kernel(
    dm, extra, x, dy, w_gate, w_up, w_down,
    gates, ups, a1, a1t, h1t, a0t, dyt, wd0, w1,
    abuf, xt, at, ht, w, gst, ust, natural, dyb, dytb,
    own_sem, nat_sem, x_sem, dy_sem, dyt_sem, st_sem, at_sem, out_sem, w_sem, sends, recvs,
):
    tiles, units = dm.tiles, dm.chunks + extra
    gather = Gather(dm, w, sends, recvs)
    me = gather.me
    place = lambda u: (u // dm.chunks, u % dm.chunks)
    for u in range(units):
        fetch_own(dm, *place(u), u, me, w, (w_gate, w_up), own_sem.at[u])
    for layer in range(2):
        pltpu.make_async_copy(w_down.at[layer], natural.at[layer], nat_sem.at[layer]).start()
    for t in range(tiles):
        pltpu.make_async_copy(x.at[pl.ds(t * TILE, TILE), :], abuf.at[pl.ds(t * TILE, TILE), :], x_sem.at[t]).start()
    for t in range(2):
        pltpu.make_async_copy(dy.at[pl.ds(t * TILE, TILE), :], dyb.at[t], dy_sem.at[t]).start()
    greet({"dp": gather.right}, {"dp": gather.left}, {"rep": gather.other})
    for layer in range(2):
        pltpu.make_async_copy(w_down.at[layer], natural.at[layer], nat_sem.at[layer]).wait()
    columns = pl.ds(pl.multiple_of(me * LANES, LANES), LANES)
    for u in range(units):
        layer, chunk = place(u)
        w[u, 2, :, columns] = natural[layer, pl.ds(chunk * LANES, LANES), :].T
    await_own(dm, 0, me, w, own_sem.at[0])
    gather.step1(0)

    @pl.loop(0, tiles)
    def _(t):
        at_t = sliced(t, TILE)
        pltpu.make_async_copy(x.at[at_t, :], abuf.at[at_t, :], x_sem.at[t]).wait()
        tile = abuf[at_t, :]
        wide = tile.astype(F32)
        a = (wide * scale_of(wide, -1, dm.d)).astype(BF)
        xt[:, at_t] = tile.T
        at[:, at_t] = a.T
        abuf[at_t, :] = a

    pltpu.make_async_copy(at, a0t, at_sem.at[0]).start()
    await_own(dm, 1, me, w, own_sem.at[1])
    gather.step2(0)
    gather.step1(1)

    @pl.loop(0, tiles)
    def _(t):
        slot = lax.rem(t, 2)

        @pl.when(t >= 2)
        def _():
            pltpu.make_async_copy(dytb.at[slot], dyt.at[:, sliced(t - 2, TILE)], dyt_sem.at[slot]).wait()

        pltpu.make_async_copy(dy.at[sliced(t, TILE), :], dyb.at[slot], dy_sem.at[slot]).wait()
        dytb[slot] = dyb[slot].T
        pltpu.make_async_copy(dytb.at[slot], dyt.at[:, sliced(t, TILE)], dyt_sem.at[slot]).start()

        @pl.when(t + 2 < tiles)
        def _():
            pltpu.make_async_copy(dy.at[sliced(t + 2, TILE), :], dyb.at[slot], dy_sem.at[slot]).start()

    for t in range(tiles - 2, tiles):
        pltpu.make_async_copy(dytb.at[t % 2], dyt.at[:, pl.ds(t * TILE, TILE)], dyt_sem.at[t % 2]).wait()
    gather.step3(0)

    def stored(i, which):
        slot, chunk, at_t = lax.rem(i, 2), i // tiles, sliced(lax.rem(i, tiles), TILE)
        return pltpu.make_async_copy((gst, ust)[which].at[slot], (gates, ups)[which].at[chunk, at_t, :], st_sem.at[which, slot])

    def results(t):
        at_t = sliced(t, TILE)
        return (
            pltpu.make_async_copy(abuf.at[at_t, :], a1.at[at_t, :], out_sem.at[0, t]),
            pltpu.make_async_copy(at.at[:, at_t], a1t.at[:, at_t], out_sem.at[1, t]),
            pltpu.make_async_copy(xt.at[:, at_t], h1t.at[:, at_t], out_sem.at[2, t]),
        )

    def tile_step(i, last):
        c, t = i // tiles, lax.rem(i, tiles)
        slot, at_t = lax.rem(i, 2), sliced(t, TILE)

        @pl.when(t == 0)
        def _():
            gather.done(c)
            if last:
                pltpu.make_async_copy(w.at[0 : dm.chunks, 2], wd0, w_sem.at[0]).start()

        @pl.when(jnp.logical_and(t == 1, c + 1 < units))
        def _():
            gather.step2(c + 1)

        @pl.when(jnp.logical_and(t == 1, c + 2 < units))
        def _():
            await_own(dm, c + 2, me, w, own_sem.at[c + 2])
            gather.step1(c + 2)

        @pl.when(jnp.logical_and(t == 5, c + 1 < units))
        def _():
            gather.step3(c + 1)

        @pl.when(i >= 2)
        def _():
            stored(i - 2, 0).wait()
            stored(i - 2, 1).wait()

        a = abuf[at_t, :]
        gate = dot(a, w[c, 0])
        up = dot(a, w[c, 1])
        gst[slot] = gate
        ust[slot] = up
        act = (gate * jax.nn.sigmoid(gate) * up).astype(BF)
        total = jnp.where(c == 0, 0.0, ht[:, at_t]) + dot(w[c, 2], act, NT)
        if last:
            h = xt[:, at_t] + total.astype(BF)
            wide = h.astype(F32)
            a = (wide * scale_of(wide, 0, dm.d)).astype(BF)
            xt[:, at_t] = h
            at[:, at_t] = a
            abuf[at_t, :] = a.T
        else:
            ht[:, at_t] = total
        stored(i, 0).start()
        stored(i, 1).start()
        if last:
            for copy in results(t):
                copy.start()

    steps = dm.chunks * tiles

    @pl.loop(0, steps - tiles)
    def _(i):
        tile_step(i, False)

    pltpu.make_async_copy(at, a0t, at_sem.at[0]).wait()

    @pl.loop(steps - tiles, steps)
    def _(i):
        tile_step(i, True)

    for u in range(dm.chunks, units):
        gather.done(u)
    pltpu.make_async_copy(w.at[dm.chunks : units], w1, w_sem.at[1]).start()
    for i in range(steps - 2, steps):
        stored(i, 0).wait()
        stored(i, 1).wait()
    for t in range(tiles):
        for copy in results(t):
            copy.wait()
    pltpu.make_async_copy(w.at[0 : dm.chunks, 2], wd0, w_sem.at[0]).wait()
    pltpu.make_async_copy(w.at[dm.chunks : units], w1, w_sem.at[1]).wait()
    for u in range(units):
        gather.drain(u)


class Scatter:
    def __init__(self, dm, acc, send, recv, sends, recvs):
        self.dm, self.acc, self.send, self.recv, self.sends, self.recvs = dm, acc, send, recv, sends, recvs
        self.me, self.right, self.left = ring(dm.n)
        self.far = lax.rem(self.me + 2, dm.n)

    def _copy(self, c, kind):
        device = {"dp": self.right if kind % 2 == 0 else self.left}
        slot = lax.rem(c, 2)
        return remote(self.send.at[kind], self.recv.at[slot, kind], self.sends.at[kind], self.recvs.at[slot, kind], device)

    def _parts(self, c, owner, half):
        dm, slot = self.dm, lax.rem(c, 2)
        wide = self.acc[slot, half, sliced(owner, dm.rows), :]
        columns = pl.ds(pl.multiple_of(owner * LANES, LANES), LANES)
        size = dm.d // 2 // dm.n
        pieces = [self.acc[slot, 2, pl.ds(half * (dm.d // 2) + i * size, size), columns] for i in range(dm.n)]
        return wide, pieces

    def _places(self):
        dm = self.dm
        yield (slice(0, dm.rows), slice(None))
        for i in range(dm.n):
            yield (slice(dm.rows, dm.packed), slice(i * LANES, (i + 1) * LANES))

    def _put(self, c, kind, owner, half, add=None):
        wide, pieces = self._parts(c, owner, half)
        for term, (rows, columns) in zip([wide] + pieces, self._places(), strict=True):
            if add is not None:
                term = term + self.recv[lax.rem(c, 2), add, rows, columns].astype(F32)
            self.send[kind, rows, columns] = term.astype(BF)
        self._copy(c, kind).start()

    def step1(self, c):
        self._put(c, 0, self.far, 0)
        self._put(c, 1, self.far, 1)
        self._put(c, 2, self.right, 1)
        self._put(c, 3, self.left, 0)

    def step2(self, c):
        for kind, owner, half in ((0, self.right, 0), (1, self.left, 1)):
            self._copy(c, kind).wait_recv()
            self._put(c, kind + 4, owner, half, add=kind)
        for kind in (0, 1):
            self._copy(c, kind).wait_send()

    def step3(self, c, grads, squares):
        for kind in (2, 3, 4, 5):
            self._copy(c, kind).wait_recv()
        slot = lax.rem(c, 2)
        for half, kinds in ((0, (4, 3)), (1, (2, 5))):
            wide, pieces = self._parts(c, self.me, half)
            for term, (rows, columns) in zip([wide] + pieces, self._places(), strict=True):
                for kind in kinds:
                    term = term + self.recv[slot, kind, rows, columns].astype(F32)
                g = term.astype(BF)
                grads[c, half, rows, columns] = g
                g = g.astype(F32)
                g = jnp.sum((g * g).reshape(-1, 8, g.shape[-1]), 0)
                for j in range(0, g.shape[-1], LANES):
                    squares[...] += g[:, j : j + LANES]
        for kind in (2, 3, 4, 5):
            self._copy(c, kind).wait_send()


def elementwise(gate, up, by_act):
    by_act = by_act.astype(BF).astype(F32)
    s = jax.nn.sigmoid(gate)
    silu = gate * s
    act = (silu * up).astype(BF)
    by_up = (by_act * silu).astype(BF)
    by_gate = (by_act * up * (s * (1.0 + gate * (1.0 - s)))).astype(BF)
    return act, by_gate, by_up


def add_gradients(acc, slot, first, at, dyt, act, by_gate, by_up):
    for which, (left, right) in enumerate(((at, by_gate), (at, by_up), (dyt, act))):
        acc[slot, which] = jnp.where(first, 0.0, acc[slot, which]) + dot(left, right)


def backward1_kernel(
    dm, a1, a1t, dy, dyt, h1t, w_gate, w_up, w_down, w1,
    grads_out, squares_out, dh, dht, by_gates, by_ups,
    abuf, at, dyb, dytb, w, natural, acc, bg, bu, bg2, bu2, hb, dhb, dhtb, send, recv, grads, squares,
    own_sem, nat_sem, w_sem, in_sem, b_sem, b2_sem, h_sem, o_sem, g_sem, sends, recvs, rsends, rrecvs,
):
    tiles, units = dm.tiles, dm.chunks
    gather = Gather(dm, w, sends, recvs)
    scatter = Scatter(dm, acc, send, recv, rsends, rrecvs)
    me, layer = gather.me, 1
    loads = lambda t: (
        pltpu.make_async_copy(a1.at[sliced(t, TILE), :], abuf.at[sliced(t, TILE), :], in_sem.at[0, t]),
        pltpu.make_async_copy(dy.at[sliced(t, TILE), :], dyb.at[sliced(t, TILE), :], in_sem.at[1, t]),
        pltpu.make_async_copy(a1t.at[:, sliced(t, TILE)], at.at[:, sliced(t, TILE)], in_sem.at[2, t]),
        pltpu.make_async_copy(dyt.at[:, sliced(t, TILE)], dytb.at[:, sliced(t, TILE)], in_sem.at[3, t]),
    )
    pltpu.make_async_copy(w1.at[0], w.at[0], w_sem.at[0]).start()
    for copy in loads(0):
        copy.start()
    for u in range(1, units):
        fetch_own(dm, layer, u, u, me, w, (w_gate, w_up), own_sem.at[u])
    pltpu.make_async_copy(w_down.at[layer], natural, nat_sem.at[0]).start()
    for t in range(1, tiles):
        for copy in loads(t):
            copy.start()
    greet({"dp": gather.right}, {"dp": gather.left}, {"rep": gather.other})
    pltpu.make_async_copy(w_down.at[layer], natural, nat_sem.at[0]).wait()
    columns = pl.ds(pl.multiple_of(me * LANES, LANES), LANES)
    for u in range(1, units):
        w[u, 2, :, columns] = natural[pl.ds(u * LANES, LANES), :].T
    await_own(dm, 1, me, w, own_sem.at[1])
    gather.step1(1)
    squares[...] = jnp.zeros_like(squares)
    pltpu.make_async_copy(w1.at[0], w.at[0], w_sem.at[0]).wait()

    def stored(i, which):
        slot, chunk, at_t = lax.rem(i, 2), i // tiles, sliced(lax.rem(i, tiles), TILE)
        return pltpu.make_async_copy((bg, bu)[which].at[slot], (by_gates, by_ups)[which].at[chunk, at_t, :], b_sem.at[which, slot])

    steps = dm.chunks * tiles

    @pl.loop(0, steps)
    def _(i):
        c, t = i // tiles, lax.rem(i, tiles)
        slot, at_t = lax.rem(i, 2), sliced(t, TILE)

        @pl.when(c == 0)
        def _():
            for copy in loads(t):
                copy.wait()

        @pl.when(jnp.logical_and(t == 0, c >= 1))
        def _():
            gather.done(c)
            scatter.step1(c - 1)

        @pl.when(i == 2)
        def _():
            gather.step2(1)
            await_own(dm, 2, me, w, own_sem.at[2])
            gather.step1(2)

        @pl.when(i == 4)
        def _():
            gather.step3(1)

        @pl.when(i == 5)
        def _():
            gather.step2(2)
            await_own(dm, 3, me, w, own_sem.at[3])
            gather.step1(3)

        @pl.when(i == 7)
        def _():
            gather.step3(2)

        @pl.when(i == tiles + 1)
        def _():
            gather.step2(3)

        @pl.when(i == tiles + 3)
        def _():
            gather.step3(3)

        @pl.when(jnp.logical_and(t == 5, c >= 1))
        def _():
            scatter.step2(c - 1)

        @pl.when(jnp.logical_and(t == 7, c >= 1))
        def _():
            scatter.step3(c - 1, grads, squares)

        @pl.when(i >= 2)
        def _():
            stored(i - 2, 0).wait()
            stored(i - 2, 1).wait()

        a = abuf[at_t, :]
        act, by_gate, by_up = elementwise(dot(a, w[c, 0]), dot(a, w[c, 1]), dot(dyb[at_t, :], w[c, 2]))
        bg[slot] = by_gate
        bu[slot] = by_up
        add_gradients(acc, lax.rem(c, 2), t == 0, at[:, at_t], dytb[:, at_t], act, by_gate, by_up)
        stored(i, 0).start()
        stored(i, 1).start()

    last = dm.chunks - 1
    scatter.step1(last)
    for i in range(steps - 2, steps):
        stored(i, 0).wait()
        stored(i, 1).wait()

    def inputs(t):
        slot, at_t = lax.rem(t, 2), sliced(t, TILE)
        return (
            pltpu.make_async_copy(by_gates.at[:, at_t, :], bg2.at[slot], b2_sem.at[0, slot]),
            pltpu.make_async_copy(by_ups.at[:, at_t, :], bu2.at[slot], b2_sem.at[1, slot]),
            pltpu.make_async_copy(h1t.at[:, at_t], hb.at[slot], h_sem.at[slot]),
        )

    def results(t):
        slot, at_t = lax.rem(t, 2), sliced(t, TILE)
        return (
            pltpu.make_async_copy(dhb.at[slot], dh.at[at_t, :], o_sem.at[0, slot]),
            pltpu.make_async_copy(dhtb.at[slot], dht.at[:, at_t], o_sem.at[1, slot]),
        )

    for copy in inputs(0):
        copy.start()

    @pl.loop(0, tiles)
    def _(t):
        slot, at_t = lax.rem(t, 2), sliced(t, TILE)

        @pl.when(t + 1 < tiles)
        def _():
            for copy in inputs(t + 1):
                copy.start()

        @pl.when(t == 3)
        def _():
            scatter.step2(last)

        @pl.when(t == 6)
        def _():
            scatter.step3(last, grads, squares)

        for copy in inputs(t):
            copy.wait()

        @pl.when(t >= 2)
        def _():
            for copy in results(t - 2):
                copy.wait()

        by_a = jnp.zeros((dm.d, TILE), F32)
        for c in range(dm.chunks):
            by_a = by_a + dot(w[c, 0], bg2[slot, c], NT) + dot(w[c, 1], bu2[slot, c], NT)
        by_a = by_a.astype(BF).astype(F32)
        h = hb[slot].astype(F32)
        square = jnp.sum(h * h, 0, keepdims=True) / dm.d + 1e-6
        scale = lax.rsqrt(square)
        along = jnp.sum(h * by_a, 0, keepdims=True) * (scale / square) / dm.d
        by_h = dytb[:, at_t] + (by_a * scale - h * along).astype(BF)
        dhtb[slot] = by_h
        dhb[slot] = by_h.T
        for copy in results(t):
            copy.start()

    for t in range(tiles - 2, tiles):
        for copy in results(t):
            copy.wait()
    for u in range(1, units):
        gather.drain(u)
    pltpu.make_async_copy(grads, grads_out, g_sem.at[0]).start()
    pltpu.make_async_copy(squares, squares_out, g_sem.at[1]).start()
    pltpu.make_async_copy(grads, grads_out, g_sem.at[0]).wait()
    pltpu.make_async_copy(squares, squares_out, g_sem.at[1]).wait()


def backward0_kernel(
    dm, dh, dht, a0t, gates, ups, wd0, grads1, squares1,
    grads_out, total_out,
    dhb, dhtb, at, wd, gb, ub, acc, send, recv, grads, squares, everyone,
    in_sem, w_sem, gu_sem, g_sem, rsends, rrecvs, ssends, srecvs,
):
    tiles = dm.tiles
    scatter = Scatter(dm, acc, send, recv, rsends, rrecvs)
    me = scatter.me
    loads = lambda t: (
        pltpu.make_async_copy(dh.at[sliced(t, TILE), :], dhb.at[sliced(t, TILE), :], in_sem.at[0, t]),
        pltpu.make_async_copy(dht.at[:, sliced(t, TILE)], dhtb.at[:, sliced(t, TILE)], in_sem.at[1, t]),
        pltpu.make_async_copy(a0t.at[:, sliced(t, TILE)], at.at[:, sliced(t, TILE)], in_sem.at[2, t]),
    )

    def inputs(i):
        slot, chunk, at_t = lax.rem(i, 2), i // tiles, sliced(lax.rem(i, tiles), TILE)
        return (
            pltpu.make_async_copy(gates.at[chunk, at_t, :], gb.at[slot], gu_sem.at[0, slot]),
            pltpu.make_async_copy(ups.at[chunk, at_t, :], ub.at[slot], gu_sem.at[1, slot]),
        )

    pltpu.make_async_copy(wd0, wd, w_sem.at[0]).start()
    for copy in (*loads(0), *inputs(0)):
        copy.start()
    for t in range(1, tiles):
        for copy in loads(t):
            copy.start()
    pltpu.make_async_copy(grads1, grads.at[1], g_sem.at[0]).start()
    pltpu.make_async_copy(squares1, squares, g_sem.at[1]).start()
    greet({"dp": scatter.right}, {"dp": scatter.left}, {"dp": scatter.far})
    pltpu.make_async_copy(squares1, squares, g_sem.at[1]).wait()
    pltpu.make_async_copy(wd0, wd, w_sem.at[0]).wait()
    steps = dm.chunks * tiles

    @pl.loop(0, steps)
    def _(i):
        c, t = i // tiles, lax.rem(i, tiles)
        slot, at_t = lax.rem(i, 2), sliced(t, TILE)

        @pl.when(c == 0)
        def _():
            for copy in loads(t):
                copy.wait()

        @pl.when(i + 1 < steps)
        def _():
            for copy in inputs(i + 1):
                copy.start()

        @pl.when(jnp.logical_and(t == 0, c >= 2))
        def _():
            scatter.step3(c - 2, grads.at[0], squares)

        @pl.when(jnp.logical_and(t == 0, c >= 1))
        def _():
            scatter.step1(c - 1)

        @pl.when(jnp.logical_and(t == 7, c >= 1))
        def _():
            scatter.step2(c - 1)

        for copy in inputs(i):
            copy.wait()
        act, by_gate, by_up = elementwise(gb[slot], ub[slot], dot(dhb[at_t, :], wd[c]))
        add_gradients(acc, lax.rem(c, 2), t == 0, at[:, at_t], dhtb[:, at_t], act, by_gate, by_up)

    last = dm.chunks - 1
    scatter.step3(last - 1, grads.at[0], squares)
    scatter.step1(last)
    scatter.step2(last)
    scatter.step3(last, grads.at[0], squares)
    pltpu.make_async_copy(grads1, grads.at[1], g_sem.at[0]).wait()
    pltpu.make_async_copy(grads, grads_out, g_sem.at[2]).start()

    copies = []
    for k in range(1, dm.n):
        to = lax.rem(me + k, dm.n)
        copies.append(remote(squares, everyone.at[me], ssends.at[k - 1], srecvs.at[k - 1], {"dp": to}))
    for copy in copies:
        copy.start()
    everyone[me] = squares[...]
    for copy in copies:
        copy.wait()
    total = everyone[0]
    for k in range(1, dm.n):
        total = total + everyone[k]
    total_out[...] = total
    pltpu.make_async_copy(grads, grads_out, g_sem.at[2]).wait()


def optimizer_kernel(dm, total, grads, *refs):
    ins, outs = refs[:9], refs[9:]
    count = dm.layers * 3 * dm.d * dm.ff
    factor = jnp.minimum(1.0, 0.5 * lax.rsqrt(jnp.sum(total[...]) / count + 1e-30))
    layer, q = pl.program_id(0), pl.program_id(1)
    size = dm.d // 2 // dm.n
    wide = [
        jnp.concatenate([grads[layer, c, half, 0 : dm.rows, pl.ds(pl.multiple_of(q * LANES, LANES), LANES)] for c in range(dm.chunks)], axis=1)
        for half in range(2)
    ]
    down = jnp.concatenate(
        [grads[layer, q, half, dm.rows : dm.packed, i * LANES : (i + 1) * LANES] for half in range(2) for i in range(dm.n)], axis=0
    ).T
    for which, g in enumerate((*wide, down)):
        w, m, v = (ins[which + 3 * j][0] for j in range(3))
        g = g.astype(F32) * factor
        w = w.astype(F32)
        m = 0.9 * m + 0.1 * g
        v = 0.95 * v + 0.05 * g * g
        step = m * lax.rsqrt(v + 1e-8) + 0.1 * w
        outs[which][0] = (w - 0.02 * step).astype(BF)
        outs[which + 3][0] = m
        outs[which + 6][0] = v


def step(mesh, x, dy, *arrays):
    weights, m, v = (arrays[i : i + 3] for i in (0, 3, 6))
    x, dy = x[0], dy[0]
    w_gate, w_up, w_down = weights
    n = mesh.shape["dp"]
    dm = Dims(w_gate.shape[0], x.shape[0], x.shape[1], w_gate.shape[2], n)
    tokens, d, chunk, chunks, tiles = dm.tokens, dm.d, dm.chunk, dm.chunks, dm.tiles
    hbm = pl.BlockSpec(memory_space=pltpu.HBM)
    vmem = pl.BlockSpec(memory_space=pltpu.VMEM)
    shape = jax.ShapeDtypeStruct
    dma = lambda *s: pltpu.SemaphoreType.DMA(s)
    params = lambda i: pltpu.CompilerParams(vmem_limit_bytes=VMEM_LIMIT, collective_id=i, has_side_effects=True)
    natural, turned = (tokens, d), (d, tokens)

    extra = 1
    units = chunks + extra
    gates, ups, a1, a1t, h1t, a0t, dyt, wd0, w1 = pl.pallas_call(
        functools.partial(forward_kernel, dm, extra),
        out_shape=[
            shape((chunks, tokens, chunk), F32), shape((chunks, tokens, chunk), F32), shape(natural, BF), shape(turned, BF), shape(turned, BF),
            shape(turned, BF), shape(turned, BF), shape((chunks, d, chunk), BF), shape((extra, 3, d, chunk), BF),
        ],
        in_specs=[hbm] * 5,
        out_specs=[hbm] * 9,
        scratch_shapes=[
            pltpu.VMEM(natural, BF), pltpu.VMEM(turned, BF), pltpu.VMEM(turned, BF), pltpu.VMEM(turned, F32),
            pltpu.VMEM((units, 3, d, chunk), BF), pltpu.VMEM((2, TILE, chunk), F32), pltpu.VMEM((2, TILE, chunk), F32),
            pltpu.VMEM((2, dm.own_ff, d), BF), pltpu.VMEM((2, TILE, d), BF), pltpu.VMEM((2, d, TILE), BF),
            dma(units), dma(2), dma(tiles), dma(2), dma(2), dma(2, 2), dma(1), dma(3, tiles), dma(2),
            dma(units, Gather.COPIES), dma(units, Gather.COPIES),
        ],
        compiler_params=params(0),
        name="forward",
    )(x, dy, w_gate, w_up, w_down)

    block = (dm.packed, chunk)
    grads1, squares1, dh, dht, _, _ = pl.pallas_call(
        functools.partial(backward1_kernel, dm),
        out_shape=[
            shape((chunks, 2, *block), BF), shape((8, LANES), F32), shape(natural, BF), shape(turned, BF),
            shape((chunks, tokens, chunk), BF), shape((chunks, tokens, chunk), BF),
        ],
        in_specs=[hbm] * 9,
        out_specs=[hbm] * 6,
        scratch_shapes=[
            pltpu.VMEM(natural, BF), pltpu.VMEM(turned, BF), pltpu.VMEM(natural, BF), pltpu.VMEM(turned, BF),
            pltpu.VMEM((chunks, 3, d, chunk), BF), pltpu.VMEM((dm.own_ff, d), BF), pltpu.VMEM((2, 3, d, chunk), F32),
            pltpu.VMEM((2, TILE, chunk), BF), pltpu.VMEM((2, TILE, chunk), BF),
            pltpu.VMEM((2, chunks, TILE, chunk), BF), pltpu.VMEM((2, chunks, TILE, chunk), BF), pltpu.VMEM((2, d, TILE), BF),
            pltpu.VMEM((2, TILE, d), BF), pltpu.VMEM((2, d, TILE), BF),
            pltpu.VMEM((6, *block), BF), pltpu.VMEM((2, 6, *block), BF), pltpu.VMEM((chunks, 2, *block), BF), pltpu.VMEM((8, LANES), F32),
            dma(chunks), dma(1), dma(1), dma(4, tiles), dma(2, 2), dma(2, 2), dma(2), dma(2, 2), dma(2),
            dma(chunks, Gather.COPIES), dma(chunks, Gather.COPIES), dma(6), dma(2, 6),
        ],
        compiler_params=params(1),
        name="backward1",
    )(a1, a1t, dy, dyt, h1t, w_gate, w_up, w_down, w1)

    grads, total = pl.pallas_call(
        functools.partial(backward0_kernel, dm),
        out_shape=[shape((2, chunks, 2, *block), BF), shape((8, LANES), F32)],
        in_specs=[hbm] * 8,
        out_specs=[hbm, vmem],
        scratch_shapes=[
            pltpu.VMEM(natural, BF), pltpu.VMEM(turned, BF), pltpu.VMEM(turned, BF), pltpu.VMEM((chunks, d, chunk), BF),
            pltpu.VMEM((2, TILE, chunk), F32), pltpu.VMEM((2, TILE, chunk), F32), pltpu.VMEM((2, 3, d, chunk), F32),
            pltpu.VMEM((6, *block), BF), pltpu.VMEM((2, 6, *block), BF), pltpu.VMEM((2, chunks, 2, *block), BF), pltpu.VMEM((8, LANES), F32),
            pltpu.VMEM((n, 8, LANES), F32),
            dma(3, tiles), dma(1), dma(2, 2), dma(3), dma(6), dma(2, 6), dma(n - 1), dma(n - 1),
        ],
        compiler_params=params(2),
        name="backward0",
    )(dh, dht, a0t, gates, ups, wd0, grads1, squares1)

    wide = pl.BlockSpec((1, dm.rows, chunks * LANES), lambda l, q: (l, 0, q))
    down = pl.BlockSpec((1, LANES, d), lambda l, q: (l, q, 0))
    whole = lambda s: pl.BlockSpec(s, lambda l, q: (0,) * len(s))
    return tuple(
        pl.pallas_call(
            functools.partial(optimizer_kernel, dm),
            out_shape=[shape(w.shape, BF) for w in weights] + [shape(w.shape, F32) for w in weights] * 2,
            grid=(dm.layers, dm.n),
            in_specs=[whole((8, LANES)), whole((2, chunks, 2, *block))] + [wide, wide, down] * 3,
            out_specs=[wide, wide, down] * 3,
            compiler_params=pltpu.CompilerParams(dimension_semantics=("arbitrary", "arbitrary")),
            name="optimizer",
        )(total, grads, *weights, *m, *v)
    )


def solution(mesh):
    states, cut = P(("rep", "dp"), None, None), P(None, "dp", None)
    return jax.shard_map(
        functools.partial(step, mesh),
        mesh=mesh,
        in_specs=(states, states) + (cut,) * 9,
        out_specs=(P("rep", "dp", None),) * 9,
        check_vma=False,
    )
```

```python
import dataclasses
import functools

import jax
import jax.numpy as jnp
from jax import lax
from jax.experimental import pallas as pl
from jax.experimental.pallas import tpu as pltpu
from jax.sharding import PartitionSpec as P

BF, F32 = jnp.bfloat16, jnp.float32
LANES = 128
TILE = 1024
SMALL = 512
HALF = 256
VMEM_LIMIT = 67043328
NT = (((1,), (1,)), ((), ()))
NN = (((1,), (0,)), ((), ()))


@dataclasses.dataclass(frozen=True)
class Dims:
    layers: int
    tokens: int
    d: int
    ff: int
    n: int

    @property
    def own_ff(self):
        return self.ff // self.n

    @property
    def rows(self):
        return self.d // self.n

    @property
    def chunk(self):
        return self.n * LANES

    @property
    def chunks(self):
        return self.own_ff // LANES

    @property
    def tiles(self):
        return self.tokens // TILE

    @property
    def small(self):
        return self.tokens // SMALL

    @property
    def packed(self):
        return self.rows + self.d // 2 // self.n


def dot(a, b, dims=NN):
    return lax.dot_general(a, b, dims, preferred_element_type=F32)


def sliced(i, size):
    return pl.ds(pl.multiple_of(i * size, size), size)


def ring(n):
    me = lax.axis_index("dp")
    return me, lax.rem(me + 1, n), lax.rem(me + n - 1, n)


def partner():
    rep = lax.axis_index("rep")
    core = lax.rem(rep, 2)
    return core, rep + 1 - 2 * core


def greet(*others):
    for other in others:
        pl.semaphore_signal(pltpu.get_barrier_semaphore(), inc=1, device_id=other, device_id_type=pl.DeviceIdType.MESH)


def greeted(count):
    pl.semaphore_wait(pltpu.get_barrier_semaphore(), count)


def remote(src, dst, send, recv, device):
    return pltpu.make_async_remote_copy(src_ref=src, dst_ref=dst, send_sem=send, recv_sem=recv, device_id=device, device_id_type=pl.DeviceIdType.MESH)


class Gather:
    COPIES = 14

    def __init__(self, dm, w, sends, recvs):
        self.dm, self.w, self.sends, self.recvs = dm, w, sends, recvs
        self.me, self.right, self.left = ring(dm.n)
        self.far = lax.rem(self.me + 2, dm.n)
        self.core, self.other = partner()

    def _both(self, unit, source):
        half = self.dm.rows // 2
        at = pl.multiple_of(source * self.dm.rows + self.core * half, half)
        return self.w.at[unit, 0:2, pl.ds(at, half), :]

    def _one(self, unit, which, source):
        half = self.dm.rows // 2
        at = pl.multiple_of(source * self.dm.rows + self.core * half, half)
        return self.w.at[unit, which, pl.ds(at, half), :]

    def _down(self, unit, source, quarter=None):
        half = self.dm.d // 2
        columns = pl.ds(pl.multiple_of(source * LANES, LANES), LANES)
        if quarter is None:
            return self.w.at[unit, 2, pl.ds(pl.multiple_of(self.core * half, half), half), columns]
        return self.w.at[unit, 2, pl.ds(pl.multiple_of(self.core * half + quarter * (half // 2), half // 2), half // 2), columns]

    def _copy(self, unit, index, ref, device):
        return remote(ref, ref, self.sends.at[unit, index], self.recvs.at[unit, index], device)

    def own(self, unit, part):
        ref = self._down(unit, self.me) if part else self._both(unit, self.me)
        return [self._copy(unit, 2 * to + part, ref, device) for to, device in enumerate(({"dp": self.right}, {"dp": self.left}))]

    def relayed(self, unit, part):
        if part:
            right, left = self._down(unit, self.left, 0), self._down(unit, self.right, 1)
        else:
            right, left = self._one(unit, 0, self.left), self._one(unit, 1, self.right)
        return [self._copy(unit, 4 + part, right, {"dp": self.right}), self._copy(unit, 6 + part, left, {"dp": self.left})]

    def shared(self, unit, part, sources):
        out = []
        for s in sources:
            source = (self.left, self.right, self.far)[s]
            ref = self._down(unit, source) if part else self._both(unit, source)
            out.append(self._copy(unit, 8 + 2 * s + part, ref, {"rep": self.other}))
        return out

    def _arrivals(self, unit, index, ref):
        return remote(ref, ref, self.sends.at[unit, index], self.recvs.at[unit, index], {"dp": self.right})

    def step1(self, unit, parts=(0, 1)):
        for part in parts:
            for copy in self.own(unit, part):
                copy.start()

    def step2(self, unit):
        for part in range(2):
            for to, source in enumerate((self.left, self.right)):
                ref = self._down(unit, source) if part else self._both(unit, source)
                self._arrivals(unit, 2 * to + part, ref).wait_recv()
            for copy in self.relayed(unit, part) + self.shared(unit, part, (0, 1)):
                copy.start()

    def step3(self, unit):
        for part in range(2):
            for k in range(2):
                ref = self._down(unit, self.far, k) if part else self._one(unit, k, self.far)
                self._arrivals(unit, 4 + 2 * k + part, ref).wait_recv()
            for copy in self.shared(unit, part, (2,)):
                copy.start()

    def _theirs(self, unit, s):
        dm, other = self.dm, 1 - self.core
        source = (self.left, self.right, self.far)[s]
        half = dm.rows // 2
        at = pl.multiple_of(source * dm.rows + other * half, half)
        columns = pl.ds(pl.multiple_of(source * LANES, LANES), LANES)
        rows = pl.ds(pl.multiple_of(other * (dm.d // 2), dm.d // 2), dm.d // 2)
        return self.w.at[unit, 0:2, pl.ds(at, half), :], self.w.at[unit, 2, rows, columns]

    def done(self, unit):
        for s in range(3):
            both, down = self._theirs(unit, s)
            self._arrivals(unit, 8 + 2 * s, both).wait_recv()
            self._arrivals(unit, 9 + 2 * s, down).wait_recv()

    def drain(self, unit):
        for part in range(2):
            for copy in self.own(unit, part) + self.relayed(unit, part) + self.shared(unit, part, (0, 1, 2)):
                copy.wait_send()


def fetch_own(dm, layer, chunk, unit, me, w, sources, sem):
    for which in range(2):
        for q in range(dm.n):
            pltpu.make_async_copy(
                sources[which].at[layer, :, pl.ds(q * dm.own_ff + chunk * LANES, LANES)],
                w.at[unit, which, sliced(me, dm.rows), pl.ds(q * LANES, LANES)],
                sem,
            ).start()


def await_own(dm, unit, me, w, sem):
    ref = w.at[unit, 0:2, sliced(me, dm.rows), :]
    pltpu.make_async_copy(ref, ref, sem).wait()


def scale_of(wide, axis, count):
    return lax.rsqrt(jnp.sum(wide * wide, axis, keepdims=True) / count + 1e-6)


def move(src, dst, sem):
    return pltpu.make_async_copy(src, dst, sem)


def forward_kernel(
    dm, extra, x, dy, w_gate, w_up, w_down,
    gates, ups, acts, a1, a1t, h1t, a0t, dyt, wd0, w1,
    abuf, xt, at, ht, w, gst, ust, ast, natural, dyb, dytb,
    own_sem, nat_sem, x_sem, dy_sem, dyt_sem, st_sem, at_sem, out_sem, w_sem, sends, recvs,
):
    tiles, units = dm.tiles, dm.chunks + extra
    gather = Gather(dm, w, sends, recvs)
    me = gather.me
    place = lambda u: (u // dm.chunks, u % dm.chunks)
    greet({"dp": gather.right}, {"dp": gather.left}, {"rep": gather.other})
    fetch_own(dm, *place(0), 0, me, w, (w_gate, w_up), own_sem.at[0])
    move(w_down.at[0], natural.at[0], nat_sem.at[0]).start()
    for t in range(dm.small):
        move(x.at[pl.ds(t * SMALL, SMALL), :], abuf.at[pl.ds(t * SMALL, SMALL), :], x_sem.at[t]).start()
    await_own(dm, 0, me, w, own_sem.at[0])
    greeted(3)
    gather.step1(0, (0,))
    columns = pl.ds(pl.multiple_of(me * LANES, LANES), LANES)
    move(w_down.at[0], natural.at[0], nat_sem.at[0]).wait()
    w[0, 2, :, columns] = natural[0, 0:LANES, :].T
    gather.step1(0, (1,))
    for u in range(1, units):
        fetch_own(dm, *place(u), u, me, w, (w_gate, w_up), own_sem.at[u])
    move(w_down.at[1], natural.at[1], nat_sem.at[1]).start()
    for t in range(dm.small):
        move(dy.at[pl.ds(t * SMALL, SMALL), :], dyb.at[pl.ds(t * SMALL, SMALL), :], dy_sem.at[t]).start()

    @pl.loop(0, dm.small)
    def _(t):
        at_t = sliced(t, SMALL)
        move(x.at[at_t, :], abuf.at[at_t, :], x_sem.at[t]).wait()
        tile = abuf[at_t, :]
        wide = tile.astype(F32)
        a = (wide * scale_of(wide, -1, dm.d)).astype(BF)
        xt[:, at_t] = tile.T
        at[:, at_t] = a.T
        abuf[at_t, :] = a

    gather.step2(0)
    move(w_down.at[1], natural.at[1], nat_sem.at[1]).wait()
    for u in range(1, units):
        layer, chunk = place(u)
        w[u, 2, :, columns] = natural[layer, pl.ds(chunk * LANES, LANES), :].T
    await_own(dm, 1, me, w, own_sem.at[1])
    gather.step1(1)
    move(at, a0t, at_sem.at[0]).start()

    @pl.loop(0, dm.small)
    def _(t):
        at_t = sliced(t, SMALL)
        move(dy.at[at_t, :], dyb.at[at_t, :], dy_sem.at[t]).wait()
        dytb[:, at_t] = dyb[at_t, :].T

    move(dytb, dyt, dyt_sem.at[0]).start()
    gather.step3(0)

    def stored(i):
        slot, chunk, at_t = lax.rem(i, 2), i // tiles, sliced(lax.rem(i, tiles), TILE)
        pairs = ((gst, gates), (ust, ups), (ast, acts))
        return [move(a.at[slot], b.at[chunk, at_t, :], st_sem.at[k, slot]) for k, (a, b) in enumerate(pairs)]

    def results(t):
        at_t = sliced(t, TILE)
        return (
            move(abuf.at[at_t, :], a1.at[at_t, :], out_sem.at[0, t]),
            move(at.at[:, at_t], a1t.at[:, at_t], out_sem.at[1, t]),
            move(xt.at[:, at_t], h1t.at[:, at_t], out_sem.at[2, t]),
        )

    def tile_step(i, last):
        c, t = i // tiles, lax.rem(i, tiles)
        slot, at_t = lax.rem(i, 2), sliced(t, TILE)

        @pl.when(t == 0)
        def _():
            gather.done(c)
            if last:
                move(w.at[0 : dm.chunks, 2], wd0, w_sem.at[0]).start()

        @pl.when(t == 1)
        def _():
            gather.step2(c + 1)

        @pl.when(t == 1 if not last else t == 2)
        def _():
            if last:
                gather.step2(c + 2)
            else:
                await_own(dm, c + 2, me, w, own_sem.at[c + 2])
                gather.step1(c + 2)

        @pl.when(t == 3)
        def _():
            gather.step3(c + 1)

        if not last:

            @pl.when(i == (dm.chunks - 1) * tiles - 1)
            def _():
                await_own(dm, units - 1, me, w, own_sem.at[units - 1])
                gather.step1(units - 1)

        @pl.when(i >= 1)
        def _():
            for copy in stored(i - 1):
                copy.start()

        @pl.when(i >= 2)
        def _():
            for copy in stored(i - 2):
                copy.wait()

        if last:

            @pl.when(t >= 1)
            def _():
                for copy in results(t - 1):
                    copy.start()

        a = abuf[at_t, :]
        for b in range(0, dm.chunk, HALF):
            part = slice(b, b + HALF)
            gate = dot(a, w[c, 0, :, part])
            up = dot(a, w[c, 1, :, part])
            gst[slot, :, part] = gate
            ust[slot, :, part] = up
            ast[slot, :, part] = (gate * jax.nn.sigmoid(gate) * up).astype(BF)
        if not last:
            ht[:, at_t] = jnp.where(c == 0, 0.0, ht[:, at_t]) + dot(w[c, 2], ast[slot], NT)
            return
        for b in range(0, TILE, HALF):
            at_b = pl.ds(pl.multiple_of(t * TILE + b, HALF), HALF)
            total = ht[:, at_b] + dot(w[c, 2], ast[slot, b : b + HALF, :], NT)
            h = xt[:, at_b] + total.astype(BF)
            wide = h.astype(F32)
            a = (wide * scale_of(wide, 0, dm.d)).astype(BF)
            xt[:, at_b] = h
            at[:, at_b] = a
            abuf[at_b, :] = a.T

    steps = dm.chunks * tiles

    @pl.loop(0, steps - tiles)
    def _(i):
        tile_step(i, False)

    move(at, a0t, at_sem.at[0]).wait()

    @pl.loop(steps - tiles, steps)
    def _(i):
        tile_step(i, True)

    for copy in (*stored(steps - 1), *results(tiles - 1)):
        copy.start()
    gather.step3(units - 1)
    for u in range(dm.chunks, units):
        gather.done(u)
    move(w.at[dm.chunks : units], w1, w_sem.at[1]).start()
    for i in range(steps - 2, steps):
        for copy in stored(i):
            copy.wait()
    for t in range(tiles):
        for copy in results(t):
            copy.wait()
    move(w.at[0 : dm.chunks, 2], wd0, w_sem.at[0]).wait()
    move(w.at[dm.chunks : units], w1, w_sem.at[1]).wait()
    move(dytb, dyt, dyt_sem.at[0]).wait()
    for u in range(units):
        gather.drain(u)


class Scatter:
    def __init__(self, dm, wide, acc, send, recv, sends, recvs):
        self.dm, self.wide, self.acc, self.send, self.recv, self.sends, self.recvs = dm, wide, acc, send, recv, sends, recvs
        self.me, self.right, self.left = ring(dm.n)
        self.far = lax.rem(self.me + 2, dm.n)

    def _copy(self, c, kind):
        device = {"dp": self.right if kind % 2 == 0 else self.left}
        s, r = lax.rem(c, self.send.shape[0]), lax.rem(c, self.recv.shape[0])
        return remote(self.send.at[s, kind], self.recv.at[r, kind], self.sends.at[s, kind], self.recvs.at[r, kind], device)

    def _parts(self, c, owner, half):
        dm, slot = self.dm, lax.rem(c, self.acc.shape[0])
        if self.wide:
            return [(self.acc[slot, half, sliced(owner, dm.rows), :], slice(None))]
        columns = pl.ds(pl.multiple_of(owner * LANES, LANES), LANES)
        size = dm.d // 2 // dm.n
        return [
            (self.acc[slot, pl.ds(half * (dm.d // 2) + i * size, size), columns], slice(i * LANES, (i + 1) * LANES)) for i in range(dm.n)
        ]

    def _put(self, c, kind, owner, half, add=None):
        s, r = lax.rem(c, self.send.shape[0]), lax.rem(c, self.recv.shape[0])
        for term, columns in self._parts(c, owner, half):
            if add is not None:
                term = term + self.recv[r, add, :, columns].astype(F32)
            self.send[s, kind, :, columns] = term.astype(BF)
        self._copy(c, kind).start()

    def step1(self, c):
        self._put(c, 0, self.far, 0)
        self._put(c, 1, self.far, 1)
        self._put(c, 2, self.right, 1)
        self._put(c, 3, self.left, 0)

    def step2(self, c):
        for kind, owner, half in ((0, self.right, 0), (1, self.left, 1)):
            self._copy(c, kind).wait_recv()
            self._put(c, kind + 4, owner, half, add=kind)
        for kind in (0, 1):
            self._copy(c, kind).wait_send()

    def step3(self, c, put, squares):
        for kind in (2, 3, 4, 5):
            self._copy(c, kind).wait_recv()
        r = lax.rem(c, self.recv.shape[0])
        for half, kinds in ((0, (4, 3)), (1, (2, 5))):
            for term, columns in self._parts(c, self.me, half):
                for kind in kinds:
                    term = term + self.recv[r, kind, :, columns].astype(F32)
                g = term.astype(BF)
                put(half, columns, g)
                g = g.astype(F32)
                g = jnp.sum((g * g).reshape(-1, 8, g.shape[-1]), 0)
                for j in range(0, g.shape[-1], LANES):
                    squares[...] += g[:, j : j + LANES]
        for kind in (2, 3, 4, 5):
            self._copy(c, kind).wait_send()


def back_through(gate, up, by_act):
    by_act = by_act.astype(BF).astype(F32)
    s = jax.nn.sigmoid(gate)
    by_up = (by_act * (gate * s)).astype(BF)
    by_gate = (by_act * up * (s * (1.0 + gate * (1.0 - s)))).astype(BF)
    return by_gate, by_up


def backward1_kernel(
    dm, a1, a1t, dy, dyt, h1t, w_gate, w_up, w_down, w1,
    grads_out, squares_out, dh, dht, by_gates, by_ups,
    abuf, at, dyb, dytb, w, natural, wacc, dacc, ba, bg, bu, stash, hb, dhb, dhtb, wsend, wrecv, dsend, drecv, grads, squares,
    own_sem, nat_sem, w_sem, in_sem, b_sem, b2_sem, h_sem, o_sem, g_sem, sends, recvs, wsends, wrecvs, dsends, drecvs,
):
    tiles, small, units = dm.tiles, dm.small, dm.chunks
    gather = Gather(dm, w, sends, recvs)
    wides = Scatter(dm, True, wacc, wsend, wrecv, wsends, wrecvs)
    downs = Scatter(dm, False, dacc, dsend, drecv, dsends, drecvs)
    me, layer, known = gather.me, 1, w1.shape[0]
    loads = lambda t: (
        move(a1.at[sliced(t, TILE), :], abuf.at[sliced(t, TILE), :], in_sem.at[0, t]),
        move(dy.at[sliced(t, TILE), :], dyb.at[sliced(t, TILE), :], in_sem.at[1, t]),
        move(a1t.at[:, sliced(t, TILE)], at.at[:, sliced(t, TILE)], in_sem.at[2, t]),
        move(dyt.at[:, sliced(t, TILE)], dytb.at[:, sliced(t, TILE)], in_sem.at[3, t]),
    )
    greet({"dp": gather.right}, {"dp": gather.left}, {"rep": gather.other})
    move(w_down.at[layer], natural, nat_sem.at[0]).start()
    for u in range(known, units):
        fetch_own(dm, layer, u, u, me, w, (w_gate, w_up), own_sem.at[u])
    move(w1.at[0], w.at[0], w_sem.at[0]).start()
    for copy in loads(0):
        copy.start()
    for u in range(1, known):
        move(w1.at[u], w.at[u], w_sem.at[u]).start()
    squares[...] = jnp.zeros_like(squares)
    move(w_down.at[layer], natural, nat_sem.at[0]).wait()
    columns = pl.ds(pl.multiple_of(me * LANES, LANES), LANES)
    for u in range(known, units):
        w[u, 2, :, columns] = natural[pl.ds(u * LANES, LANES), :].T
    for u in range(known, units):
        await_own(dm, u, me, w, own_sem.at[u])
    greeted(3)
    gather.step1(known)
    for t in range(1, tiles):
        for copy in loads(t):
            copy.start()
    move(w1.at[0], w.at[0], w_sem.at[0]).wait()

    def stored(i):
        slot, chunk, at_t = lax.rem(i, 2), i // tiles, sliced(lax.rem(i, tiles), TILE)
        return [move(a.at[slot], b.at[chunk, at_t, :], b_sem.at[k, slot]) for k, (a, b) in enumerate(((bg, by_gates), (bu, by_ups)))]

    def step1(c):
        wides.step1(c)
        downs.step1(c)

    def step2(c):
        wides.step2(c)
        downs.step2(c)

    def step3(c):
        def put(first, last):
            def put(half, columns, g):
                grads[c, half, first:last, columns] = g

            return put

        wides.step3(c, put(0, dm.rows), squares)
        downs.step3(c, put(dm.rows, dm.packed), squares)

    def inputs(t):
        slot, third, at_t = lax.rem(t, 2), lax.rem(t, 3), sliced(t, SMALL)
        out = [move(h1t.at[:, at_t], hb.at[third], h_sem.at[third])]
        for k, (src, dst) in enumerate(((by_gates, abuf), (by_ups, dyb))):
            for c in range(dm.chunks):
                out.append(move(src.at[c, at_t, :], dst.at[sliced(slot * dm.chunks + c, SMALL), 0 : dm.chunk], b2_sem.at[k, slot, c]))
        return out

    steps = dm.chunks * tiles

    @pl.loop(0, steps)
    def _(i):
        c, t = i // tiles, lax.rem(i, tiles)
        slot, at_t = lax.rem(i, 2), sliced(t, TILE)

        @pl.when(c == 0)
        def _():
            for copy in loads(t):
                copy.wait()

        @pl.when(jnp.logical_and(t == 0, c >= 2))
        def _():
            gather.done(c)
            step3(c - 2)

        @pl.when(jnp.logical_and(t == 0, c >= 1))
        def _():
            step1(c - 1)

        @pl.when(i == 2)
        def _():
            gather.step2(known)
            gather.step1(known + 1)

        @pl.when(i == 3)
        def _():
            for u in range(1, known):
                move(w1.at[u], w.at[u], w_sem.at[u]).wait()
            gather.step3(known)

        @pl.when(i == 5)
        def _():
            gather.step2(known + 1)

        @pl.when(i == 7)
        def _():
            gather.step3(known + 1)

        @pl.when(jnp.logical_and(t == 2, c >= 1))
        def _():
            step2(c - 1)

        @pl.when(i >= 1)
        def _():
            for copy in stored(i - 1):
                copy.start()

        @pl.when(i >= 2)
        def _():
            for copy in stored(i - 2):
                copy.wait()

        @pl.when(i == steps - 1)
        def _():
            for copy in inputs(0):
                copy.start()

        a, y = abuf[at_t, :], dyb[at_t, :]
        for b in range(0, dm.chunk, HALF):
            part = slice(b, b + HALF)
            gate, up = dot(a, w[c, 0, :, part]), dot(a, w[c, 1, :, part])
            by_gate, by_up = back_through(gate, up, dot(y, w[c, 2, :, part]))
            ba[:, part] = (gate * jax.nn.sigmoid(gate) * up).astype(BF)
            bg[slot, :, part] = by_gate
            bu[slot, :, part] = by_up
        s = lax.rem(c, 2)
        wacc[s, 0] = jnp.where(t == 0, 0.0, wacc[s, 0]) + dot(at[:, at_t], bg[slot])
        wacc[s, 1] = jnp.where(t == 0, 0.0, wacc[s, 1]) + dot(at[:, at_t], bu[slot])
        dacc[s] = jnp.where(t == 0, 0.0, dacc[s]) + dot(dytb[:, at_t], ba[...])

    last = dm.chunks - 1
    for copy in stored(steps - 1):
        copy.start()
    step3(last - 1)
    step1(last)
    for i in range(steps - 2, steps):
        for copy in stored(i):
            copy.wait()

    def results(t):
        slot, at_t = lax.rem(t, 2), sliced(t, SMALL)
        return (
            move(dhb.at[slot], dh.at[at_t, :], o_sem.at[0, slot]),
            move(dhtb.at[slot], dht.at[:, at_t], o_sem.at[1, slot]),
        )

    def matmuls(t):
        slot, total = lax.rem(t, 2), None
        for c in range(dm.chunks):
            rows = sliced(slot * dm.chunks + c, SMALL)
            term = dot(w[c, 0], abuf[rows, 0 : dm.chunk], NT) + dot(w[c, 1], dyb[rows, 0 : dm.chunk], NT)
            total = term if total is None else total + term
        return total.astype(BF)

    def finish(t, by_a):
        slot, at_t = lax.rem(t, 2), sliced(t, SMALL)
        by_a = by_a.astype(F32)
        h = hb[lax.rem(t, 3)].astype(F32)
        square = jnp.sum(h * h, 0, keepdims=True) / dm.d + 1e-6
        scale = lax.rsqrt(square)
        along = jnp.sum(h * by_a, 0, keepdims=True) * (scale / square) / dm.d
        by_h = dytb[:, at_t] + (by_a * scale - h * along).astype(BF)
        dhtb[slot] = by_h
        dhb[slot] = by_h.T

    for copy in inputs(1):
        copy.start()
    for copy in inputs(0):
        copy.wait()
    stash[...] = matmuls(0)

    @pl.loop(1, small)
    def _(t):
        @pl.when(t >= 2)
        def _():
            for copy in results(t - 2):
                copy.start()

        @pl.when(t == 3)
        def _():
            step2(last)

        @pl.when(t == 6)
        def _():
            step3(last)

        for copy in inputs(t):
            copy.wait()

        @pl.when(t + 1 < small)
        def _():
            for copy in inputs(t + 1):
                copy.start()

        @pl.when(t >= 3)
        def _():
            for copy in results(t - 3):
                copy.wait()

        finish(t - 1, stash[...])
        stash[...] = matmuls(t)

    for copy in results(small - 2):
        copy.start()
    for copy in results(small - 3):
        copy.wait()
    finish(small - 1, stash[...])
    for copy in results(small - 1):
        copy.start()
    for t in (small - 2, small - 1):
        for copy in results(t):
            copy.wait()
    for u in range(known, units):
        gather.drain(u)
    move(grads, grads_out, g_sem.at[0]).start()
    move(squares, squares_out, g_sem.at[1]).start()
    move(grads, grads_out, g_sem.at[0]).wait()
    move(squares, squares_out, g_sem.at[1]).wait()


def backward0_kernel(
    dm, dh, dht, a0t, gates, ups, acts, wd0, grads1, squares1,
    grads_out, total_out,
    dhb, dhtb, at, wd, ab, gb, ub, bg, bu, wacc, dacc, wsend, wrecv, dsend, drecv, grads, squares, everyone,
    in_sem, w_sem, a_sem, gu_sem, g_sem, wsends, wrecvs, dsends, drecvs, ssends, srecvs,
):
    halves, cuts = 2, dm.chunk // HALF
    wides = Scatter(dm, True, wacc, wsend, wrecv, wsends, wrecvs)
    downs = Scatter(dm, False, dacc, dsend, drecv, dsends, drecvs)
    me, span = wides.me, dm.tokens // halves
    greet({"dp": wides.right}, {"dp": wides.left}, {"dp": wides.far})

    def hidden(i):
        slot = lax.rem(i, 2)
        return move(acts.at[i // halves, sliced(lax.rem(i, halves), span), :], ab.at[slot], a_sem.at[slot])

    def inputs(i):
        slot, unit, at_t = lax.rem(i, 2), i // halves, sliced(lax.rem(i, halves), span)
        columns = pl.ds(pl.multiple_of(lax.rem(unit, cuts) * HALF, HALF), HALF)
        return (
            move(gates.at[unit // cuts, at_t, columns], gb.at[slot], gu_sem.at[0, slot]),
            move(ups.at[unit // cuts, at_t, columns], ub.at[slot], gu_sem.at[1, slot]),
        )

    firsts = [move(dht.at[:, pl.ds(k * span, span)], dhtb.at[:, pl.ds(k * span, span)], in_sem.at[k]) for k in range(halves)]
    rest = [move(dh, dhb, in_sem.at[2]), move(a0t, at, in_sem.at[3]), move(wd0, wd, w_sem.at[0])]
    firsts[0].start()
    hidden(0).start()
    firsts[1].start()
    hidden(1).start()
    move(squares1, squares, g_sem.at[1]).start()
    @pl.loop(0, dm.chunks * halves)
    def _(i):
        c, t = i // halves, lax.rem(i, halves)
        for k in range(halves):

            @pl.when(i == k)
            def _():
                firsts[k].wait()

        @pl.when(i == 1)
        def _():
            greeted(3)

        @pl.when(jnp.logical_and(i >= 1, i + 1 < dm.chunks * halves))
        def _():
            hidden(i + 1).start()

        @pl.when(i == 2)
        def _():
            for copy in rest:
                copy.start()

        @pl.when(i == 5)
        def _():
            for copy in (*inputs(0), *inputs(1), move(grads1, grads.at[1], g_sem.at[0])):
                copy.start()

        hidden(i).wait()
        dacc[c] = jnp.where(t == 0, 0.0, dacc[c]) + dot(dhtb[:, sliced(t, span)], ab[lax.rem(i, 2)])

        @pl.when(t == halves - 1)
        def _():
            downs.step1(c)

    for copy in rest:
        copy.wait()
    move(squares1, squares, g_sem.at[1]).wait()

    def put_down(c):
        def put(half, columns, g):
            grads[0, c, half, dm.rows : dm.packed, columns] = g

        return put

    def put_wide(unit):
        def put(half, columns, g):
            grads[0, unit // cuts, half, 0 : dm.rows, pl.ds(pl.multiple_of(lax.rem(unit, cuts) * HALF, HALF), HALF)] = g

        return put

    units = dm.chunks * cuts
    steps = units * halves

    @pl.loop(0, steps)
    def _(i):
        unit, t = i // halves, lax.rem(i, halves)
        slot = lax.rem(i, 2)

        @pl.when(jnp.logical_and(t == 0, unit >= 1))
        def _():
            wides.step1(unit - 1)

        @pl.when(jnp.logical_and(t == 1, unit >= 2))
        def _():
            wides.step2(unit - 2)

        @pl.when(jnp.logical_and(t == 1, unit >= 3))
        def _():
            wides.step3(unit - 3, put_wide(unit - 3), squares)

        @pl.when(i < dm.chunks)
        def _():
            downs.step2(i)

        @pl.when(jnp.logical_and(i >= dm.chunks, i < 2 * dm.chunks))
        def _():
            downs.step3(i - dm.chunks, put_down(i - dm.chunks), squares)

        @pl.when(jnp.logical_and(i >= 1, i + 1 < steps))
        def _():
            for copy in inputs(i + 1):
                copy.start()

        for copy in inputs(i):
            copy.wait()
        weights = wd[unit // cuts, :, pl.ds(pl.multiple_of(lax.rem(unit, cuts) * HALF, HALF), HALF)]
        blocks = [(slice(b, b + SMALL), sliced(t * (span // SMALL) + b // SMALL, SMALL)) for b in range(0, span, SMALL)]
        by_acts = [dot(dhb[tokens, :], weights) for _, tokens in blocks]
        totals = [None, None]
        for (rows, tokens), by_act in zip(blocks, by_acts, strict=True):
            bg[rows, :], bu[rows, :] = back_through(gb[slot, rows, :], ub[slot, rows, :], by_act)
            for which, right in enumerate((bg, bu)):
                term = dot(at[:, tokens], right[rows, :])
                totals[which] = term if totals[which] is None else totals[which] + term
        s = lax.rem(unit, wacc.shape[0])
        for which in range(2):
            wacc[s, which] = jnp.where(t == 0, 0.0, wacc[s, which]) + totals[which]

    last = units - 1
    wides.step1(last)
    wides.step2(last - 1)
    wides.step3(last - 2, put_wide(last - 2), squares)
    wides.step2(last)
    wides.step3(last - 1, put_wide(last - 1), squares)
    wides.step3(last, put_wide(last), squares)
    move(grads1, grads.at[1], g_sem.at[0]).wait()
    move(grads, grads_out, g_sem.at[2]).start()

    copies = []
    for k in range(1, dm.n):
        to = lax.rem(me + k, dm.n)
        copies.append(remote(squares, everyone.at[me], ssends.at[k - 1], srecvs.at[k - 1], {"dp": to}))
    for copy in copies:
        copy.start()
    everyone[me] = squares[...]
    for copy in copies:
        copy.wait()
    total = everyone[0]
    for k in range(1, dm.n):
        total = total + everyone[k]
    total_out[...] = total
    move(grads, grads_out, g_sem.at[2]).wait()


def optimizer_kernel(dm, total, grads, *refs):
    ins, outs = refs[:9], refs[9:]
    count = dm.layers * 3 * dm.d * dm.ff
    factor = jnp.minimum(1.0, 0.5 * lax.rsqrt(jnp.sum(total[...]) / count + 1e-30))
    layer, q = pl.program_id(0), pl.program_id(1)
    size = dm.d // 2 // dm.n
    wide = [
        jnp.concatenate([grads[layer, c, half, 0 : dm.rows, pl.ds(pl.multiple_of(q * LANES, LANES), LANES)] for c in range(dm.chunks)], axis=1)
        for half in range(2)
    ]
    down = jnp.concatenate(
        [grads[layer, q, half, dm.rows : dm.packed, i * LANES : (i + 1) * LANES] for half in range(2) for i in range(dm.n)], axis=0
    ).T
    for which, g in enumerate((*wide, down)):
        w, m, v = (ins[which + 3 * j][0] for j in range(3))
        g = g.astype(F32) * factor
        w = w.astype(F32)
        m = 0.9 * m + 0.1 * g
        v = 0.95 * v + 0.05 * g * g
        step = m * lax.rsqrt(v + 1e-8) + 0.1 * w
        outs[which][0] = (w - 0.02 * step).astype(BF)
        outs[which + 3][0] = m
        outs[which + 6][0] = v


def step(mesh, x, dy, *arrays):
    weights, m, v = (arrays[i : i + 3] for i in (0, 3, 6))
    x, dy = x[0], dy[0]
    w_gate, w_up, w_down = weights
    n = mesh.shape["dp"]
    dm = Dims(w_gate.shape[0], x.shape[0], x.shape[1], w_gate.shape[2], n)
    tokens, d, chunk, chunks, tiles = dm.tokens, dm.d, dm.chunk, dm.chunks, dm.tiles
    hbm = pl.BlockSpec(memory_space=pltpu.HBM)
    vmem = pl.BlockSpec(memory_space=pltpu.VMEM)
    shape = jax.ShapeDtypeStruct
    dma = lambda *s: pltpu.SemaphoreType.DMA(s)
    params = lambda i: pltpu.CompilerParams(vmem_limit_bytes=VMEM_LIMIT, collective_id=i, has_side_effects=True)
    natural, turned = (tokens, d), (d, tokens)

    extra = 2
    units = chunks + extra
    per_chunk = (chunks, tokens, chunk)
    gates, ups, acts, a1, a1t, h1t, a0t, dyt, wd0, w1 = pl.pallas_call(
        functools.partial(forward_kernel, dm, extra),
        out_shape=[
            shape(per_chunk, F32), shape(per_chunk, F32), shape(per_chunk, BF), shape(natural, BF), shape(turned, BF), shape(turned, BF),
            shape(turned, BF), shape(turned, BF), shape((chunks, d, chunk), BF), shape((extra, 3, d, chunk), BF),
        ],
        in_specs=[hbm] * 5,
        out_specs=[hbm] * 10,
        scratch_shapes=[
            pltpu.VMEM(natural, BF), pltpu.VMEM(turned, BF), pltpu.VMEM(turned, BF), pltpu.VMEM(turned, F32),
            pltpu.VMEM((units, 3, d, chunk), BF), pltpu.VMEM((2, TILE, chunk), F32), pltpu.VMEM((2, TILE, chunk), F32), pltpu.VMEM((2, TILE, chunk), BF),
            pltpu.VMEM((2, dm.own_ff, d), BF), pltpu.VMEM(natural, BF), pltpu.VMEM(turned, BF),
            dma(units), dma(2), dma(dm.small), dma(dm.small), dma(1), dma(3, 2), dma(1), dma(3, tiles), dma(2),
            dma(units, Gather.COPIES), dma(units, Gather.COPIES),
        ],
        compiler_params=params(0),
        name="forward",
    )(x, dy, w_gate, w_up, w_down)

    block = (dm.packed, chunk)
    wide, thin, down = (dm.rows, chunk), (dm.rows, HALF), (dm.packed - dm.rows, chunk)
    grads1, squares1, dh, dht, _, _ = pl.pallas_call(
        functools.partial(backward1_kernel, dm),
        out_shape=[
            shape((chunks, 2, *block), BF), shape((8, LANES), F32), shape(natural, BF), shape(turned, BF), shape(per_chunk, BF), shape(per_chunk, BF),
        ],
        in_specs=[hbm] * 9,
        out_specs=[hbm] * 6,
        scratch_shapes=[
            pltpu.VMEM(natural, BF), pltpu.VMEM(turned, BF), pltpu.VMEM(natural, BF), pltpu.VMEM(turned, BF),
            pltpu.VMEM((chunks, 3, d, chunk), BF), pltpu.VMEM((dm.own_ff, d), BF), pltpu.VMEM((2, 2, d, chunk), F32), pltpu.VMEM((2, d, chunk), F32),
            pltpu.VMEM((TILE, chunk), BF), pltpu.VMEM((2, TILE, chunk), BF), pltpu.VMEM((2, TILE, chunk), BF),
            pltpu.VMEM((d, SMALL), BF), pltpu.VMEM((3, d, SMALL), BF), pltpu.VMEM((2, SMALL, d), BF), pltpu.VMEM((2, d, SMALL), BF),
            pltpu.VMEM((1, 6, *wide), BF), pltpu.VMEM((2, 6, *wide), BF), pltpu.VMEM((1, 6, *down), BF), pltpu.VMEM((2, 6, *down), BF),
            pltpu.VMEM((chunks, 2, *block), BF), pltpu.VMEM((8, LANES), F32),
            dma(chunks), dma(1), dma(extra), dma(4, tiles), dma(2, 2), dma(2, 2, chunks), dma(3), dma(2, 2), dma(2),
            dma(chunks, Gather.COPIES), dma(chunks, Gather.COPIES), dma(1, 6), dma(2, 6), dma(1, 6), dma(2, 6),
        ],
        compiler_params=params(1),
        name="backward1",
    )(a1, a1t, dy, dyt, h1t, w_gate, w_up, w_down, w1)

    grads, total = pl.pallas_call(
        functools.partial(backward0_kernel, dm),
        out_shape=[shape((2, chunks, 2, *block), BF), shape((8, LANES), F32)],
        in_specs=[hbm] * 9,
        out_specs=[hbm, vmem],
        scratch_shapes=[
            pltpu.VMEM(natural, BF), pltpu.VMEM(turned, BF), pltpu.VMEM(turned, BF), pltpu.VMEM((chunks, d, chunk), BF),
            pltpu.VMEM((2, tokens // 2, chunk), BF), pltpu.VMEM((2, tokens // 2, HALF), F32), pltpu.VMEM((2, tokens // 2, HALF), F32),
            pltpu.VMEM((tokens // 2, HALF), BF), pltpu.VMEM((tokens // 2, HALF), BF), pltpu.VMEM((4, 2, d, HALF), F32), pltpu.VMEM((chunks, d, chunk), F32),
            pltpu.VMEM((3, 6, *thin), BF), pltpu.VMEM((5, 6, *thin), BF), pltpu.VMEM((chunks, 6, *down), BF), pltpu.VMEM((chunks, 6, *down), BF),
            pltpu.VMEM((2, chunks, 2, *block), BF), pltpu.VMEM((8, LANES), F32), pltpu.VMEM((n, 8, LANES), F32),
            dma(4), dma(1), dma(2), dma(2, 2), dma(3), dma(3, 6), dma(5, 6), dma(chunks, 6), dma(chunks, 6), dma(n - 1), dma(n - 1),
        ],
        compiler_params=params(2),
        name="backward0",
    )(dh, dht, a0t, gates, ups, acts, wd0, grads1, squares1)

    wide = pl.BlockSpec((1, dm.rows, chunks * LANES), lambda l, q: (l, 0, q))
    down = pl.BlockSpec((1, LANES, d), lambda l, q: (l, q, 0))
    whole = lambda s: pl.BlockSpec(s, lambda l, q: (0,) * len(s))
    return tuple(
        pl.pallas_call(
            functools.partial(optimizer_kernel, dm),
            out_shape=[shape(w.shape, BF) for w in weights] + [shape(w.shape, F32) for w in weights] * 2,
            grid=(dm.layers, dm.n),
            in_specs=[whole((8, LANES)), whole((2, chunks, 2, *block))] + [wide, wide, down] * 3,
            out_specs=[wide, wide, down] * 3,
            compiler_params=pltpu.CompilerParams(dimension_semantics=("arbitrary", "arbitrary")),
            name="optimizer",
        )(total, grads, *weights, *m, *v)
    )


def solution(mesh):
    states, cut = P(("rep", "dp"), None, None), P(None, "dp", None)
    return jax.shard_map(
        functools.partial(step, mesh),
        mesh=mesh,
        in_specs=(states, states) + (cut,) * 9,
        out_specs=(P("rep", "dp", None),) * 9,
        check_vma=False,
    )
```

```python
import dataclasses
import functools

import jax
import jax.numpy as jnp
from jax import lax
from jax.experimental import pallas as pl
from jax.experimental.pallas import tpu as pltpu
from jax.sharding import PartitionSpec as P

BF, F32 = jnp.bfloat16, jnp.float32
LANES = 128
TILE = 1024
SMALL = 512
HALF = 256
ROWS = 512
CUT_TILE = 1024
VMEM_LIMIT = 67043328
NT = (((1,), (1,)), ((), ()))
NN = (((1,), (0,)), ((), ()))


@dataclasses.dataclass(frozen=True)
class Dims:
    layers: int
    tokens: int
    d: int
    ff: int
    n: int

    @property
    def own_ff(self):
        return self.ff // self.n

    @property
    def rows(self):
        return self.d // self.n

    @property
    def chunk(self):
        return self.n * LANES

    @property
    def chunks(self):
        return self.own_ff // LANES

    @property
    def tiles(self):
        return self.tokens // TILE

    @property
    def small(self):
        return self.tokens // SMALL

    @property
    def packed(self):
        return self.rows + self.d // 2 // self.n


def dot(a, b, dims=NN):
    return lax.dot_general(a, b, dims, preferred_element_type=F32)


def sliced(i, size):
    return pl.ds(pl.multiple_of(i * size, size), size)


def ring(n):
    me = lax.axis_index("dp")
    return me, lax.rem(me + 1, n), lax.rem(me + n - 1, n)


def partner():
    rep = lax.axis_index("rep")
    core = lax.rem(rep, 2)
    return core, rep + 1 - 2 * core


def greet(*others):
    for other in others:
        pl.semaphore_signal(pltpu.get_barrier_semaphore(), inc=1, device_id=other, device_id_type=pl.DeviceIdType.MESH)


def greeted(count):
    pl.semaphore_wait(pltpu.get_barrier_semaphore(), count)


def remote(src, dst, send, recv, device):
    return pltpu.make_async_remote_copy(src_ref=src, dst_ref=dst, send_sem=send, recv_sem=recv, device_id=device, device_id_type=pl.DeviceIdType.MESH)


def scale_of(wide, axis, count):
    return lax.rsqrt(jnp.sum(wide * wide, axis, keepdims=True) / count + 1e-6)


def move(src, dst, sem):
    return pltpu.make_async_copy(src, dst, sem)


class Gather:
    COPIES = 14

    def __init__(self, dm, w, sends, recvs):
        self.dm, self.w, self.sends, self.recvs = dm, w, sends, recvs
        self.me, self.right, self.left = ring(dm.n)
        self.far = lax.rem(self.me + 2, dm.n)
        self.core, self.other = partner()

    def slot(self, unit):
        return lax.rem(unit, self.w.shape[0])

    def _both(self, unit, source):
        half = self.dm.rows // 2
        at = pl.multiple_of(source * self.dm.rows + self.core * half, half)
        return self.w.at[self.slot(unit), 0:2, pl.ds(at, half), :]

    def _one(self, unit, which, source):
        half = self.dm.rows // 2
        at = pl.multiple_of(source * self.dm.rows + self.core * half, half)
        return self.w.at[self.slot(unit), which, pl.ds(at, half), :]

    def _down(self, unit, source, quarter=None):
        half = self.dm.d // 2
        columns = pl.ds(pl.multiple_of(source * LANES, LANES), LANES)
        if quarter is None:
            return self.w.at[self.slot(unit), 2, pl.ds(pl.multiple_of(self.core * half, half), half), columns]
        return self.w.at[self.slot(unit), 2, pl.ds(pl.multiple_of(self.core * half + quarter * (half // 2), half // 2), half // 2), columns]

    def _copy(self, unit, index, ref, device):
        return remote(ref, ref, self.sends.at[unit, index], self.recvs.at[unit, index], device)

    def own(self, unit, part):
        ref = self._down(unit, self.me) if part else self._both(unit, self.me)
        return [self._copy(unit, 2 * to + part, ref, device) for to, device in enumerate(({"dp": self.right}, {"dp": self.left}))]

    def relayed(self, unit, part):
        if part:
            right, left = self._down(unit, self.left, 0), self._down(unit, self.right, 1)
        else:
            right, left = self._one(unit, 0, self.left), self._one(unit, 1, self.right)
        return [self._copy(unit, 4 + part, right, {"dp": self.right}), self._copy(unit, 6 + part, left, {"dp": self.left})]

    def shared(self, unit, part, sources):
        out = []
        for s in sources:
            source = (self.left, self.right, self.far)[s]
            ref = self._down(unit, source) if part else self._both(unit, source)
            out.append(self._copy(unit, 8 + 2 * s + part, ref, {"rep": self.other}))
        return out

    def _arrivals(self, unit, index, ref):
        return remote(ref, ref, self.sends.at[unit, index], self.recvs.at[unit, index], {"dp": self.right})

    def step1(self, unit, parts=(0, 1)):
        for part in parts:
            for copy in self.own(unit, part):
                copy.start()

    def step2(self, unit):
        for part in range(2):
            for to, source in enumerate((self.left, self.right)):
                ref = self._down(unit, source) if part else self._both(unit, source)
                self._arrivals(unit, 2 * to + part, ref).wait_recv()
            for copy in self.relayed(unit, part) + self.shared(unit, part, (0, 1)):
                copy.start()

    def step3(self, unit):
        for part in range(2):
            for k in range(2):
                ref = self._down(unit, self.far, k) if part else self._one(unit, k, self.far)
                self._arrivals(unit, 4 + 2 * k + part, ref).wait_recv()
            for copy in self.shared(unit, part, (2,)):
                copy.start()

    def _theirs(self, unit, s):
        dm, other = self.dm, 1 - self.core
        source = (self.left, self.right, self.far)[s]
        half = dm.rows // 2
        at = pl.multiple_of(source * dm.rows + other * half, half)
        columns = pl.ds(pl.multiple_of(source * LANES, LANES), LANES)
        rows = pl.ds(pl.multiple_of(other * (dm.d // 2), dm.d // 2), dm.d // 2)
        return self.w.at[self.slot(unit), 0:2, pl.ds(at, half), :], self.w.at[self.slot(unit), 2, rows, columns]

    def done(self, unit):
        for s in range(3):
            both, down = self._theirs(unit, s)
            self._arrivals(unit, 8 + 2 * s, both).wait_recv()
            self._arrivals(unit, 9 + 2 * s, down).wait_recv()

    def drain(self, unit):
        for part in range(2):
            for copy in self.own(unit, part) + self.relayed(unit, part) + self.shared(unit, part, (0, 1, 2)):
                copy.wait_send()

    def fetch(self, unit, sources, sem):
        dm = self.dm
        layer, chunk = unit // dm.chunks, lax.rem(unit, dm.chunks)
        for which in range(2):
            for q in range(dm.n):
                columns = pl.ds(pl.multiple_of(q * dm.own_ff + chunk * LANES, LANES), LANES)
                to = self.w.at[self.slot(unit), which, sliced(self.me, dm.rows), q * LANES : (q + 1) * LANES]
                move(sources[which].at[layer, :, columns], to, sem.at[unit]).start()

    def fetched(self, unit, sem):
        ref = self.w.at[self.slot(unit), 0:2, sliced(self.me, self.dm.rows), :]
        move(ref, ref, sem.at[unit]).wait()

    def turn(self, unit, natural):
        columns = pl.ds(pl.multiple_of(self.me * LANES, LANES), LANES)
        self.w[self.slot(unit), 2, :, columns] = natural[sliced(lax.rem(unit, self.dm.chunks), LANES), :].T


class Scatter:
    def __init__(self, dm, wide, term, place, slots, send, recv, sends, recvs):
        self.dm, self.wide, self.term, self.place, self.slots = dm, wide, term, place, slots
        self.send, self.recv, self.sends, self.recvs = send, recv, sends, recvs
        self.me, self.right, self.left = ring(dm.n)
        self.far = lax.rem(self.me + 2, dm.n)

    def _copy(self, c, kind):
        device = {"dp": self.right if kind % 2 == 0 else self.left}
        slot = lax.rem(c, self.slots)
        return remote(self.place(self.send, c, kind), self.place(self.recv, c, kind), self.sends.at[slot, kind], self.recvs.at[slot, kind], device)

    def _parts(self, c, owner, half):
        dm = self.dm
        if self.wide:
            return [(self.term(c, half)[sliced(owner, dm.rows), :], slice(None))]
        columns = pl.ds(pl.multiple_of(owner * LANES, LANES), LANES)
        size = dm.d // 2 // dm.n
        own = self.term(c, half).at[:, columns]
        return [(own[pl.ds(half * (dm.d // 2) + i * size, size), :], slice(i * LANES, (i + 1) * LANES)) for i in range(dm.n)]

    def _put(self, c, kind, owner, half, add=None):
        to = self.place(self.send, c, kind)
        for term, columns in self._parts(c, owner, half):
            if add is not None:
                term = term + self.place(self.recv, c, add)[:, columns].astype(F32)
            to[:, columns] = term.astype(BF)
        self._copy(c, kind).start()

    def step1(self, c):
        self._put(c, 0, self.far, 0)
        self._put(c, 1, self.far, 1)
        self._put(c, 2, self.right, 1)
        self._put(c, 3, self.left, 0)

    def step2(self, c):
        for kind, owner, half in ((0, self.right, 0), (1, self.left, 1)):
            self._copy(c, kind).wait_recv()
            self._put(c, kind + 4, owner, half, add=kind)
        for kind in (0, 1):
            self._copy(c, kind).wait_send()

    def step3(self, c, put, squares):
        for kind in (2, 3, 4, 5):
            self._copy(c, kind).wait_recv()
        for half, kinds in ((0, (4, 3)), (1, (2, 5))):
            for term, columns in self._parts(c, self.me, half):
                for kind in kinds:
                    term = term + self.place(self.recv, c, kind)[:, columns].astype(F32)
                g = term.astype(BF)
                put(half, columns, g)
                g = g.astype(F32)
                g = jnp.sum((g * g).reshape(-1, 8, g.shape[-1]), 0)
                for j in range(0, g.shape[-1], LANES):
                    squares[...] += g[:, j : j + LANES]
        for kind in (2, 3, 4, 5):
            self._copy(c, kind).wait_send()


def back_through(gate, up, by_act):
    by_act = by_act.astype(BF).astype(F32)
    s = jax.nn.sigmoid(gate)
    by_up = (by_act * (gate * s)).astype(BF)
    by_gate = (by_act * up * (s * (1.0 + gate * (1.0 - s)))).astype(BF)
    return by_gate, by_up


def hidden_of(gate, up):
    return (gate * jax.nn.sigmoid(gate) * up).astype(BF)


def add_to(ref, first, term):
    ref[...] = jnp.where(first, 0.0, ref[...]) + term


def whole_kernel(
    dm, x, dy, w_gate, w_up, w_down,
    grads_out, total_out, gates, ups, acts, a0t, wd0, by_gates, by_ups,
    abuf, at, xt, dyb, dytb, big, w, natural, wsend, wrecv, dsend, drecv, squares, everyone,
    own_sem, nat_sem, x_sem, dy_sem, st_sem, by_sem, in_sem, gu_sem, ab_sem, misc_sem, g_sem, ready,
    gsends, grecvs, wsends, wrecvs, dsends, drecvs, ssends, srecvs,
):
    chunks, tiles, small, units = dm.chunks, dm.tiles, dm.small, dm.layers * dm.chunks
    steps = chunks * tiles
    gather = Gather(dm, w, gsends, grecvs)
    me, left, right, far = gather.me, gather.left, gather.right, gather.far
    sources = (w_gate, w_up)
    big_block = lambda i, width: big.at[:, pl.ds(pl.multiple_of(i * width, width), width)]
    saved = [move(w.at[c, 2], wd0.at[c], misc_sem.at[c]) for c in range(chunks - 1)]
    at_last = [move(wd0.at[c], w.at[chunks - 1, c], misc_sem.at[3 + c]) for c in range(chunks - 2)]
    at_end = move(wd0.at[chunks - 2], w.at[chunks, 0], misc_sem.at[5])
    a0t_out, a0t_back = move(at, a0t, misc_sem.at[6]), move(a0t, at, misc_sem.at[7])
    rest = dm.tokens // 2
    dy_back = move(dy.at[rest:, :], dyb.at[rest:, :], misc_sem.at[8])

    greet({"dp": right}, {"dp": left}, {"rep": gather.other}, {"dp": far})
    gather.fetch(0, sources, own_sem)
    move(w_down.at[0], natural, nat_sem.at[0]).start()
    for t in range(small):
        move(x.at[pl.ds(t * SMALL, SMALL), :], abuf.at[pl.ds(t * SMALL, SMALL), :], x_sem.at[t]).start()
    gather.fetched(0, own_sem)
    greeted(4)
    gather.step1(0, (0,))
    move(w_down.at[0], natural, nat_sem.at[0]).wait()
    gather.turn(0, natural)
    gather.step1(0, (1,))
    for u in range(1, chunks + 1):
        gather.fetch(u, sources, own_sem)
    for t in range(small):
        move(dy.at[pl.ds(t * SMALL, SMALL), :], dyb.at[pl.ds(t * SMALL, SMALL), :], dy_sem.at[t]).start()

    @pl.loop(0, 2 * small)
    def _(t):
        @pl.when(lax.rem(t, 2) == 0)
        def _():
            ref = abuf.at[sliced(t // 2, SMALL), :]
            move(ref, ref, x_sem.at[t // 2]).wait()

        at_t = sliced(t, HALF)
        tile = abuf[at_t, :]
        wide = tile.astype(F32)
        a = (wide * scale_of(wide, -1, dm.d)).astype(BF)
        xt[:, at_t] = tile.T
        at[:, at_t] = a.T
        abuf[at_t, :] = a

    gather.step2(0)

    @pl.loop(1, chunks)
    def _(u):
        gather.turn(u, natural)

    move(w_down.at[1], natural, nat_sem.at[1]).start()
    gather.fetched(1, own_sem)
    gather.step1(1)
    a0t_out.start()

    @pl.loop(0, small)
    def _(t):
        at_t = sliced(t, SMALL)
        move(dy.at[at_t, :], dyb.at[at_t, :], dy_sem.at[t]).wait()
        dytb[:, at_t] = dyb[at_t, :].T

    squares[...] = jnp.zeros_like(squares)
    move(w_down.at[1], natural, nat_sem.at[1]).wait()
    gather.turn(chunks, natural)
    gather.step3(0)

    def forward(gst, ust):
        def ast(slot):
            return dyb.at[pl.ds(pl.multiple_of(rest + slot * TILE, TILE), TILE), 0 : dm.chunk]

        def stored(i):
            slot, chunk, at_t = lax.rem(i, 2), i // tiles, sliced(lax.rem(i, tiles), TILE)
            pairs = ((gst.at[slot], gates), (ust.at[slot], ups), (ast(slot), acts))
            return [move(a, b.at[chunk, at_t, :], st_sem.at[k, slot]) for k, (a, b) in enumerate(pairs)]

        def tile_step(i, last):
            c, t = i // tiles, lax.rem(i, tiles)
            slot, at_t = lax.rem(i, 2), sliced(t, TILE)

            @pl.when(t == 0)
            def _():
                gather.done(c)

            if not last:
                for k in range(chunks - 1):

                    @pl.when(i == k * tiles)
                    def _():
                        saved[k].start()

                    @pl.when(i == k * tiles + 3)
                    def _():
                        saved[k].wait()

            @pl.when(t == 1)
            def _():
                gather.step2(c + 1)

            if not last:

                @pl.when(i == tiles + 1)
                def _():
                    gather.drain(0)
                    gather.fetch(chunks + 1, sources, own_sem)
                    gather.turn(chunks + 1, natural)

                @pl.when(t == 1)
                def _():
                    gather.fetched(c + 2, own_sem)
                    gather.step1(c + 2)

                @pl.when(i == 2 * tiles + 3)
                def _():
                    gather.drain(1)
                    gather.fetch(chunks + 2, sources, own_sem)
                    gather.turn(chunks + 2, natural)
                    gather.fetched(chunks + 1, own_sem)
                    gather.step1(chunks + 1)

            else:

                @pl.when(t == 1)
                def _():
                    gather.drain(2)
                    gather.fetch(chunks + 3, sources, own_sem)
                    gather.turn(chunks + 3, natural)

                @pl.when(t == 2)
                def _():
                    gather.step2(c + 2)

            @pl.when(t == 3)
            def _():
                gather.step3(c + 1)

            @pl.when(i >= 1)
            def _():
                for copy in stored(i - 1):
                    copy.start()

            @pl.when(i >= 2)
            def _():
                for copy in stored(i - 2):
                    copy.wait()

            hidden = ast(slot)
            for r in range(0, TILE, SMALL):
                a, rows = abuf[sliced(t * (TILE // SMALL) + r // SMALL, SMALL), :], slice(r, r + SMALL)
                for b in range(0, dm.chunk, HALF):
                    part = slice(b, b + HALF)
                    gate = dot(a, w[c, 0, :, part])
                    up = dot(a, w[c, 1, :, part])
                    gst[slot, rows, part] = gate
                    ust[slot, rows, part] = up
                    hidden[rows, part] = hidden_of(gate, up)
            if not last:
                add_to(big.at[:, at_t], c == 0, dot(w[c, 2], hidden[...], NT))
                return
            for b in range(0, TILE, HALF):
                at_b = pl.ds(pl.multiple_of(t * TILE + b, HALF), HALF)
                total = big[:, at_b] + dot(w[c, 2], hidden[b : b + HALF, :], NT)
                h = xt[:, at_b] + total.astype(BF)
                wide = h.astype(F32)
                a = (wide * scale_of(wide, 0, dm.d)).astype(BF)
                xt[:, at_b] = h
                at[:, at_b] = a
                abuf[at_b, :] = a.T

        @pl.loop(0, steps - tiles)
        def _(i):
            tile_step(i, False)

        a0t_out.wait()

        @pl.loop(steps - tiles, steps)
        def _(i):
            tile_step(i, True)

        for copy in stored(steps - 1):
            copy.start()
        gather.step3(chunks + 1)
        gather.fetched(chunks + 2, own_sem)
        gather.step1(chunks + 2)
        gather.drain(chunks - 1)
        for copy in at_last:
            copy.start()
        for i in range(steps - 2, steps):
            for copy in stored(i):
                copy.wait()

    pl.run_scoped(forward, pltpu.VMEM((2, TILE, dm.chunk), F32), pltpu.VMEM((2, TILE, dm.chunk), F32))

    def full(buffer, c, kind):
        return buffer.at[lax.rem(c, buffer.shape[0]), kind]

    def pair(buffer, c, kind):
        return buffer.at[lax.rem(c, 2), kind]

    def cut(buffer, c, kind):
        slot = lax.rem(c, 4)
        return buffer.at[slot // 2, kind, :, pl.ds(pl.multiple_of(lax.rem(slot, 2) * HALF, HALF), HALF)]

    def backward1(ba, bg, bu, stash, grads):
        wides = Scatter(
            dm, True, lambda c, half: big_block(2 * lax.rem(c, 2) + half, dm.chunk), pair, 2, wsend, wrecv, wsends, wrecvs
        )
        downs = Scatter(dm, False, lambda c, half: big_block(4 + lax.rem(c, 2), dm.chunk), pair, 2, dsend, drecv, dsends, drecvs)

        def stored(i):
            slot, chunk, at_t = lax.rem(i, 2), i // tiles, sliced(lax.rem(i, tiles), TILE)
            return [move(a.at[slot], b.at[chunk, at_t, :], by_sem.at[k, slot]) for k, (a, b) in enumerate(((bg, by_gates), (bu, by_ups)))]

        def step1(c):
            wides.step1(c)
            downs.step1(c)

        def step2(c):
            wides.step2(c)
            downs.step2(c)

        out = lambda c: move(grads.at[lax.rem(c, 2)], grads_out.at[1, c], g_sem.at[1 + lax.rem(c, 2)])

        def step3(c, again):
            if again is True:
                out(c - 2).wait()

            def put(first, last):
                def put(half, columns, g):
                    grads[lax.rem(c, 2), half * dm.packed + first : half * dm.packed + last, columns] = g

                return put

            wides.step3(c, put(0, dm.rows), squares)
            downs.step3(c, put(dm.rows, dm.packed), squares)
            out(c).start()

        def gate_tile(slot, c):
            return at.at[0:SMALL, pl.ds(pl.multiple_of((slot * chunks + c) * dm.chunk, dm.chunk), dm.chunk)]

        def up_tile(slot, c):
            return dyb.at[sliced(slot * chunks + c, SMALL), 0 : dm.chunk]

        def inputs(t):
            slot, at_t = lax.rem(t, 2), sliced(t, SMALL)
            return [
                move(src.at[c, at_t, :], tile(slot, c), in_sem.at[k, slot, c])
                for k, (src, tile) in enumerate(((by_gates, gate_tile), (by_ups, up_tile)))
                for c in range(chunks)
            ]

        @pl.loop(0, steps)
        def _(i):
            c, t = i // tiles, lax.rem(i, tiles)
            slot, at_t = lax.rem(i, 2), sliced(t, TILE)

            @pl.when(t == 0)
            def _():
                gather.done(chunks + c)

            @pl.when(i == 0)
            def _():
                dy_back.start()

            @pl.when(i == 2)
            def _():
                dy_back.wait()

            @pl.when(jnp.logical_and(t == 0, c >= 2))
            def _():
                step3(c - 2, False)

            @pl.when(jnp.logical_and(t == 0, c >= 1))
            def _():
                step1(c - 1)

            @pl.when(i == 2)
            def _():
                gather.step2(units - 2)
                gather.fetched(units - 1, own_sem)
                gather.step1(units - 1)

            @pl.when(i == 3)
            def _():
                gather.step3(units - 2)

            @pl.when(i == 5)
            def _():
                gather.step2(units - 1)

            @pl.when(i == 7)
            def _():
                gather.step3(units - 1)

            @pl.when(jnp.logical_and(t == 2, c >= 1))
            def _():
                step2(c - 1)

            @pl.when(i >= 1)
            def _():
                for copy in stored(i - 1):
                    copy.start()

            @pl.when(i >= 2)
            def _():
                for copy in stored(i - 2):
                    copy.wait()

            @pl.when(i == steps - 1)
            def _():
                for copy in inputs(0):
                    copy.start()

            s = gather.slot(chunks + c)
            for r in range(0, TILE, ROWS):
                tokens, rows = sliced(t * (TILE // ROWS) + r // ROWS, ROWS), slice(r, r + ROWS)
                a, y = abuf[tokens, :], dyb[tokens, :]
                for b in range(0, dm.chunk, HALF):
                    part = slice(b, b + HALF)
                    gate, up = dot(a, w[s, 0, :, part]), dot(a, w[s, 1, :, part])
                    by_gate, by_up = back_through(gate, up, dot(y, w[s, 2, :, part]))
                    ba[rows, part] = hidden_of(gate, up)
                    bg[slot, rows, part] = by_gate
                    bu[slot, rows, part] = by_up
            add_to(wides.term(c, 0), t == 0, dot(at[:, at_t], bg[slot]))
            add_to(wides.term(c, 1), t == 0, dot(at[:, at_t], bu[slot]))
            add_to(downs.term(c, 0), t == 0, dot(dytb[:, at_t], ba[...]))

        last = chunks - 1
        for copy in stored(steps - 1):
            copy.start()
        step3(last - 1, True)
        step1(last)
        for i in range(steps - 2, steps):
            for copy in stored(i):
                copy.wait()

        def matmuls(t):
            slot, total = lax.rem(t, 2), None
            for c in range(chunks):
                s = (chunks + c) % (chunks + 1)
                term = dot(w[s, 0], gate_tile(slot, c)[...], NT) + dot(w[s, 1], up_tile(slot, c)[...], NT)
                total = term if total is None else total + term
            return total.astype(BF)

        def finish(t):
            for k in range(0, SMALL, LANES):
                at_k = sliced(t * (SMALL // LANES) + k // LANES, LANES)
                by_a = stash[:, k : k + LANES].astype(F32)
                h = xt[:, at_k].astype(F32)
                square = jnp.sum(h * h, 0, keepdims=True) / dm.d + 1e-6
                scale = lax.rsqrt(square)
                along = jnp.sum(h * by_a, 0, keepdims=True) * (scale / square) / dm.d
                by_h = dytb[:, at_k] + (by_a * scale - h * along).astype(BF)
                dytb[:, at_k] = by_h
                abuf[at_k, :] = by_h.T

        for copy in inputs(1):
            copy.start()
        for copy in inputs(0):
            copy.wait()
        stash[...] = matmuls(0)

        @pl.loop(1, small)
        def _(t):
            @pl.when(t == 3)
            def _():
                step2(last)

            @pl.when(t == 6)
            def _():
                step3(last, True)
                for neighbour in (left, right):
                    pl.semaphore_signal(ready, inc=1, device_id={"dp": neighbour}, device_id_type=pl.DeviceIdType.MESH)

            for copy in inputs(t):
                copy.wait()

            @pl.when(t + 1 < small)
            def _():
                for copy in inputs(t + 1):
                    copy.start()

            @pl.when(t == small - 1)
            def _():
                hidden(0).start()

            finish(t - 1)
            stash[...] = matmuls(t)

        hidden(1).start()
        a0t_back.start()
        for u in range(chunks, units):
            gather.drain(u)
        at_end.start()
        finish(small - 1)
        for c in (last - 1, last):
            out(c).wait()

    span = dm.tokens // 2

    def hidden_at(i):
        return dyb.at[sliced(lax.rem(i, 2), span), 0 : dm.chunk]

    def hidden(i):
        return move(acts.at[i // 2, sliced(lax.rem(i, 2), span), :], hidden_at(i), ab_sem.at[lax.rem(i, 2)])

    pl.run_scoped(
        backward1,
        pltpu.VMEM((TILE, dm.chunk), BF), pltpu.VMEM((2, TILE, dm.chunk), BF), pltpu.VMEM((2, TILE, dm.chunk), BF), pltpu.VMEM((dm.d, SMALL), BF),
        pltpu.VMEM((2, 2 * dm.packed, dm.chunk), BF),
    )

    def backward0(gb, ub, bg, bu):
        cuts, parts = dm.chunk // HALF, dm.tokens // gb.shape[1]
        wides = Scatter(
            dm, True, lambda u, half: big_block(2 * chunks * cuts // 2 + 2 * lax.rem(u, 4) + half, HALF), cut, 4, wsend, wrecv, wsends, wrecvs
        )
        downs = Scatter(dm, False, lambda c, half: big_block(c, dm.chunk), full, chunks, dsend, drecv, dsends, drecvs)

        def inputs(i):
            slot, unit, at_t = lax.rem(i, 2), i // parts, sliced(lax.rem(i, parts), gb.shape[1])
            columns = pl.ds(pl.multiple_of(lax.rem(unit, cuts) * HALF, HALF), HALF)
            return (
                move(gates.at[unit // cuts, at_t, columns], gb.at[slot], gu_sem.at[0, slot]),
                move(ups.at[unit // cuts, at_t, columns], ub.at[slot], gu_sem.at[1, slot]),
            )

        @pl.loop(0, 2 * chunks)
        def _(i):
            c, t = i // 2, lax.rem(i, 2)

            @pl.when(i == 1)
            def _():
                pl.semaphore_wait(ready, 2)

            @pl.when(jnp.logical_and(i >= 1, i + 1 < 2 * chunks))
            def _():
                hidden(i + 1).start()

            @pl.when(i == 5)
            def _():
                for copy in (*inputs(0), *inputs(1)):
                    copy.start()

            hidden(i).wait()
            add_to(downs.term(c, 0), t == 0, dot(dytb[:, sliced(t, span)], hidden_at(i)[...]))

            @pl.when(t == 1)
            def _():
                downs.step1(c)

        a0t_back.wait()
        at_end.wait()
        for copy in at_last:
            copy.wait()

        def sums(c):
            return w.at[c // 3, lax.rem(c, 3), 0 : 2 * dm.packed, :]

        def put_down(c):
            def put(half, columns, g):
                sums(c)[pl.ds(half * dm.packed + dm.rows, dm.packed - dm.rows), columns] = g

            return put

        def put_wide(unit):
            def put(half, columns, g):
                to = sums(unit // cuts).at[:, pl.ds(pl.multiple_of(lax.rem(unit, cuts) * HALF, HALF), HALF)]
                to[pl.ds(half * dm.packed, dm.rows), :] = g

            return put

        cut_units = chunks * cuts
        first, middle = 0, parts // 2

        @pl.loop(0, cut_units * parts)
        def _(i):
            unit, t, slot = i // parts, lax.rem(i, parts), lax.rem(i, 2)

            @pl.when(jnp.logical_and(t == first, unit >= 1))
            def _():
                wides.step1(unit - 1)

            @pl.when(jnp.logical_and(t == middle, unit >= 3))
            def _():
                wides.step3(unit - 3, put_wide(unit - 3), squares)

            @pl.when(jnp.logical_and(t == middle, unit >= 2))
            def _():
                wides.step2(unit - 2)

            @pl.when(i < chunks)
            def _():
                downs.step2(i)

            @pl.when(jnp.logical_and(i >= 2 * chunks, i < 3 * chunks))
            def _():
                downs.step3(i - 2 * chunks, put_down(i - 2 * chunks), squares)

            @pl.when(jnp.logical_and(i >= 1, i + 1 < cut_units * parts))
            def _():
                for copy in inputs(i + 1):
                    copy.start()

            for copy in inputs(i):
                copy.wait()
            c = unit // cuts
            slot_w, which = chunks - 1 + (c // 2) * (1 - lax.rem(c, 2)), lax.rem(c, 2) * (1 + c // 2)
            weights = w[slot_w, which, :, pl.ds(pl.multiple_of(lax.rem(unit, cuts) * HALF, HALF), HALF)]
            size = gb.shape[1]
            blocks = [(slice(b, b + SMALL), sliced(t * (size // SMALL) + b // SMALL, SMALL)) for b in range(0, size, SMALL)]
            by_acts = [dot(abuf[tokens, :], weights) for _, tokens in blocks]
            totals = [None, None]
            for (rows, tokens), by_act in zip(blocks, by_acts, strict=True):
                bg[rows, :], bu[rows, :] = back_through(gb[slot, rows, :], ub[slot, rows, :], by_act)
                for k, right in enumerate((bg, bu)):
                    term = dot(at[:, tokens], right[rows, :])
                    totals[k] = term if totals[k] is None else totals[k] + term
            for k in range(2):
                add_to(wides.term(unit, k), t == 0, totals[k])

        last = cut_units - 1
        wides.step1(last)
        wides.step2(last - 1)
        wides.step3(last - 2, put_wide(last - 2), squares)
        wides.step2(last)
        wides.step3(last - 1, put_wide(last - 1), squares)
        wides.step3(last, put_wide(last), squares)
        out = [move(sums(c), grads_out.at[0, c], g_sem.at[1 + c]) for c in range(chunks)]
        for copy in out:
            copy.start()
        copies = []
        for k in range(1, dm.n):
            to = lax.rem(me + k, dm.n)
            copies.append(remote(squares, everyone.at[me], ssends.at[k - 1], srecvs.at[k - 1], {"dp": to}))
        for copy in copies:
            copy.start()
        everyone[me] = squares[...]
        for copy in copies:
            copy.wait()
        total = everyone[0]
        for k in range(1, dm.n):
            total = total + everyone[k]
        total_out[...] = total
        for copy in out:
            copy.wait()

    part = CUT_TILE
    pl.run_scoped(
        backward0,
        pltpu.VMEM((2, part, HALF), F32), pltpu.VMEM((2, part, HALF), F32), pltpu.VMEM((part, HALF), BF), pltpu.VMEM((part, HALF), BF),
    )


def optimizer_kernel(dm, total, grads_in, *refs):
    ins, outs, (grads, *buffers), (g_sem, in_sem, out_sem) = refs[:9], refs[9:18], refs[18:25], refs[25:]
    stores = [buffers[0:2], buffers[2:4], buffers[4:6]]
    halves = 2
    pieces = [(layer, which, half) for layer in range(dm.layers) for which in range(3) for half in range(halves)]

    def places(piece):
        layer, which, half = piece
        out = []
        for kind in range(3):
            if which < 2:
                cut = slice(half * dm.ff // halves, (half + 1) * dm.ff // halves)
                here = stores[kind][0].at[2 * layer + which, :, cut]
                out.append((ins[3 * kind + which].at[layer, :, cut], here, outs[3 * kind + which].at[layer, :, cut]))
            else:
                cut = slice(half * dm.own_ff // halves, (half + 1) * dm.own_ff // halves)
                here = stores[kind][1].at[layer, cut, :]
                out.append((ins[3 * kind + which].at[layer, cut, :], here, outs[3 * kind + which].at[layer, cut, :]))
        return out

    fetch = [move(grads_in.at[layer], grads.at[layer], g_sem.at[layer]) for layer in range(dm.layers)]
    loads = [[move(a, b, in_sem.at[k, kind]) for kind, (a, b, _) in enumerate(places(p))] for k, p in enumerate(pieces)]
    writes = [[move(b, c, out_sem.at[k, kind]) for kind, (_, b, c) in enumerate(places(p))] for k, p in enumerate(pieces)]
    for layer in range(dm.layers):
        fetch[layer].start()
        for k, piece in enumerate(pieces):
            if piece[0] == layer:
                for copy in loads[k]:
                    copy.start()
    count = dm.layers * 3 * dm.d * dm.ff
    factor = jnp.minimum(1.0, 0.5 * lax.rsqrt(jnp.sum(total[...]) / count + 1e-30))
    size = dm.d // 2 // dm.n

    def adamw(g, refs, at):
        w, m, v = (ref[at] for ref in refs)
        g = g.astype(F32) * factor
        w = w.astype(F32)
        m = 0.9 * m + 0.1 * g
        v = 0.95 * v + 0.05 * g * g
        change = m * lax.rsqrt(v + 1e-8) + 0.1 * w
        refs[0][at] = (w - 0.02 * change).astype(BF)
        refs[1][at] = m
        refs[2][at] = v

    for k, (layer, which, half) in enumerate(pieces):
        if (which, half) == (0, 0):
            fetch[layer].wait()
        for copy in loads[k]:
            copy.wait()
        refs = [here for _, here, _ in places(pieces[k])]
        if which < 2:
            for b in range(dm.ff // halves // LANES):
                q, c = divmod(half * dm.ff // halves // LANES + b, dm.chunks)
                g = grads[layer, c, which * dm.packed : which * dm.packed + dm.rows, q * LANES : (q + 1) * LANES]
                adamw(g, refs, (slice(None), slice(b * LANES, (b + 1) * LANES)))
        else:
            for b in range(dm.own_ff // halves // LANES):
                c = half * dm.own_ff // halves // LANES + b
                for row in range(2 * dm.n):
                    side, i = divmod(row, dm.n)
                    start = side * dm.packed + dm.rows
                    g = grads[layer, c, start : start + size, i * LANES : (i + 1) * LANES]
                    if row == 0:
                        rows = []
                    rows.append(g)
                adamw(jnp.concatenate(rows, axis=0).T, refs, (slice(b * LANES, (b + 1) * LANES), slice(None)))
        for copy in writes[k]:
            copy.start()
    for copies in writes:
        for copy in copies:
            copy.wait()


def step(mesh, x, dy, *arrays):
    weights, m, v = (arrays[i : i + 3] for i in (0, 3, 6))
    x, dy = x[0], dy[0]
    w_gate, w_up, w_down = weights
    n = mesh.shape["dp"]
    dm = Dims(w_gate.shape[0], x.shape[0], x.shape[1], w_gate.shape[2], n)
    tokens, d, chunk, chunks, tiles = dm.tokens, dm.d, dm.chunk, dm.chunks, dm.tiles
    hbm = pl.BlockSpec(memory_space=pltpu.HBM)
    vmem = pl.BlockSpec(memory_space=pltpu.VMEM)
    shape = jax.ShapeDtypeStruct
    dma = lambda *s: pltpu.SemaphoreType.DMA(s)
    natural, turned, per_chunk = (tokens, d), (d, tokens), (chunks, tokens, chunk)
    block, wide, down = (2 * dm.packed, chunk), (dm.rows, chunk), (dm.packed - dm.rows, chunk)
    units = dm.layers * chunks
    semaphores = [
        dma(units), dma(2), dma(dm.small), dma(dm.small), dma(3, 2), dma(2, 2), dma(2, 2, chunks), dma(2, 2), dma(2), dma(9), dma(1 + chunks),
        pltpu.SemaphoreType.REGULAR,
        dma(units, Gather.COPIES), dma(units, Gather.COPIES), dma(4, 6), dma(4, 6), dma(chunks, 6), dma(chunks, 6), dma(n - 1), dma(n - 1),
    ]

    def kernel(*refs):
        pl.run_scoped(lambda *scoped: whole_kernel(dm, *refs, *scoped), *semaphores)

    grads, total, *_ = pl.pallas_call(
        kernel,
        out_shape=[
            shape((2, chunks, *block), BF), shape((8, LANES), F32), shape(per_chunk, F32), shape(per_chunk, F32), shape(per_chunk, BF),
            shape(turned, BF), shape((chunks - 1, d, chunk), BF), shape(per_chunk, BF), shape(per_chunk, BF),
        ],
        in_specs=[hbm] * 5,
        out_specs=[hbm, vmem] + [hbm] * 7,
        scratch_shapes=[
            pltpu.VMEM(natural, BF), pltpu.VMEM(turned, BF), pltpu.VMEM(turned, BF), pltpu.VMEM(natural, BF), pltpu.VMEM(turned, BF),
            pltpu.VMEM(turned, F32), pltpu.VMEM((chunks + 1, 3, d, chunk), BF), pltpu.VMEM((dm.own_ff, d), BF),
            pltpu.VMEM((2, 6, *wide), BF), pltpu.VMEM((2, 6, *wide), BF), pltpu.VMEM((chunks, 6, *down), BF), pltpu.VMEM((chunks, 6, *down), BF),
            pltpu.VMEM((8, LANES), F32), pltpu.VMEM((n, 8, LANES), F32),
        ],
        compiler_params=pltpu.CompilerParams(vmem_limit_bytes=VMEM_LIMIT, collective_id=0, has_side_effects=True),
        name="whole",
    )(x, dy, w_gate, w_up, w_down)

    wides, downs = (2 * dm.layers, dm.rows, dm.ff), (dm.layers, dm.own_ff, d)
    return tuple(
        pl.pallas_call(
            functools.partial(optimizer_kernel, dm),
            out_shape=[shape(w.shape, BF) for w in weights] + [shape(w.shape, F32) for w in weights] * 2,
            in_specs=[vmem] + [hbm] * 10,
            out_specs=[hbm] * 9,
            scratch_shapes=[
                pltpu.VMEM((2, chunks, *block), BF), pltpu.VMEM(wides, BF), pltpu.VMEM(downs, BF),
                pltpu.VMEM(wides, F32), pltpu.VMEM(downs, F32), pltpu.VMEM(wides, F32), pltpu.VMEM(downs, F32),
                dma(dm.layers), dma(6 * dm.layers, 3), dma(6 * dm.layers, 3),
            ],
            compiler_params=pltpu.CompilerParams(vmem_limit_bytes=VMEM_LIMIT),
            name="optimizer",
        )(total, grads, *weights, *m, *v)
    )


def solution(mesh):
    states, cut = P(("rep", "dp"), None, None), P(None, "dp", None)
    return jax.shard_map(
        functools.partial(step, mesh),
        mesh=mesh,
        in_specs=(states, states) + (cut,) * 9,
        out_specs=(P("rep", "dp", None),) * 9,
        check_vma=False,
    )
```

```python
import dataclasses
import functools

import jax
import jax.numpy as jnp
from jax import lax
from jax.experimental import pallas as pl
from jax.experimental.pallas import tpu as pltpu
from jax.sharding import PartitionSpec as P

BF, F32 = jnp.bfloat16, jnp.float32
LANES = 128
TILE = 1024
SMALL = 512
HALF = 256
ROWS = 1024
PIECE = 512
CUT_TILE = 2048
VMEM_LIMIT = 67043328
NT = (((1,), (1,)), ((), ()))
NN = (((1,), (0,)), ((), ()))


@dataclasses.dataclass(frozen=True)
class Dims:
    layers: int
    tokens: int
    d: int
    ff: int
    n: int

    @property
    def own_ff(self):
        return self.ff // self.n

    @property
    def rows(self):
        return self.d // self.n

    @property
    def chunk(self):
        return self.n * LANES

    @property
    def chunks(self):
        return self.own_ff // LANES

    @property
    def tiles(self):
        return self.tokens // TILE

    @property
    def small(self):
        return self.tokens // SMALL

    @property
    def packed(self):
        return self.rows + self.d // 2 // self.n


def dot(a, b, dims=NN):
    return lax.dot_general(a, b, dims, preferred_element_type=F32)


def sliced(i, size):
    return pl.ds(pl.multiple_of(i * size, size), size)


def ring(n):
    me = lax.axis_index("dp")
    return me, lax.rem(me + 1, n), lax.rem(me + n - 1, n)


def partner():
    rep = lax.axis_index("rep")
    core = lax.rem(rep, 2)
    return core, rep + 1 - 2 * core


def greet(*others):
    for other in others:
        pl.semaphore_signal(pltpu.get_barrier_semaphore(), inc=1, device_id=other, device_id_type=pl.DeviceIdType.MESH)


def greeted(count):
    pl.semaphore_wait(pltpu.get_barrier_semaphore(), count)


def remote(src, dst, send, recv, device):
    return pltpu.make_async_remote_copy(src_ref=src, dst_ref=dst, send_sem=send, recv_sem=recv, device_id=device, device_id_type=pl.DeviceIdType.MESH)


def scale_of(wide, axis, count):
    return lax.rsqrt(jnp.sum(wide * wide, axis, keepdims=True) / count + 1e-6)


def move(src, dst, sem):
    return pltpu.make_async_copy(src, dst, sem)


class Gather:
    COPIES = 14

    def __init__(self, dm, w, sends, recvs):
        self.dm, self.w, self.sends, self.recvs = dm, w, sends, recvs
        self.me, self.right, self.left = ring(dm.n)
        self.far = lax.rem(self.me + 2, dm.n)
        self.core, self.other = partner()

    def slot(self, unit):
        return lax.rem(unit, self.w.shape[0])

    def _both(self, unit, source):
        half = self.dm.rows // 2
        at = pl.multiple_of(source * self.dm.rows + self.core * half, half)
        return self.w.at[self.slot(unit), 0:2, pl.ds(at, half), :]

    def _one(self, unit, which, source):
        half = self.dm.rows // 2
        at = pl.multiple_of(source * self.dm.rows + self.core * half, half)
        return self.w.at[self.slot(unit), which, pl.ds(at, half), :]

    def _down(self, unit, source, quarter=None):
        half = self.dm.d // 2
        columns = pl.ds(pl.multiple_of(source * LANES, LANES), LANES)
        if quarter is None:
            return self.w.at[self.slot(unit), 2, pl.ds(pl.multiple_of(self.core * half, half), half), columns]
        return self.w.at[self.slot(unit), 2, pl.ds(pl.multiple_of(self.core * half + quarter * (half // 2), half // 2), half // 2), columns]

    def _copy(self, unit, index, ref, device):
        return remote(ref, ref, self.sends.at[unit, index], self.recvs.at[unit, index], device)

    def own(self, unit, part):
        ref = self._down(unit, self.me) if part else self._both(unit, self.me)
        return [self._copy(unit, 2 * to + part, ref, device) for to, device in enumerate(({"dp": self.right}, {"dp": self.left}))]

    def relayed(self, unit, part):
        if part:
            right, left = self._down(unit, self.left, 0), self._down(unit, self.right, 1)
        else:
            right, left = self._one(unit, 0, self.left), self._one(unit, 1, self.right)
        return [self._copy(unit, 4 + part, right, {"dp": self.right}), self._copy(unit, 6 + part, left, {"dp": self.left})]

    def shared(self, unit, part, sources):
        out = []
        for s in sources:
            source = (self.left, self.right, self.far)[s]
            ref = self._down(unit, source) if part else self._both(unit, source)
            out.append(self._copy(unit, 8 + 2 * s + part, ref, {"rep": self.other}))
        return out

    def _arrivals(self, unit, index, ref):
        return remote(ref, ref, self.sends.at[unit, index], self.recvs.at[unit, index], {"dp": self.right})

    def step1(self, unit, parts=(0, 1)):
        for part in parts:
            for copy in self.own(unit, part):
                copy.start()

    def step2(self, unit):
        for part in range(2):
            for to, source in enumerate((self.left, self.right)):
                ref = self._down(unit, source) if part else self._both(unit, source)
                self._arrivals(unit, 2 * to + part, ref).wait_recv()
            for copy in self.relayed(unit, part) + self.shared(unit, part, (0, 1)):
                copy.start()

    def step3(self, unit):
        for part in range(2):
            for k in range(2):
                ref = self._down(unit, self.far, k) if part else self._one(unit, k, self.far)
                self._arrivals(unit, 4 + 2 * k + part, ref).wait_recv()
            for copy in self.shared(unit, part, (2,)):
                copy.start()

    def _theirs(self, unit, s):
        dm, other = self.dm, 1 - self.core
        source = (self.left, self.right, self.far)[s]
        half = dm.rows // 2
        at = pl.multiple_of(source * dm.rows + other * half, half)
        columns = pl.ds(pl.multiple_of(source * LANES, LANES), LANES)
        rows = pl.ds(pl.multiple_of(other * (dm.d // 2), dm.d // 2), dm.d // 2)
        return self.w.at[self.slot(unit), 0:2, pl.ds(at, half), :], self.w.at[self.slot(unit), 2, rows, columns]

    def done(self, unit):
        for s in range(3):
            both, down = self._theirs(unit, s)
            self._arrivals(unit, 8 + 2 * s, both).wait_recv()
            self._arrivals(unit, 9 + 2 * s, down).wait_recv()

    def drain(self, unit):
        for part in range(2):
            for copy in self.own(unit, part) + self.relayed(unit, part) + self.shared(unit, part, (0, 1, 2)):
                copy.wait_send()

    def fetch(self, unit, sources, sem):
        dm = self.dm
        layer, chunk = unit // dm.chunks, lax.rem(unit, dm.chunks)
        for which in range(2):
            for q in range(dm.n):
                columns = pl.ds(pl.multiple_of(q * dm.own_ff + chunk * LANES, LANES), LANES)
                to = self.w.at[self.slot(unit), which, sliced(self.me, dm.rows), q * LANES : (q + 1) * LANES]
                move(sources[which].at[layer, :, columns], to, sem.at[unit]).start()

    def fetched(self, unit, sem):
        ref = self.w.at[self.slot(unit), 0:2, sliced(self.me, self.dm.rows), :]
        move(ref, ref, sem.at[unit]).wait()

    def turn(self, unit, natural):
        columns = pl.ds(pl.multiple_of(self.me * LANES, LANES), LANES)
        self.w[self.slot(unit), 2, :, columns] = natural[sliced(lax.rem(unit, self.dm.chunks), LANES), :].T


class Scatter:
    def __init__(self, dm, wide, term, place, slots, send, recv, sends, recvs):
        self.dm, self.wide, self.term, self.place, self.slots = dm, wide, term, place, slots
        self.send, self.recv, self.sends, self.recvs = send, recv, sends, recvs
        self.me, self.right, self.left = ring(dm.n)
        self.far = lax.rem(self.me + 2, dm.n)

    def _copy(self, c, kind):
        device = {"dp": self.right if kind % 2 == 0 else self.left}
        slot = lax.rem(c, self.slots)
        return remote(self.place(self.send, c, kind), self.place(self.recv, c, kind), self.sends.at[slot, kind], self.recvs.at[slot, kind], device)

    def _parts(self, c, owner, half):
        dm = self.dm
        if self.wide:
            return [(self.term(c, half)[sliced(owner, dm.rows), :], slice(None))]
        columns = pl.ds(pl.multiple_of(owner * LANES, LANES), LANES)
        size = dm.d // 2 // dm.n
        own = self.term(c, half).at[:, columns]
        return [(own[pl.ds(half * (dm.d // 2) + i * size, size), :], slice(i * LANES, (i + 1) * LANES)) for i in range(dm.n)]

    def _put(self, c, kind, owner, half, add=None):
        to = self.place(self.send, c, kind)
        for term, columns in self._parts(c, owner, half):
            if add is not None:
                term = term + self.place(self.recv, c, add)[:, columns].astype(F32)
            to[:, columns] = term.astype(BF)
        self._copy(c, kind).start()

    def step1(self, c, kinds=(0, 1, 2, 3)):
        for kind in kinds:
            self._put(c, kind, (self.far, self.far, self.right, self.left)[kind], (0, 1, 1, 0)[kind])

    def step2(self, c):
        for kind, owner, half in ((0, self.right, 0), (1, self.left, 1)):
            self._copy(c, kind).wait_recv()
            self._put(c, kind + 4, owner, half, add=kind)
        for kind in (0, 1):
            self._copy(c, kind).wait_send()

    def step3(self, c, put, squares):
        for kind in (2, 3, 4, 5):
            self._copy(c, kind).wait_recv()
        for half, kinds in ((0, (4, 3)), (1, (2, 5))):
            for term, columns in self._parts(c, self.me, half):
                for kind in kinds:
                    term = term + self.place(self.recv, c, kind)[:, columns].astype(F32)
                g = term.astype(BF)
                put(half, columns, g)
                g = g.astype(F32)
                g = jnp.sum((g * g).reshape(-1, 8, g.shape[-1]), 0)
                for j in range(0, g.shape[-1], LANES):
                    squares[...] += g[:, j : j + LANES]
        for kind in (2, 3, 4, 5):
            self._copy(c, kind).wait_send()


def back_through(gate, up, by_act):
    by_act = by_act.astype(BF).astype(F32)
    s = jax.nn.sigmoid(gate)
    by_up = (by_act * (gate * s)).astype(BF)
    by_gate = (by_act * up * (s * (1.0 + gate * (1.0 - s)))).astype(BF)
    return by_gate, by_up


def hidden_of(gate, up):
    return (gate * jax.nn.sigmoid(gate) * up).astype(BF)


def add_to(ref, first, term):
    ref[...] = jnp.where(first, 0.0, ref[...]) + term


def whole_kernel(
    dm, x, dy, w_gate, w_up, w_down,
    grads_out, squares_out, gates, ups, acts, a0t, wd0, by_gates, by_ups,
    abuf, at, xt, dyb, dytb, big, w, natural, wsend, wrecv, dsend, drecv, squares,
    own_sem, nat_sem, x_sem, dy_sem, st_sem, by_sem, in_sem, gu_sem, ab_sem, misc_sem, g_sem, ready,
    gsends, grecvs, wsends, wrecvs, dsends, drecvs, ssends, srecvs,
):
    chunks, tiles, small, units = dm.chunks, dm.tiles, dm.small, dm.layers * dm.chunks
    steps = chunks * tiles
    gather = Gather(dm, w, gsends, grecvs)
    me, left, right, far = gather.me, gather.left, gather.right, gather.far
    sources = (w_gate, w_up)
    big_block = lambda i, width: big.at[:, pl.ds(pl.multiple_of(i * width, width), width)]
    saved = [move(w.at[c, 2], wd0.at[c], misc_sem.at[c]) for c in range(chunks - 1)]
    at_last = [move(wd0.at[c], w.at[chunks - 1, c], misc_sem.at[3 + c]) for c in range(chunks - 2)]
    at_end = move(wd0.at[chunks - 2], w.at[chunks, 0], misc_sem.at[5])
    a0t_out, a0t_back = move(at, a0t, misc_sem.at[6]), move(a0t, at, misc_sem.at[7])
    rest = dm.tokens // 2
    dy_back = move(dy.at[rest:, :], dyb.at[rest:, :], misc_sem.at[8])

    greet({"dp": right}, {"dp": left}, {"rep": gather.other}, {"dp": far})
    gather.fetch(0, sources, own_sem)
    move(w_down.at[0], natural, nat_sem.at[0]).start()
    for t in range(small):
        move(x.at[pl.ds(t * SMALL, SMALL), :], abuf.at[pl.ds(t * SMALL, SMALL), :], x_sem.at[t]).start()
    gather.fetched(0, own_sem)
    greeted(4)
    gather.step1(0, (0,))
    move(w_down.at[0], natural, nat_sem.at[0]).wait()
    gather.turn(0, natural)
    gather.step1(0, (1,))
    for u in range(1, chunks + 1):
        gather.fetch(u, sources, own_sem)
    for t in range(small):
        move(dy.at[pl.ds(t * SMALL, SMALL), :], dyb.at[pl.ds(t * SMALL, SMALL), :], dy_sem.at[t]).start()

    @pl.loop(0, 2 * small)
    def _(t):
        @pl.when(lax.rem(t, 2) == 0)
        def _():
            ref = abuf.at[sliced(t // 2, SMALL), :]
            move(ref, ref, x_sem.at[t // 2]).wait()

        at_t = sliced(t, HALF)
        tile = abuf[at_t, :]
        wide = tile.astype(F32)
        a = (wide * scale_of(wide, -1, dm.d)).astype(BF)
        xt[:, at_t] = tile.T
        at[:, at_t] = a.T
        abuf[at_t, :] = a

    gather.step2(0)

    @pl.loop(1, chunks)
    def _(u):
        gather.turn(u, natural)

    move(w_down.at[1], natural, nat_sem.at[1]).start()
    gather.fetched(1, own_sem)
    gather.step1(1)
    a0t_out.start()

    @pl.loop(0, small)
    def _(t):
        at_t = sliced(t, SMALL)
        move(dy.at[at_t, :], dyb.at[at_t, :], dy_sem.at[t]).wait()
        dytb[:, at_t] = dyb[at_t, :].T

    squares[...] = jnp.zeros_like(squares)
    move(w_down.at[1], natural, nat_sem.at[1]).wait()
    gather.turn(chunks, natural)
    gather.step3(0)

    def forward(gst, ust):
        def ast(slot):
            return dyb.at[pl.ds(pl.multiple_of(rest + slot * TILE, TILE), TILE), 0 : dm.chunk]

        def stored(i):
            slot, chunk, at_t = lax.rem(i, 2), i // tiles, sliced(lax.rem(i, tiles), TILE)
            pairs = ((gst.at[slot], gates), (ust.at[slot], ups), (ast(slot), acts))
            return [move(a, b.at[chunk, at_t, :], st_sem.at[k, slot]) for k, (a, b) in enumerate(pairs)]

        def tile_step(i, last):
            c, t = i // tiles, lax.rem(i, tiles)
            slot, at_t = lax.rem(i, 2), sliced(t, TILE)

            @pl.when(t == 0)
            def _():
                gather.done(c)

            if not last:
                for k in range(chunks - 1):

                    @pl.when(i == k * tiles)
                    def _():
                        saved[k].start()

                    @pl.when(i == k * tiles + 3)
                    def _():
                        saved[k].wait()

            @pl.when(t == 1)
            def _():
                gather.step2(c + 1)

            if not last:

                @pl.when(i == tiles + 1)
                def _():
                    gather.drain(0)
                    gather.fetch(chunks + 1, sources, own_sem)
                    gather.turn(chunks + 1, natural)

                @pl.when(t == 1)
                def _():
                    gather.fetched(c + 2, own_sem)
                    gather.step1(c + 2)

                @pl.when(i == 2 * tiles + 3)
                def _():
                    gather.drain(1)
                    gather.fetch(chunks + 2, sources, own_sem)
                    gather.turn(chunks + 2, natural)
                    gather.fetched(chunks + 1, own_sem)
                    gather.step1(chunks + 1)

            else:

                @pl.when(t == 1)
                def _():
                    gather.drain(2)
                    gather.fetch(chunks + 3, sources, own_sem)
                    gather.turn(chunks + 3, natural)

                @pl.when(t == 3)
                def _():
                    gather.step2(c + 2)

            @pl.when(t == 3)
            def _():
                gather.step3(c + 1)

            @pl.when(i >= 1)
            def _():
                for copy in stored(i - 1):
                    copy.start()

            @pl.when(i >= 2)
            def _():
                for copy in stored(i - 2):
                    copy.wait()

            hidden = ast(slot)
            for r in range(0, TILE, SMALL):
                a, rows = abuf[sliced(t * (TILE // SMALL) + r // SMALL, SMALL), :], slice(r, r + SMALL)
                for b in range(0, dm.chunk, HALF):
                    part = slice(b, b + HALF)
                    gate = dot(a, w[c, 0, :, part])
                    up = dot(a, w[c, 1, :, part])
                    gst[slot, rows, part] = gate
                    ust[slot, rows, part] = up
                    hidden[rows, part] = hidden_of(gate, up)
            if not last:
                add_to(big.at[:, at_t], c == 0, dot(w[c, 2], hidden[...], NT))
                return
            for b in range(0, TILE, HALF):
                at_b = pl.ds(pl.multiple_of(t * TILE + b, HALF), HALF)
                total = big[:, at_b] + dot(w[c, 2], hidden[b : b + HALF, :], NT)
                h = xt[:, at_b] + total.astype(BF)
                wide = h.astype(F32)
                a = (wide * scale_of(wide, 0, dm.d)).astype(BF)
                xt[:, at_b] = h
                at[:, at_b] = a
                abuf[at_b, :] = a.T

        @pl.loop(0, steps - tiles)
        def _(i):
            tile_step(i, False)

        a0t_out.wait()

        @pl.loop(steps - tiles, steps)
        def _(i):
            tile_step(i, True)

        for copy in stored(steps - 1):
            copy.start()
        gather.fetched(chunks + 2, own_sem)
        gather.step1(chunks + 2)
        gather.drain(chunks - 1)
        for copy in at_last:
            copy.start()
        for i in range(steps - 2, steps):
            for copy in stored(i):
                copy.wait()

    pl.run_scoped(forward, pltpu.VMEM((2, TILE, dm.chunk), F32), pltpu.VMEM((2, TILE, dm.chunk), F32))

    def spread(buffer, c, kind):
        size = dm.packed - dm.rows
        return buffer.at[kind * size : (kind + 1) * size, pl.ds(pl.multiple_of(c * dm.chunk, dm.chunk), dm.chunk)]

    def pair(buffer, c, kind):
        return buffer.at[lax.rem(c, 2), kind]

    def cut(buffer, c, kind):
        slot = lax.rem(c, 4)
        return buffer.at[slot // 2, kind, :, pl.ds(pl.multiple_of(lax.rem(slot, 2) * HALF, HALF), HALF)]

    def backward1(ba, bg, bu, stash, grads):
        wides = Scatter(
            dm, True, lambda c, half: big_block(2 * lax.rem(c, 2) + half, dm.chunk), pair, 2, wsend, wrecv, wsends, wrecvs
        )
        downs = Scatter(dm, False, lambda c, half: big_block(4 + lax.rem(c, 2), dm.chunk), pair, 2, dsend, drecv, dsends, drecvs)

        def stored(i):
            slot, chunk, at_t = lax.rem(i, 2), i // tiles, sliced(lax.rem(i, tiles), TILE)
            return [move(a.at[slot], b.at[chunk, at_t, :], by_sem.at[k, slot]) for k, (a, b) in enumerate(((bg, by_gates), (bu, by_ups)))]

        def step1(c):
            for kinds in ((0, 1), (2, 3)):
                wides.step1(c, kinds)
                downs.step1(c, kinds)

        def step2(c):
            wides.step2(c)
            downs.step2(c)

        out = lambda c: move(grads, grads_out.at[1, c], g_sem.at[1])

        def step3(c):
            @pl.when(c >= 1)
            def _():
                out(c - 1).wait()

            def put(first, last):
                def put(half, columns, g):
                    grads[half * dm.packed + first : half * dm.packed + last, columns] = g

                return put

            wides.step3(c, put(0, dm.rows), squares)
            downs.step3(c, put(dm.rows, dm.packed), squares)
            out(c).start()

        def gate_tile(slot, c):
            return at.at[0:SMALL, pl.ds(pl.multiple_of((slot * chunks + c) * dm.chunk, dm.chunk), dm.chunk)]

        def up_tile(slot, c):
            return dyb.at[sliced(slot * chunks + c, SMALL), 0 : dm.chunk]

        def inputs(t):
            slot, at_t = lax.rem(t, 2), sliced(t, SMALL)
            return [
                move(src.at[c, at_t, :], tile(slot, c), in_sem.at[k, slot, c])
                for k, (src, tile) in enumerate(((by_gates, gate_tile), (by_ups, up_tile)))
                for c in range(chunks)
            ]

        @pl.loop(0, steps)
        def _(i):
            c, t = i // tiles, lax.rem(i, tiles)
            slot, at_t = lax.rem(i, 2), sliced(t, TILE)

            @pl.when(t == 0)
            def _():
                gather.done(chunks + c)

            @pl.when(i == 0)
            def _():
                dy_back.start()

            @pl.when(i == 1)
            def _():
                gather.step3(chunks + 1)

            @pl.when(i == 2)
            def _():
                dy_back.wait()

            @pl.when(jnp.logical_and(t == 0, c >= 2))
            def _():
                step3(c - 2)

            @pl.when(jnp.logical_and(t == 0, c >= 1))
            def _():
                step1(c - 1)

            @pl.when(i == 2)
            def _():
                gather.step2(units - 2)
                gather.fetched(units - 1, own_sem)
                gather.step1(units - 1)

            @pl.when(i == 3)
            def _():
                gather.step3(units - 2)

            @pl.when(i == 5)
            def _():
                gather.step2(units - 1)

            @pl.when(i == 7)
            def _():
                gather.step3(units - 1)

            @pl.when(jnp.logical_and(t == 2, c >= 1))
            def _():
                step2(c - 1)

            @pl.when(i >= 1)
            def _():
                for copy in stored(i - 1):
                    copy.start()

            @pl.when(i >= 2)
            def _():
                for copy in stored(i - 2):
                    copy.wait()

            @pl.when(i == steps - 1)
            def _():
                for copy in inputs(0):
                    copy.start()

            s = gather.slot(chunks + c)
            for r in range(0, TILE, ROWS):
                tokens, rows = sliced(t * (TILE // ROWS) + r // ROWS, ROWS), slice(r, r + ROWS)
                a, y = abuf[tokens, :], dyb[tokens, :]
                for b in range(0, dm.chunk, HALF):
                    part = slice(b, b + HALF)
                    gate, up = dot(a, w[s, 0, :, part]), dot(a, w[s, 1, :, part])
                    by_gate, by_up = back_through(gate, up, dot(y, w[s, 2, :, part]))
                    ba[rows, part] = hidden_of(gate, up)
                    bg[slot, rows, part] = by_gate
                    bu[slot, rows, part] = by_up
            add_to(wides.term(c, 0), t == 0, dot(at[:, at_t], bg[slot]))
            add_to(wides.term(c, 1), t == 0, dot(at[:, at_t], bu[slot]))
            add_to(downs.term(c, 0), t == 0, dot(dytb[:, at_t], ba[...]))

        last = chunks - 1
        for copy in stored(steps - 1):
            copy.start()
        step3(last - 1)
        step1(last)
        for i in range(steps - 2, steps):
            for copy in stored(i):
                copy.wait()

        def matmuls(t):
            slot, total = lax.rem(t, 2), None
            for c in range(chunks):
                s = (chunks + c) % (chunks + 1)
                term = dot(w[s, 0], gate_tile(slot, c)[...], NT) + dot(w[s, 1], up_tile(slot, c)[...], NT)
                total = term if total is None else total + term
            return total.astype(BF)

        def finish(t):
            for k in range(0, SMALL, PIECE):
                at_k = sliced(t * (SMALL // PIECE) + k // PIECE, PIECE)
                by_a = stash[:, k : k + PIECE].astype(F32)
                h = xt[:, at_k].astype(F32)
                square = jnp.sum(h * h, 0, keepdims=True) / dm.d + 1e-6
                scale = lax.rsqrt(square)
                along = jnp.sum(h * by_a, 0, keepdims=True) * (scale / square) / dm.d
                by_h = dytb[:, at_k] + (by_a * scale - h * along).astype(BF)
                dytb[:, at_k] = by_h
                abuf[at_k, :] = by_h.T

        for copy in inputs(1):
            copy.start()
        for copy in inputs(0):
            copy.wait()
        stash[...] = matmuls(0)

        @pl.loop(1, small)
        def _(t):
            @pl.when(t == 3)
            def _():
                step2(last)

            @pl.when(t == 6)
            def _():
                step3(last)

            for copy in inputs(t):
                copy.wait()

            @pl.when(t + 1 < small)
            def _():
                for copy in inputs(t + 1):
                    copy.start()

            @pl.when(t == small - 1)
            def _():
                hidden(0).start()

            finish(t - 1)
            stash[...] = matmuls(t)

        hidden(1).start()
        a0t_back.start()
        for u in range(chunks, units):
            gather.drain(u)
        at_end.start()
        hidden(0).wait()
        big[:, 0 : dm.chunk] = dot(dytb[:, 0:span], hidden_at(0)[...])
        finish(small - 1)
        for neighbour in (left, right):
            pl.semaphore_signal(ready, inc=1, device_id={"dp": neighbour}, device_id_type=pl.DeviceIdType.MESH)
        out(last).wait()

    span = dm.tokens // 2

    def hidden_at(i):
        return dyb.at[sliced(lax.rem(i, 2), span), 0 : dm.chunk]

    def hidden(i):
        return move(acts.at[i // 2, sliced(lax.rem(i, 2), span), :], hidden_at(i), ab_sem.at[lax.rem(i, 2)])

    pl.run_scoped(
        backward1,
        pltpu.VMEM((TILE, dm.chunk), BF), pltpu.VMEM((2, TILE, dm.chunk), BF), pltpu.VMEM((2, TILE, dm.chunk), BF), pltpu.VMEM((dm.d, SMALL), BF),
        pltpu.VMEM((2 * dm.packed, dm.chunk), BF),
    )

    def backward0(gb, ub, bg, bu):
        cuts, parts = dm.chunk // HALF, dm.tokens // gb.shape[1]
        wides = Scatter(
            dm, True, lambda u, half: big_block(2 * chunks * cuts // 2 + 2 * lax.rem(u, 4) + half, HALF), cut, 4, wsend, wrecv, wsends, wrecvs
        )
        downs = Scatter(
            dm, False, lambda c, half: big_block(c, dm.chunk), spread, chunks, xt.at[:, 0:rest], xt.at[:, rest:], dsends, drecvs
        )

        def inputs(i):
            slot, unit, at_t = lax.rem(i, 2), i // parts, sliced(lax.rem(i, parts), gb.shape[1])
            columns = pl.ds(pl.multiple_of(lax.rem(unit, cuts) * HALF, HALF), HALF)
            return (
                move(gates.at[unit // cuts, at_t, columns], gb.at[slot], gu_sem.at[0, slot]),
                move(ups.at[unit // cuts, at_t, columns], ub.at[slot], gu_sem.at[1, slot]),
            )

        @pl.loop(1, 2 * chunks)
        def _(i):
            c, t = i // 2, lax.rem(i, 2)

            @pl.when(i == 1)
            def _():
                pl.semaphore_wait(ready, 2)

            @pl.when(i + 1 < 2 * chunks)
            def _():
                hidden(i + 1).start()

            for k in range(2):

                @pl.when(i == 3 + 3 * k)
                def _():
                    for copy in inputs(k):
                        copy.start()

            hidden(i).wait()
            add_to(downs.term(c, 0), t == 0, dot(dytb[:, sliced(t, span)], hidden_at(i)[...]))

            @pl.when(t == 1)
            def _():
                downs.step1(c)

        a0t_back.wait()
        at_end.wait()
        for copy in at_last:
            copy.wait()

        def sums(c):
            return w.at[c // 3, lax.rem(c, 3), 0 : 2 * dm.packed, :]

        def put_down(c):
            def put(half, columns, g):
                sums(c)[pl.ds(half * dm.packed + dm.rows, dm.packed - dm.rows), columns] = g

            return put

        def put_wide(unit):
            def put(half, columns, g):
                to = sums(unit // cuts).at[:, pl.ds(pl.multiple_of(lax.rem(unit, cuts) * HALF, HALF), HALF)]
                to[pl.ds(half * dm.packed, dm.rows), :] = g

            return put

        cut_units = chunks * cuts
        first, middle = 0, parts // 2

        @pl.loop(0, cut_units * parts)
        def _(i):
            unit, t, slot = i // parts, lax.rem(i, parts), lax.rem(i, 2)

            @pl.when(jnp.logical_and(t == first, unit >= 1))
            def _():
                wides.step1(unit - 1)

            @pl.when(jnp.logical_and(t == middle, unit >= 3))
            def _():
                wides.step3(unit - 3, put_wide(unit - 3), squares)

            @pl.when(jnp.logical_and(t == middle, unit >= 2))
            def _():
                wides.step2(unit - 2)

            @pl.when(i < chunks)
            def _():
                downs.step2(i)

            @pl.when(jnp.logical_and(i >= 2 * chunks, i < 3 * chunks))
            def _():
                downs.step3(i - 2 * chunks, put_down(i - 2 * chunks), squares)

            @pl.when(jnp.logical_and(i >= 1, i + 1 < cut_units * parts))
            def _():
                for copy in inputs(i + 1):
                    copy.start()

            for copy in inputs(i):
                copy.wait()
            c = unit // cuts
            slot_w, which = chunks - 1 + (c // 2) * (1 - lax.rem(c, 2)), lax.rem(c, 2) * (1 + c // 2)
            weights = w[slot_w, which, :, pl.ds(pl.multiple_of(lax.rem(unit, cuts) * HALF, HALF), HALF)]
            size = gb.shape[1]
            blocks = [(slice(b, b + SMALL), sliced(t * (size // SMALL) + b // SMALL, SMALL)) for b in range(0, size, SMALL)]
            by_acts = [dot(abuf[tokens, :], weights) for _, tokens in blocks]
            totals = [None, None]
            for (rows, tokens), by_act in zip(blocks, by_acts, strict=True):
                bg[rows, :], bu[rows, :] = back_through(gb[slot, rows, :], ub[slot, rows, :], by_act)
                for k, right in enumerate((bg, bu)):
                    term = dot(at[:, tokens], right[rows, :])
                    totals[k] = term if totals[k] is None else totals[k] + term
            for k in range(2):
                add_to(wides.term(unit, k), t == 0, totals[k])

        last = cut_units - 1
        wides.step1(last)
        wides.step2(last - 1)
        wides.step3(last - 2, put_wide(last - 2), squares)
        wides.step2(last)
        wides.step3(last - 1, put_wide(last - 1), squares)
        wides.step3(last, put_wide(last), squares)
        out = [move(sums(c), grads_out.at[0, c], g_sem.at[1 + c]) for c in range(chunks)]
        copies = []
        for k in range(dm.n - 1, 0, -1):
            to = lax.rem(me + k, dm.n)
            copies.append(remote(squares, squares_out.at[me], ssends.at[k - 1], srecvs.at[k - 1], {"dp": to}))
        copies.append(move(squares, squares_out.at[me], g_sem.at[0]))
        for copy in copies:
            copy.start()
        for copy in out:
            copy.start()
        for copy in copies:
            copy.wait()
        for copy in out:
            copy.wait()

    part = CUT_TILE
    pl.run_scoped(
        backward0,
        pltpu.VMEM((2, part, HALF), F32), pltpu.VMEM((2, part, HALF), F32), pltpu.VMEM((part, HALF), BF), pltpu.VMEM((part, HALF), BF),
    )


def optimizer_kernel(dm, squares_in, grads_in, *refs):
    ins, outs, (squares, grads, *buffers), (g_sem, in_sem, out_sem) = refs[:9], refs[9:18], refs[18:26], refs[26:]
    move(squares_in, squares, g_sem.at[dm.layers]).start()
    stores = [buffers[0:2], buffers[2:4], buffers[4:6]]
    halves = 2
    pieces = [(layer, which, half) for layer in range(dm.layers) for which in range(3) for half in range(halves)]

    def places(piece):
        layer, which, half = piece
        out = []
        for kind in range(3):
            if which < 2:
                cut = slice(half * dm.ff // halves, (half + 1) * dm.ff // halves)
                here = stores[kind][0].at[2 * layer + which, :, cut]
                out.append((ins[3 * kind + which].at[layer, :, cut], here, outs[3 * kind + which].at[layer, :, cut]))
            else:
                cut = slice(half * dm.own_ff // halves, (half + 1) * dm.own_ff // halves)
                here = stores[kind][1].at[layer, cut, :]
                out.append((ins[3 * kind + which].at[layer, cut, :], here, outs[3 * kind + which].at[layer, cut, :]))
        return out

    fetch = [move(grads_in.at[layer], grads.at[layer], g_sem.at[layer]) for layer in range(dm.layers)]
    loads = [[move(a, b, in_sem.at[k, kind]) for kind, (a, b, _) in enumerate(places(p))] for k, p in enumerate(pieces)]
    writes = [[move(b, c, out_sem.at[k, kind]) for kind, (_, b, c) in enumerate(places(p))] for k, p in enumerate(pieces)]
    for layer in range(dm.layers):
        fetch[layer].start()
        for k, piece in enumerate(pieces):
            if piece[0] == layer:
                for copy in loads[k]:
                    copy.start()
    count = dm.layers * 3 * dm.d * dm.ff
    move(squares_in, squares, g_sem.at[dm.layers]).wait()
    total = squares[0]
    for k in range(1, dm.n):
        total = total + squares[k]
    factor = jnp.minimum(1.0, 0.5 * lax.rsqrt(jnp.sum(total) / count + 1e-30))
    size = dm.d // 2 // dm.n

    def adamw(g, refs, at):
        w, m, v = (ref[at] for ref in refs)
        g = g.astype(F32) * factor
        w = w.astype(F32)
        m = 0.9 * m + 0.1 * g
        v = 0.95 * v + 0.05 * g * g
        change = m * lax.rsqrt(v + 1e-8) + 0.1 * w
        refs[0][at] = (w - 0.02 * change).astype(BF)
        refs[1][at] = m
        refs[2][at] = v

    for k, (layer, which, half) in enumerate(pieces):
        if (which, half) == (0, 0):
            fetch[layer].wait()
        for copy in loads[k]:
            copy.wait()
        refs = [here for _, here, _ in places(pieces[k])]
        if which < 2:
            for b in range(dm.ff // halves // LANES):
                q, c = divmod(half * dm.ff // halves // LANES + b, dm.chunks)
                g = grads[layer, c, which * dm.packed : which * dm.packed + dm.rows, q * LANES : (q + 1) * LANES]
                adamw(g, refs, (slice(None), slice(b * LANES, (b + 1) * LANES)))
        else:
            for b in range(dm.own_ff // halves // LANES):
                c = half * dm.own_ff // halves // LANES + b
                for row in range(2 * dm.n):
                    side, i = divmod(row, dm.n)
                    start = side * dm.packed + dm.rows
                    g = grads[layer, c, start : start + size, i * LANES : (i + 1) * LANES]
                    if row == 0:
                        rows = []
                    rows.append(g)
                adamw(jnp.concatenate(rows, axis=0).T, refs, (slice(b * LANES, (b + 1) * LANES), slice(None)))
        for copy in writes[k]:
            copy.start()
    for copies in writes:
        for copy in copies:
            copy.wait()


def step(mesh, x, dy, *arrays):
    weights, m, v = (arrays[i : i + 3] for i in (0, 3, 6))
    x, dy = x[0], dy[0]
    w_gate, w_up, w_down = weights
    n = mesh.shape["dp"]
    dm = Dims(w_gate.shape[0], x.shape[0], x.shape[1], w_gate.shape[2], n)
    tokens, d, chunk, chunks, tiles = dm.tokens, dm.d, dm.chunk, dm.chunks, dm.tiles
    hbm = pl.BlockSpec(memory_space=pltpu.HBM)
    shape = jax.ShapeDtypeStruct
    dma = lambda *s: pltpu.SemaphoreType.DMA(s)
    natural, turned, per_chunk = (tokens, d), (d, tokens), (chunks, tokens, chunk)
    block, wide, down = (2 * dm.packed, chunk), (dm.rows, chunk), (dm.packed - dm.rows, chunk)
    units = dm.layers * chunks
    semaphores = [
        dma(units), dma(2), dma(dm.small), dma(dm.small), dma(3, 2), dma(2, 2), dma(2, 2, chunks), dma(2, 2), dma(2), dma(9), dma(1 + chunks),
        pltpu.SemaphoreType.REGULAR,
        dma(units, Gather.COPIES), dma(units, Gather.COPIES), dma(4, 6), dma(4, 6), dma(chunks, 6), dma(chunks, 6), dma(n - 1), dma(n - 1),
    ]

    def kernel(*refs):
        pl.run_scoped(lambda *scoped: whole_kernel(dm, *refs, *scoped), *semaphores)

    grads, squares, *_ = pl.pallas_call(
        kernel,
        out_shape=[
            shape((2, chunks, *block), BF), shape((n, 8, LANES), F32), shape(per_chunk, F32), shape(per_chunk, F32), shape(per_chunk, BF),
            shape(turned, BF), shape((chunks - 1, d, chunk), BF), shape(per_chunk, BF), shape(per_chunk, BF),
        ],
        in_specs=[hbm] * 5,
        out_specs=[hbm] * 9,
        scratch_shapes=[
            pltpu.VMEM(natural, BF), pltpu.VMEM(turned, BF), pltpu.VMEM(turned, BF), pltpu.VMEM(natural, BF), pltpu.VMEM(turned, BF),
            pltpu.VMEM(turned, F32), pltpu.VMEM((chunks + 1, 3, d, chunk), BF), pltpu.VMEM((dm.own_ff, d), BF),
            pltpu.VMEM((2, 6, *wide), BF), pltpu.VMEM((2, 6, *wide), BF), pltpu.VMEM((2, 6, *down), BF), pltpu.VMEM((2, 6, *down), BF),
            pltpu.VMEM((8, LANES), F32),
        ],
        compiler_params=pltpu.CompilerParams(vmem_limit_bytes=VMEM_LIMIT, collective_id=0, has_side_effects=True),
        name="whole",
    )(x, dy, w_gate, w_up, w_down)

    wides, downs = (2 * dm.layers, dm.rows, dm.ff), (dm.layers, dm.own_ff, d)
    return tuple(
        pl.pallas_call(
            functools.partial(optimizer_kernel, dm),
            out_shape=[shape(w.shape, BF) for w in weights] + [shape(w.shape, F32) for w in weights] * 2,
            in_specs=[hbm] * 11,
            out_specs=[hbm] * 9,
            scratch_shapes=[
                pltpu.VMEM((n, 8, LANES), F32), pltpu.VMEM((2, chunks, *block), BF), pltpu.VMEM(wides, BF), pltpu.VMEM(downs, BF),
                pltpu.VMEM(wides, F32), pltpu.VMEM(downs, F32), pltpu.VMEM(wides, F32), pltpu.VMEM(downs, F32),
                dma(dm.layers + 1), dma(6 * dm.layers, 3), dma(6 * dm.layers, 3),
            ],
            compiler_params=pltpu.CompilerParams(vmem_limit_bytes=VMEM_LIMIT),
            name="optimizer",
        )(squares, grads, *weights, *m, *v)
    )


def solution(mesh):
    states, cut = P(("rep", "dp"), None, None), P(None, "dp", None)
    return jax.shard_map(
        functools.partial(step, mesh),
        mesh=mesh,
        in_specs=(states, states) + (cut,) * 9,
        out_specs=(P("rep", "dp", None),) * 9,
        check_vma=False,
    )
```

```python
import dataclasses
import functools

import jax
import jax.numpy as jnp
from jax import lax
from jax.experimental import pallas as pl
from jax.experimental.pallas import tpu as pltpu
from jax.sharding import PartitionSpec as P

BF, F32 = jnp.bfloat16, jnp.float32
LANES = 128
TILE = 1024
SMALL = 512
HALF = 256
ROWS = 1024
FEW = 64
CUT_TILE = 2048
VMEM_LIMIT = 67043328
NT = (((1,), (1,)), ((), ()))
NN = (((1,), (0,)), ((), ()))


@dataclasses.dataclass(frozen=True)
class Dims:
    layers: int
    tokens: int
    d: int
    ff: int
    n: int

    @property
    def own_ff(self):
        return self.ff // self.n

    @property
    def rows(self):
        return self.d // self.n

    @property
    def chunk(self):
        return self.n * LANES

    @property
    def chunks(self):
        return self.own_ff // LANES

    @property
    def tiles(self):
        return self.tokens // TILE

    @property
    def small(self):
        return self.tokens // SMALL

    @property
    def packed(self):
        return self.rows + self.d // 2 // self.n


def dot(a, b, dims=NN):
    return lax.dot_general(a, b, dims, preferred_element_type=F32)


def sliced(i, size):
    return pl.ds(pl.multiple_of(i * size, size), size)


def ring(n):
    me = lax.axis_index("dp")
    return me, lax.rem(me + 1, n), lax.rem(me + n - 1, n)


def partner():
    rep = lax.axis_index("rep")
    core = lax.rem(rep, 2)
    return core, rep + 1 - 2 * core


def greet(*others):
    for other in others:
        pl.semaphore_signal(pltpu.get_barrier_semaphore(), inc=1, device_id=other, device_id_type=pl.DeviceIdType.MESH)


def greeted(count):
    pl.semaphore_wait(pltpu.get_barrier_semaphore(), count)


def remote(src, dst, send, recv, device):
    return pltpu.make_async_remote_copy(src_ref=src, dst_ref=dst, send_sem=send, recv_sem=recv, device_id=device, device_id_type=pl.DeviceIdType.MESH)


def scale_of(wide, axis, count):
    return lax.rsqrt(jnp.sum(wide * wide, axis, keepdims=True) / count + 1e-6)


def down_to_8(x):
    return jnp.sum(x.reshape(-1, 8, x.shape[-1]), 0)


def move(src, dst, sem):
    return pltpu.make_async_copy(src, dst, sem)


class Gather:
    COPIES = 14

    def __init__(self, dm, w, sends, recvs):
        self.dm, self.w, self.sends, self.recvs = dm, w, sends, recvs
        self.me, self.right, self.left = ring(dm.n)
        self.far = lax.rem(self.me + 2, dm.n)
        self.core, self.other = partner()

    def slot(self, unit):
        return lax.rem(unit, self.w.shape[0])

    def _both(self, unit, source):
        half = self.dm.rows // 2
        at = pl.multiple_of(source * self.dm.rows + self.core * half, half)
        return self.w.at[self.slot(unit), 0:2, pl.ds(at, half), :]

    def _one(self, unit, which, source):
        half = self.dm.rows // 2
        at = pl.multiple_of(source * self.dm.rows + self.core * half, half)
        return self.w.at[self.slot(unit), which, pl.ds(at, half), :]

    def _down(self, unit, source, quarter=None):
        half = self.dm.d // 2
        columns = pl.ds(pl.multiple_of(source * LANES, LANES), LANES)
        if quarter is None:
            return self.w.at[self.slot(unit), 2, pl.ds(pl.multiple_of(self.core * half, half), half), columns]
        return self.w.at[self.slot(unit), 2, pl.ds(pl.multiple_of(self.core * half + quarter * (half // 2), half // 2), half // 2), columns]

    def _copy(self, unit, index, ref, device):
        return remote(ref, ref, self.sends.at[unit, index], self.recvs.at[unit, index], device)

    def own(self, unit, part):
        ref = self._down(unit, self.me) if part else self._both(unit, self.me)
        return [self._copy(unit, 2 * to + part, ref, device) for to, device in enumerate(({"dp": self.right}, {"dp": self.left}))]

    def relayed(self, unit, part):
        if part:
            right, left = self._down(unit, self.left, 0), self._down(unit, self.right, 1)
        else:
            right, left = self._one(unit, 0, self.left), self._one(unit, 1, self.right)
        return [self._copy(unit, 4 + part, right, {"dp": self.right}), self._copy(unit, 6 + part, left, {"dp": self.left})]

    def shared(self, unit, part, sources):
        out = []
        for s in sources:
            source = (self.left, self.right, self.far)[s]
            ref = self._down(unit, source) if part else self._both(unit, source)
            out.append(self._copy(unit, 8 + 2 * s + part, ref, {"rep": self.other}))
        return out

    def _arrivals(self, unit, index, ref):
        return remote(ref, ref, self.sends.at[unit, index], self.recvs.at[unit, index], {"dp": self.right})

    def step1(self, unit, parts=(0, 1)):
        for part in parts:
            for copy in self.own(unit, part):
                copy.start()

    def step2(self, unit):
        for part in range(2):
            for to, source in enumerate((self.left, self.right)):
                ref = self._down(unit, source) if part else self._both(unit, source)
                self._arrivals(unit, 2 * to + part, ref).wait_recv()
            for copy in self.relayed(unit, part) + self.shared(unit, part, (0, 1)):
                copy.start()

    def step3(self, unit):
        for part in range(2):
            for k in range(2):
                ref = self._down(unit, self.far, k) if part else self._one(unit, k, self.far)
                self._arrivals(unit, 4 + 2 * k + part, ref).wait_recv()
            for copy in self.shared(unit, part, (2,)):
                copy.start()

    def _theirs(self, unit, s):
        dm, other = self.dm, 1 - self.core
        source = (self.left, self.right, self.far)[s]
        half = dm.rows // 2
        at = pl.multiple_of(source * dm.rows + other * half, half)
        columns = pl.ds(pl.multiple_of(source * LANES, LANES), LANES)
        rows = pl.ds(pl.multiple_of(other * (dm.d // 2), dm.d // 2), dm.d // 2)
        return self.w.at[self.slot(unit), 0:2, pl.ds(at, half), :], self.w.at[self.slot(unit), 2, rows, columns]

    def done(self, unit):
        for s in range(3):
            both, down = self._theirs(unit, s)
            self._arrivals(unit, 8 + 2 * s, both).wait_recv()
            self._arrivals(unit, 9 + 2 * s, down).wait_recv()

    def drain(self, unit):
        for part in range(2):
            for copy in self.own(unit, part) + self.relayed(unit, part) + self.shared(unit, part, (0, 1, 2)):
                copy.wait_send()

    def fetch(self, unit, sources, sem):
        dm = self.dm
        layer, chunk = unit // dm.chunks, lax.rem(unit, dm.chunks)
        for which in range(2):
            for q in range(dm.n):
                columns = pl.ds(pl.multiple_of(q * dm.own_ff + chunk * LANES, LANES), LANES)
                to = self.w.at[self.slot(unit), which, sliced(self.me, dm.rows), q * LANES : (q + 1) * LANES]
                move(sources[which].at[layer, :, columns], to, sem.at[unit]).start()

    def fetched(self, unit, sem):
        ref = self.w.at[self.slot(unit), 0:2, sliced(self.me, self.dm.rows), :]
        move(ref, ref, sem.at[unit]).wait()

    def turn(self, unit, natural):
        columns = pl.ds(pl.multiple_of(self.me * LANES, LANES), LANES)
        self.w[self.slot(unit), 2, :, columns] = natural[sliced(lax.rem(unit, self.dm.chunks), LANES), :].T


class Scatter:
    def __init__(self, dm, wide, terms, place, slots, send, recv, sends, recvs):
        self.dm, self.wide, self.terms, self.place, self.slots = dm, wide, terms, place, slots
        self.send, self.recv, self.sends, self.recvs = send, recv, sends, recvs
        self.me, self.right, self.left = ring(dm.n)
        self.far = lax.rem(self.me + 2, dm.n)

    def _copy(self, c, kind):
        device = {"dp": self.right if kind % 2 == 0 else self.left}
        slot = lax.rem(c, self.slots)
        return remote(self.place(self.send, c, kind), self.place(self.recv, c, kind), self.sends.at[slot, kind], self.recvs.at[slot, kind], device)

    def _parts(self, c, owner, half):
        dm = self.dm
        if self.wide:
            return [(ref[sliced(owner, dm.rows), :], slice(k * HALF, (k + 1) * HALF)) for k, ref in enumerate(self.terms(c, half))]
        size, per = dm.d // 2 // dm.n, HALF // LANES
        own = self.terms(c, owner // per).at[:, pl.ds(pl.multiple_of(lax.rem(owner, per) * LANES, LANES), LANES)]
        return [(own[pl.ds(half * (dm.d // 2) + i * size, size), :], slice(i * LANES, (i + 1) * LANES)) for i in range(dm.n)]

    def _put(self, c, kind, owner, half, add=None):
        to = self.place(self.send, c, kind)
        for term, columns in self._parts(c, owner, half):
            if add is not None:
                term = term + self.place(self.recv, c, add)[:, columns].astype(F32)
            to[:, columns] = term.astype(BF)
        self._copy(c, kind).start()

    def step1(self, c, kinds=(0, 1, 2, 3)):
        for kind in kinds:
            self._put(c, kind, (self.far, self.far, self.right, self.left)[kind], (0, 1, 1, 0)[kind])

    def step2(self, c):
        for kind, owner, half in ((0, self.right, 0), (1, self.left, 1)):
            self._copy(c, kind).wait_recv()
            self._put(c, kind + 4, owner, half, add=kind)
        for kind in (0, 1):
            self._copy(c, kind).wait_send()

    def step3(self, c, put, squares):
        for kind in (2, 3, 4, 5):
            self._copy(c, kind).wait_recv()
        for half, kinds in ((0, (4, 3)), (1, (2, 5))):
            for term, columns in self._parts(c, self.me, half):
                for kind in kinds:
                    term = term + self.place(self.recv, c, kind)[:, columns].astype(F32)
                g = term.astype(BF)
                put(half, columns, g)
                g = g.astype(F32)
                g = down_to_8(g * g)
                for j in range(0, g.shape[-1], LANES):
                    squares[...] += g[:, j : j + LANES]
        for kind in (2, 3, 4, 5):
            self._copy(c, kind).wait_send()


def back_through(gate, up, by_act):
    by_act = by_act.astype(BF).astype(F32)
    s = jax.nn.sigmoid(gate)
    by_up = (by_act * (gate * s)).astype(BF)
    by_gate = (by_act * up * (s * (1.0 + gate * (1.0 - s)))).astype(BF)
    return by_gate, by_up


def hidden_of(gate, up):
    return (gate * jax.nn.sigmoid(gate) * up).astype(BF)


def add_to(refs, first, term):
    for k, ref in enumerate(refs):
        part = term[:, k * HALF : (k + 1) * HALF]
        ref[...] = part if first is True else jnp.where(first, 0.0, ref[...]) + part


def whole_kernel(
    dm, x, dy, w_gate, w_up, w_down,
    grads_out, squares_out, gates, ups, acts, a0t, wd0, by_gates, by_ups,
    abuf, at, xt, dyb, dytb, big, w, natural, wsend, wrecv, dsend, drecv, squares,
    own_sem, nat_sem, x_sem, dy_sem, st_sem, by_sem, in_sem, gu_sem, ab_sem, misc_sem, g_sem, ready,
    gsends, grecvs, wsends, wrecvs, dsends, drecvs, ssends, srecvs,
):
    chunks, tiles, small, units = dm.chunks, dm.tiles, dm.small, dm.layers * dm.chunks
    steps = chunks * tiles
    gather = Gather(dm, w, gsends, grecvs)
    me, left, right, far = gather.me, gather.left, gather.right, gather.far
    sources = (w_gate, w_up)
    big_blocks = lambda i, width: [big.at[i * (width // HALF) + k] for k in range(width // HALF)]
    saved = [move(w.at[c, 2], wd0.at[c], misc_sem.at[c]) for c in range(chunks - 1)]
    at_last = [move(wd0.at[c], w.at[chunks - 1, c], misc_sem.at[3 + c]) for c in range(chunks - 2)]
    at_end = move(wd0.at[chunks - 2], w.at[chunks, 0], misc_sem.at[5])
    a0t_out, a0t_back = move(at, a0t, misc_sem.at[6]), move(a0t, at, misc_sem.at[7])
    rest = dm.tokens // 2
    dy_back = move(dy.at[rest:, :], dyb.at[rest:, :], misc_sem.at[8])

    greet({"dp": right}, {"dp": left}, {"rep": gather.other}, {"dp": far})
    gather.fetch(0, sources, own_sem)
    move(w_down.at[0], natural, nat_sem.at[0]).start()
    for t in range(small):
        move(x.at[pl.ds(t * SMALL, SMALL), :], abuf.at[pl.ds(t * SMALL, SMALL), :], x_sem.at[t]).start()
    gather.fetched(0, own_sem)
    greeted(4)
    gather.step1(0, (0,))
    move(w_down.at[0], natural, nat_sem.at[0]).wait()
    gather.turn(0, natural)
    gather.step1(0, (1,))
    for u in range(1, chunks + 1):
        gather.fetch(u, sources, own_sem)
    for t in range(small):
        move(dy.at[pl.ds(t * SMALL, SMALL), :], dyb.at[pl.ds(t * SMALL, SMALL), :], dy_sem.at[t]).start()

    @pl.loop(0, 2 * small)
    def _(t):
        @pl.when(lax.rem(t, 2) == 0)
        def _():
            ref = abuf.at[sliced(t // 2, SMALL), :]
            move(ref, ref, x_sem.at[t // 2]).wait()

        at_t = sliced(t, HALF)
        tile = abuf[at_t, :]
        wide = tile.astype(F32)
        a = (wide * scale_of(wide, -1, dm.d)).astype(BF)
        xt[:, at_t] = tile.T
        at[:, at_t] = a.T
        abuf[at_t, :] = a

    gather.step2(0)

    @pl.loop(1, chunks)
    def _(u):
        gather.turn(u, natural)

    move(w_down.at[1], natural, nat_sem.at[1]).start()
    gather.fetched(1, own_sem)
    gather.step1(1)
    a0t_out.start()

    @pl.loop(0, small)
    def _(t):
        at_t = sliced(t, SMALL)
        move(dy.at[at_t, :], dyb.at[at_t, :], dy_sem.at[t]).wait()
        dytb[:, at_t] = dyb[at_t, :].T

    squares[...] = jnp.zeros_like(squares)
    move(w_down.at[1], natural, nat_sem.at[1]).wait()
    gather.turn(chunks, natural)
    gather.step3(0)

    def forward(gst, ust):
        def ast(slot):
            return dyb.at[pl.ds(pl.multiple_of(rest + slot * TILE, TILE), TILE), 0 : dm.chunk]

        def stored(i):
            slot, chunk, at_t = lax.rem(i, 2), i // tiles, sliced(lax.rem(i, tiles), TILE)
            pairs = ((gst.at[slot], gates), (ust.at[slot], ups), (ast(slot), acts))
            return [move(a, b.at[chunk, at_t, :], st_sem.at[k, slot]) for k, (a, b) in enumerate(pairs)]

        def tile_step(i, last):
            c, t = i // tiles, lax.rem(i, tiles)
            slot, at_t = lax.rem(i, 2), sliced(t, TILE)

            @pl.when(t == 0)
            def _():
                gather.done(c)

            if not last:
                for k in range(chunks - 1):

                    @pl.when(i == k * tiles)
                    def _():
                        saved[k].start()

                    @pl.when(i == k * tiles + 3)
                    def _():
                        saved[k].wait()

            @pl.when(t == 1)
            def _():
                gather.step2(c + 1)

            if not last:

                @pl.when(i == tiles + 1)
                def _():
                    gather.drain(0)
                    gather.fetch(chunks + 1, sources, own_sem)
                    gather.turn(chunks + 1, natural)

                @pl.when(t == 1)
                def _():
                    gather.fetched(c + 2, own_sem)
                    gather.step1(c + 2)

                @pl.when(i == 2 * tiles + 3)
                def _():
                    gather.drain(1)
                    gather.fetch(chunks + 2, sources, own_sem)
                    gather.turn(chunks + 2, natural)
                    gather.fetched(chunks + 1, own_sem)
                    gather.step1(chunks + 1)

            else:

                @pl.when(t == 1)
                def _():
                    gather.drain(2)
                    gather.fetch(chunks + 3, sources, own_sem)
                    gather.turn(chunks + 3, natural)

                @pl.when(t == 3)
                def _():
                    gather.step2(c + 2)

            @pl.when(t == 3)
            def _():
                gather.step3(c + 1)

            @pl.when(i >= 1)
            def _():
                for copy in stored(i - 1):
                    copy.start()

            @pl.when(i >= 2)
            def _():
                for copy in stored(i - 2):
                    copy.wait()

            hidden = ast(slot)
            for r in range(0, TILE, SMALL):
                a, rows = abuf[sliced(t * (TILE // SMALL) + r // SMALL, SMALL), :], slice(r, r + SMALL)
                for b in range(0, dm.chunk, HALF):
                    part = slice(b, b + HALF)
                    gate = dot(a, w[c, 0, :, part])
                    up = dot(a, w[c, 1, :, part])
                    gst[slot, rows, part] = gate
                    ust[slot, rows, part] = up
                    hidden[rows, part] = hidden_of(gate, up)
            if not last:
                add_to(big_blocks(t, TILE), c == 0, dot(w[c, 2], hidden[...], NT))
                return
            for b in range(0, TILE, HALF):
                at_b = pl.ds(pl.multiple_of(t * TILE + b, HALF), HALF)
                total = big[t * (TILE // HALF) + b // HALF] + dot(w[c, 2], hidden[b : b + HALF, :], NT)
                h = xt[:, at_b] + total.astype(BF)
                wide = h.astype(F32)
                a = (wide * scale_of(wide, 0, dm.d)).astype(BF)
                xt[:, at_b] = h
                at[:, at_b] = a
                abuf[at_b, :] = a.T

        @pl.loop(0, steps - tiles)
        def _(i):
            tile_step(i, False)

        a0t_out.wait()

        @pl.loop(steps - tiles, steps)
        def _(i):
            tile_step(i, True)

        for copy in stored(steps - 1):
            copy.start()
        gather.fetched(chunks + 2, own_sem)
        gather.step1(chunks + 2)
        gather.drain(chunks - 1)
        for copy in at_last:
            copy.start()
        for i in range(steps - 2, steps):
            for copy in stored(i):
                copy.wait()

    pl.run_scoped(forward, pltpu.VMEM((2, TILE, dm.chunk), F32), pltpu.VMEM((2, TILE, dm.chunk), F32))

    def spread(buffer, c, kind):
        size = dm.packed - dm.rows
        return buffer.at[kind * size : (kind + 1) * size, pl.ds(pl.multiple_of(c * dm.chunk, dm.chunk), dm.chunk)]

    def pair(buffer, c, kind):
        return buffer.at[lax.rem(c, 2), kind]

    def cut(buffer, c, kind):
        slot = lax.rem(c, 4)
        return buffer.at[slot // 2, kind, :, pl.ds(pl.multiple_of(lax.rem(slot, 2) * HALF, HALF), HALF)]

    def backward1(ba, bg, bu, stash, grads):
        wides = Scatter(
            dm, True, lambda c, half: big_blocks(2 * lax.rem(c, 2) + half, dm.chunk), pair, 2, wsend, wrecv, wsends, wrecvs
        )
        down_blocks = lambda c: big_blocks(4 + lax.rem(c, 2), dm.chunk)
        downs = Scatter(dm, False, lambda c, k: big.at[(4 + lax.rem(c, 2)) * (dm.chunk // HALF) + k], pair, 2, dsend, drecv, dsends, drecvs)

        def stored(i):
            slot, chunk, at_t = lax.rem(i, 2), i // tiles, sliced(lax.rem(i, tiles), TILE)
            return [move(a.at[slot], b.at[chunk, at_t, :], by_sem.at[k, slot]) for k, (a, b) in enumerate(((bg, by_gates), (bu, by_ups)))]

        def step1(c):
            for kinds in ((0, 1), (2, 3)):
                wides.step1(c, kinds)
                downs.step1(c, kinds)

        def step2(c):
            wides.step2(c)
            downs.step2(c)

        out = lambda c: move(grads, grads_out.at[1, c], g_sem.at[1])

        def step3(c):
            @pl.when(c >= 1)
            def _():
                out(c - 1).wait()

            def put(first, last):
                def put(half, columns, g):
                    grads[half * dm.packed + first : half * dm.packed + last, columns] = g

                return put

            wides.step3(c, put(0, dm.rows), squares)
            downs.step3(c, put(dm.rows, dm.packed), squares)
            out(c).start()

        def gate_tile(slot, c):
            return at.at[0:SMALL, pl.ds(pl.multiple_of((slot * chunks + c) * dm.chunk, dm.chunk), dm.chunk)]

        def up_tile(slot, c):
            return dyb.at[sliced(slot * chunks + c, SMALL), 0 : dm.chunk]

        def inputs(t):
            slot, at_t = lax.rem(t, 2), sliced(t, SMALL)
            return [
                move(src.at[c, at_t, :], tile(slot, c), in_sem.at[k, slot, c])
                for k, (src, tile) in enumerate(((by_gates, gate_tile), (by_ups, up_tile)))
                for c in range(chunks)
            ]

        @pl.loop(0, steps)
        def _(i):
            c, t = i // tiles, lax.rem(i, tiles)
            slot, at_t = lax.rem(i, 2), sliced(t, TILE)

            @pl.when(t == 0)
            def _():
                gather.done(chunks + c)

            @pl.when(i == 0)
            def _():
                dy_back.start()

            @pl.when(i == 1)
            def _():
                gather.step3(chunks + 1)

            @pl.when(i == 2)
            def _():
                dy_back.wait()

            @pl.when(jnp.logical_and(t == 0, c >= 2))
            def _():
                step3(c - 2)

            @pl.when(jnp.logical_and(t == 0, c >= 1))
            def _():
                step1(c - 1)

            @pl.when(i == 2)
            def _():
                gather.step2(units - 2)
                gather.fetched(units - 1, own_sem)
                gather.step1(units - 1)

            @pl.when(i == 4)
            def _():
                gather.step3(units - 2)

            @pl.when(i == 5)
            def _():
                gather.step2(units - 1)

            @pl.when(i == 9)
            def _():
                gather.step3(units - 1)

            @pl.when(jnp.logical_and(t == 2, c >= 1))
            def _():
                step2(c - 1)

            @pl.when(i >= 1)
            def _():
                for copy in stored(i - 1):
                    copy.start()

            @pl.when(i >= 2)
            def _():
                for copy in stored(i - 2):
                    copy.wait()

            @pl.when(i == steps - 1)
            def _():
                for copy in inputs(0):
                    copy.start()

            s = gather.slot(chunks + c)
            for r in range(0, TILE, ROWS):
                tokens, rows = sliced(t * (TILE // ROWS) + r // ROWS, ROWS), slice(r, r + ROWS)
                a, y = abuf[tokens, :], dyb[tokens, :]
                for b in range(0, dm.chunk, HALF):
                    part = slice(b, b + HALF)
                    gate, up = dot(a, w[s, 0, :, part]), dot(a, w[s, 1, :, part])
                    by_gate, by_up = back_through(gate, up, dot(y, w[s, 2, :, part]))
                    ba[rows, part] = hidden_of(gate, up)
                    bg[slot, rows, part] = by_gate
                    bu[slot, rows, part] = by_up
            add_to(wides.terms(c, 0), t == 0, dot(at[:, at_t], bg[slot]))
            add_to(wides.terms(c, 1), t == 0, dot(at[:, at_t], bu[slot]))
            add_to(down_blocks(c), t == 0, dot(dytb[:, at_t], ba[...]))

        last = chunks - 1
        for copy in stored(steps - 1):
            copy.start()
        step3(last - 1)
        step1(last)
        for i in range(steps - 2, steps):
            for copy in stored(i):
                copy.wait()

        def matmuls(t):
            slot, total = lax.rem(t, 2), None
            for c in range(chunks):
                s = (chunks + c) % (chunks + 1)
                term = dot(w[s, 0], gate_tile(slot, c)[...], NT) + dot(w[s, 1], up_tile(slot, c)[...], NT)
                total = term if total is None else total + term
            return total.astype(BF)

        def finish(t):
            for k in range(0, SMALL, HALF):
                at_k = sliced(t * (SMALL // HALF) + k // HALF, HALF)
                square = along = jnp.zeros((8, HALF), F32)
                for r in range(0, dm.d, FEW):
                    by_a, h = stash[r : r + FEW, k : k + HALF].astype(F32), xt[r : r + FEW, at_k].astype(F32)
                    square, along = square + down_to_8(h * h), along + down_to_8(h * by_a)
                square = jnp.sum(square, 0, keepdims=True) / dm.d + 1e-6
                scale = lax.rsqrt(square)
                along = jnp.sum(along, 0, keepdims=True) * (scale / square) / dm.d
                for r in range(0, dm.d, FEW):
                    by_a, h = stash[r : r + FEW, k : k + HALF].astype(F32), xt[r : r + FEW, at_k].astype(F32)
                    by_h = dytb[r : r + FEW, at_k] + (by_a * scale - h * along).astype(BF)
                    dytb[r : r + FEW, at_k] = by_h
                    abuf[at_k, r : r + FEW] = by_h.T

        for copy in inputs(1):
            copy.start()
        for copy in inputs(0):
            copy.wait()
        stash[...] = matmuls(0)

        @pl.loop(1, small)
        def _(t):
            @pl.when(t == 3)
            def _():
                step2(last)

            @pl.when(t == 6)
            def _():
                step3(last)

            for copy in inputs(t):
                copy.wait()

            @pl.when(t + 1 < small)
            def _():
                for copy in inputs(t + 1):
                    copy.start()

            @pl.when(t == small - 1)
            def _():
                hidden(0).start()

            finish(t - 1)
            stash[...] = matmuls(t)

        hidden(1).start()
        a0t_back.start()
        for u in range(chunks, units):
            gather.drain(u)
        at_end.start()
        hidden(0).wait()
        add_to(big_blocks(0, dm.chunk), True, dot(dytb[:, 0:span], hidden_at(0)[...]))
        finish(small - 1)
        for neighbour in (left, right):
            pl.semaphore_signal(ready, inc=1, device_id={"dp": neighbour}, device_id_type=pl.DeviceIdType.MESH)
        out(last).wait()

    span = dm.tokens // 2

    def hidden_at(i):
        return dyb.at[sliced(lax.rem(i, 2), span), 0 : dm.chunk]

    def hidden(i):
        return move(acts.at[i // 2, sliced(lax.rem(i, 2), span), :], hidden_at(i), ab_sem.at[lax.rem(i, 2)])

    pl.run_scoped(
        backward1,
        pltpu.VMEM((TILE, dm.chunk), BF), pltpu.VMEM((2, TILE, dm.chunk), BF), pltpu.VMEM((2, TILE, dm.chunk), BF), pltpu.VMEM((dm.d, SMALL), BF),
        pltpu.VMEM((2 * dm.packed, dm.chunk), BF),
    )

    def backward0(gb, ub, bg, bu):
        cuts, parts = dm.chunk // HALF, dm.tokens // gb.shape[1]
        wides = Scatter(
            dm, True, lambda u, half: big_blocks(chunks * cuts + 2 * lax.rem(u, 4) + half, HALF), cut, 4, wsend, wrecv, wsends, wrecvs
        )
        downs = Scatter(
            dm, False, lambda c, k: big.at[c * cuts + k], spread, chunks, xt.at[:, 0:rest], xt.at[:, rest:], dsends, drecvs
        )

        def inputs(i):
            slot, unit, at_t = lax.rem(i, 2), i // parts, sliced(lax.rem(i, parts), gb.shape[1])
            columns = pl.ds(pl.multiple_of(lax.rem(unit, cuts) * HALF, HALF), HALF)
            return (
                move(gates.at[unit // cuts, at_t, columns], gb.at[slot], gu_sem.at[0, slot]),
                move(ups.at[unit // cuts, at_t, columns], ub.at[slot], gu_sem.at[1, slot]),
            )

        @pl.loop(1, 2 * chunks)
        def _(i):
            c, t = i // 2, lax.rem(i, 2)

            @pl.when(i + 1 < 2 * chunks)
            def _():
                hidden(i + 1).start()

            for k in range(4):

                @pl.when(i == 2 + k + k // 2)
                def _():
                    inputs(k // 2)[k % 2].start()

            hidden(i).wait()
            add_to(big_blocks(c, dm.chunk), t == 0, dot(dytb[:, sliced(t, span)], hidden_at(i)[...]))

            @pl.when(i == 1)
            def _():
                pl.semaphore_wait(ready, 2)

            @pl.when(t == 1)
            def _():
                downs.step1(c)

            @pl.when(jnp.logical_and(t == 1, c >= 2))
            def _():
                downs.step2(c - 2)

        a0t_back.wait()
        at_end.wait()
        for copy in at_last:
            copy.wait()

        def sums(c):
            return w.at[c // 3, lax.rem(c, 3), 0 : 2 * dm.packed, :]

        def put_down(c):
            def put(half, columns, g):
                sums(c)[pl.ds(half * dm.packed + dm.rows, dm.packed - dm.rows), columns] = g

            return put

        def put_wide(unit):
            def put(half, columns, g):
                to = sums(unit // cuts).at[:, pl.ds(pl.multiple_of(lax.rem(unit, cuts) * HALF, HALF), HALF)]
                to[pl.ds(half * dm.packed, dm.rows), :] = g

            return put

        cut_units = chunks * cuts
        first, middle = 0, parts // 2

        @pl.loop(0, cut_units * parts)
        def _(i):
            unit, t, slot = i // parts, lax.rem(i, parts), lax.rem(i, 2)

            @pl.when(jnp.logical_and(t == first, unit >= 1))
            def _():
                wides.step1(unit - 1)

            @pl.when(jnp.logical_and(t == middle, unit >= 3))
            def _():
                wides.step3(unit - 3, put_wide(unit - 3), squares)

            @pl.when(jnp.logical_and(t == middle, unit >= 2))
            def _():
                wides.step2(unit - 2)

            @pl.when(jnp.logical_and(i >= 1, i < 3))
            def _():
                downs.step2(chunks - 3 + i)

            @pl.when(jnp.logical_and(i >= 4, i < 4 + chunks))
            def _():
                downs.step3(i - 4, put_down(i - 4), squares)

            @pl.when(jnp.logical_and(i >= 1, i + 1 < cut_units * parts))
            def _():
                for copy in inputs(i + 1):
                    copy.start()

            for copy in inputs(i):
                copy.wait()
            c = unit // cuts
            slot_w, which = chunks - 1 + (c // 2) * (1 - lax.rem(c, 2)), lax.rem(c, 2) * (1 + c // 2)
            weights = w[slot_w, which, :, pl.ds(pl.multiple_of(lax.rem(unit, cuts) * HALF, HALF), HALF)]
            size = gb.shape[1]
            blocks = [(slice(b, b + SMALL), sliced(t * (size // SMALL) + b // SMALL, SMALL)) for b in range(0, size, SMALL)]
            by_acts = [dot(abuf[tokens, :], weights) for _, tokens in blocks]
            totals = [None, None]
            for (rows, tokens), by_act in zip(blocks, by_acts, strict=True):
                bg[rows, :], bu[rows, :] = back_through(gb[slot, rows, :], ub[slot, rows, :], by_act)
                for k, right in enumerate((bg, bu)):
                    term = dot(at[:, tokens], right[rows, :])
                    totals[k] = term if totals[k] is None else totals[k] + term
            for k in range(2):
                add_to(wides.terms(unit, k), t == 0, totals[k])

        last = cut_units - 1
        wides.step1(last)
        wides.step2(last - 1)
        wides.step3(last - 2, put_wide(last - 2), squares)
        wides.step2(last)
        wides.step3(last - 1, put_wide(last - 1), squares)
        wides.step3(last, put_wide(last), squares)
        out = [move(sums(c), grads_out.at[0, c], g_sem.at[1 + c]) for c in range(chunks)]
        copies = []
        for k in range(dm.n - 1, 0, -1):
            to = lax.rem(me + k, dm.n)
            copies.append(remote(squares, squares_out.at[me], ssends.at[k - 1], srecvs.at[k - 1], {"dp": to}))
        copies.append(move(squares, squares_out.at[me], g_sem.at[0]))
        for copy in copies:
            copy.start()
        for copy in out:
            copy.start()
        for copy in copies:
            copy.wait()
        for copy in out:
            copy.wait()

    part = CUT_TILE
    pl.run_scoped(
        backward0,
        pltpu.VMEM((2, part, HALF), F32), pltpu.VMEM((2, part, HALF), F32), pltpu.VMEM((part, HALF), BF), pltpu.VMEM((part, HALF), BF),
    )


def optimizer_kernel(dm, squares_in, grads_in, *refs):
    ins, outs, (squares, grads, *buffers), (g_sem, in_sem, out_sem) = refs[:9], refs[9:18], refs[18:26], refs[26:]
    move(squares_in, squares, g_sem.at[dm.layers]).start()
    stores = [buffers[0:2], buffers[2:4], buffers[4:6]]
    halves = 2
    pieces = [(layer, which, half) for layer in range(dm.layers) for which in range(3) for half in range(halves)]

    def places(piece):
        layer, which, half = piece
        out = []
        for kind in range(3):
            if which < 2:
                cut = slice(half * dm.ff // halves, (half + 1) * dm.ff // halves)
                here = stores[kind][0].at[2 * layer + which, :, cut]
                out.append((ins[3 * kind + which].at[layer, :, cut], here, outs[3 * kind + which].at[layer, :, cut]))
            else:
                cut = slice(half * dm.own_ff // halves, (half + 1) * dm.own_ff // halves)
                here = stores[kind][1].at[layer, cut, :]
                out.append((ins[3 * kind + which].at[layer, cut, :], here, outs[3 * kind + which].at[layer, cut, :]))
        return out

    fetch = [move(grads_in.at[layer], grads.at[layer], g_sem.at[layer]) for layer in range(dm.layers)]
    loads = [[move(a, b, in_sem.at[k, kind]) for kind, (a, b, _) in enumerate(places(p))] for k, p in enumerate(pieces)]
    writes = [[move(b, c, out_sem.at[k, kind]) for kind, (_, b, c) in enumerate(places(p))] for k, p in enumerate(pieces)]
    for layer in range(dm.layers):
        fetch[layer].start()
        for k, piece in enumerate(pieces):
            if piece[0] == layer:
                for copy in loads[k]:
                    copy.start()
    count = dm.layers * 3 * dm.d * dm.ff
    move(squares_in, squares, g_sem.at[dm.layers]).wait()
    total = squares[0]
    for k in range(1, dm.n):
        total = total + squares[k]
    factor = jnp.minimum(1.0, 0.5 * lax.rsqrt(jnp.sum(total) / count + 1e-30))
    size = dm.d // 2 // dm.n

    def adamw(g, refs, at):
        w, m, v = (ref[at] for ref in refs)
        g = g.astype(F32) * factor
        w = w.astype(F32)
        m = 0.9 * m + 0.1 * g
        v = 0.95 * v + 0.05 * g * g
        change = m * lax.rsqrt(v + 1e-8) + 0.1 * w
        refs[0][at] = (w - 0.02 * change).astype(BF)
        refs[1][at] = m
        refs[2][at] = v

    for k, (layer, which, half) in enumerate(pieces):
        if (which, half) == (0, 0):
            fetch[layer].wait()
        for copy in loads[k]:
            copy.wait()
        refs = [here for _, here, _ in places(pieces[k])]
        if which < 2:
            for b in range(dm.ff // halves // LANES):
                q, c = divmod(half * dm.ff // halves // LANES + b, dm.chunks)
                g = grads[layer, c, which * dm.packed : which * dm.packed + dm.rows, q * LANES : (q + 1) * LANES]
                adamw(g, refs, (slice(None), slice(b * LANES, (b + 1) * LANES)))
        else:
            for b in range(dm.own_ff // halves // LANES):
                c = half * dm.own_ff // halves // LANES + b
                for row in range(2 * dm.n):
                    side, i = divmod(row, dm.n)
                    start = side * dm.packed + dm.rows
                    g = grads[layer, c, start : start + size, i * LANES : (i + 1) * LANES]
                    if row == 0:
                        rows = []
                    rows.append(g)
                adamw(jnp.concatenate(rows, axis=0).T, refs, (slice(b * LANES, (b + 1) * LANES), slice(None)))
        for copy in writes[k]:
            copy.start()
    for copies in writes:
        for copy in copies:
            copy.wait()


def step(mesh, x, dy, *arrays):
    weights, m, v = (arrays[i : i + 3] for i in (0, 3, 6))
    x, dy = x[0], dy[0]
    w_gate, w_up, w_down = weights
    n = mesh.shape["dp"]
    dm = Dims(w_gate.shape[0], x.shape[0], x.shape[1], w_gate.shape[2], n)
    tokens, d, chunk, chunks, tiles = dm.tokens, dm.d, dm.chunk, dm.chunks, dm.tiles
    hbm = pl.BlockSpec(memory_space=pltpu.HBM)
    shape = jax.ShapeDtypeStruct
    dma = lambda *s: pltpu.SemaphoreType.DMA(s)
    natural, turned, per_chunk = (tokens, d), (d, tokens), (chunks, tokens, chunk)
    block, wide, down = (2 * dm.packed, chunk), (dm.rows, chunk), (dm.packed - dm.rows, chunk)
    units = dm.layers * chunks
    semaphores = [
        dma(units), dma(2), dma(dm.small), dma(dm.small), dma(3, 2), dma(2, 2), dma(2, 2, chunks), dma(2, 2), dma(2), dma(9), dma(1 + chunks),
        pltpu.SemaphoreType.REGULAR,
        dma(units, Gather.COPIES), dma(units, Gather.COPIES), dma(4, 6), dma(4, 6), dma(chunks, 6), dma(chunks, 6), dma(n - 1), dma(n - 1),
    ]

    def kernel(*refs):
        pl.run_scoped(lambda *scoped: whole_kernel(dm, *refs, *scoped), *semaphores)

    grads, squares, *_ = pl.pallas_call(
        kernel,
        out_shape=[
            shape((2, chunks, *block), BF), shape((n, 8, LANES), F32), shape(per_chunk, F32), shape(per_chunk, F32), shape(per_chunk, BF),
            shape(turned, BF), shape((chunks - 1, d, chunk), BF), shape(per_chunk, BF), shape(per_chunk, BF),
        ],
        in_specs=[hbm] * 5,
        out_specs=[hbm] * 9,
        scratch_shapes=[
            pltpu.VMEM(natural, BF), pltpu.VMEM(turned, BF), pltpu.VMEM(turned, BF), pltpu.VMEM(natural, BF), pltpu.VMEM(turned, BF),
            pltpu.VMEM((tokens // HALF, d, HALF), F32), pltpu.VMEM((chunks + 1, 3, d, chunk), BF), pltpu.VMEM((dm.own_ff, d), BF),
            pltpu.VMEM((2, 6, *wide), BF), pltpu.VMEM((2, 6, *wide), BF), pltpu.VMEM((2, 6, *down), BF), pltpu.VMEM((2, 6, *down), BF),
            pltpu.VMEM((8, LANES), F32),
        ],
        compiler_params=pltpu.CompilerParams(vmem_limit_bytes=VMEM_LIMIT, collective_id=0, has_side_effects=True),
        name="whole",
    )(x, dy, w_gate, w_up, w_down)

    wides, downs = (2 * dm.layers, dm.rows, dm.ff), (dm.layers, dm.own_ff, d)
    return tuple(
        pl.pallas_call(
            functools.partial(optimizer_kernel, dm),
            out_shape=[shape(w.shape, BF) for w in weights] + [shape(w.shape, F32) for w in weights] * 2,
            in_specs=[hbm] * 11,
            out_specs=[hbm] * 9,
            scratch_shapes=[
                pltpu.VMEM((n, 8, LANES), F32), pltpu.VMEM((2, chunks, *block), BF), pltpu.VMEM(wides, BF), pltpu.VMEM(downs, BF),
                pltpu.VMEM(wides, F32), pltpu.VMEM(downs, F32), pltpu.VMEM(wides, F32), pltpu.VMEM(downs, F32),
                dma(dm.layers + 1), dma(6 * dm.layers, 3), dma(6 * dm.layers, 3),
            ],
            compiler_params=pltpu.CompilerParams(vmem_limit_bytes=VMEM_LIMIT),
            name="optimizer",
        )(squares, grads, *weights, *m, *v)
    )


def solution(mesh):
    states, cut = P(("rep", "dp"), None, None), P(None, "dp", None)
    return jax.shard_map(
        functools.partial(step, mesh),
        mesh=mesh,
        in_specs=(states, states) + (cut,) * 9,
        out_specs=(P("rep", "dp", None),) * 9,
        check_vma=False,
    )
```
